128 devices in a mesh: dp: 16 (over z, y), ep: 8 (over x, core).
Axes of the slice: x: 4, y: 4, z: 4, core: 2. Of those that a mesh axis runs over, the one named last changes fastest.
Arguments:
- tok_x: bfloat16 [32768, 4096], P(('dp', 'ep'))
- tok_dy: bfloat16 [32768, 4096], P(('dp', 'ep'))
- exp_first: int32 [32768], P(('dp', 'ep'))
- exp_second: int32 [32768], P(('dp', 'ep'))
- eligible: int32 [32768, 16], P(('dp', 'ep'))
- slot_first: int32 [32768], P(('dp', 'ep'))
- slot_second: int32 [32768], P(('dp', 'ep'))
- ln_weight: bfloat16 [4096], replicated
- ln_bias: bfloat16 [4096], replicated
- router: bfloat16 [4096, 16], replicated
- w_gate: bfloat16 [16, 4096, 448], P('ep')
- w_up: bfloat16 [16, 4096, 448], P('ep')
- w_down: bfloat16 [16, 448, 4096], P('ep')
Outputs:
- output 1: bfloat16 [32768, 4096], P(('dp', 'ep'))
- output 2: bfloat16 [32768, 4096], P(('dp', 'ep'))
- output 3: float32 [16, 4096, 448], P('ep')
- output 4: float32 [16, 4096, 448], P('ep')
- output 5: float32 [16, 448, 4096], P('ep')
- output 6: float32 [4096, 16], replicated
- output 7: float32 [4096], replicated
- output 8: float32 [4096], replicated
All inputs are finite; a program needn't handle non-finite values.
Results may differ from the reference program's by a relative error of at most 0.00505461.
Values are sent between devices in bfloat16 or wider.
A program may use at most 1 GiB of HBM per device.

```python
import jax
import jax.numpy as jnp
from jax import lax

SHARDS = 128
TOK_DEV = 256
D_MODEL = 4096
FF_DIM = 448
EXPERTS = 16
SLOT_CAP = 48
LN_EPS = 1e-5


def draw_routing(rng_key):
    n_tok = SHARDS * TOK_DEV
    key_list = jax.random.split(rng_key, 5)
    pick_a = jax.random.randint(key_list[0], (n_tok,), 0, EXPERTS)
    pick_b = jax.random.randint(key_list[1], (n_tok,), 0, EXPERTS)
    pick_c = jax.random.randint(key_list[2], (n_tok,), 0, EXPERTS)
    first_pick = jnp.minimum(jnp.minimum(pick_a, pick_b), pick_c)
    second_pick = (first_pick + 1 + jax.random.randint(key_list[3], (n_tok,), 0, EXPERTS - 1)) % EXPERTS
    expert_ids = jnp.arange(EXPERTS)
    hot_first = (first_pick[:, None] == expert_ids[None, :]).astype(jnp.int32)
    hot_second = (second_pick[:, None] == expert_ids[None, :]).astype(jnp.int32)
    extra_bits = (jax.random.randint(key_list[4], (n_tok, EXPERTS), 0, 8) == 0).astype(jnp.int32)
    eligible = jnp.maximum(extra_bits, jnp.maximum(hot_first, hot_second))
    per_first = hot_first.reshape(SHARDS, TOK_DEV, EXPERTS)
    per_second = hot_second.reshape(SHARDS, TOK_DEV, EXPERTS)
    rank_first = jnp.sum((jnp.cumsum(per_first, axis=1) - per_first) * per_first, axis=2).reshape(n_tok)
    used_first = jnp.sum(per_first, axis=1, keepdims=True)
    rank_second = jnp.sum((jnp.cumsum(per_second, axis=1) - per_second + used_first) * per_second, axis=2).reshape(n_tok)
    slot_first = jnp.where(rank_first < SLOT_CAP, rank_first, -1)
    slot_second = jnp.where(rank_second < SLOT_CAP, rank_second, -1)
    return first_pick, second_pick, eligible, slot_first, slot_second


def setup_inputs(seed: int = 0) -> dict:
    key_list = jax.random.split(jax.random.key(seed), 10)
    n_tok = SHARDS * TOK_DEV
    first_pick, second_pick, eligible, slot_first, slot_second = draw_routing(key_list[0])
    tok_x = jax.random.normal(key_list[1], (n_tok, D_MODEL), jnp.float32).astype(jnp.bfloat16)
    tok_dy = jax.random.normal(key_list[2], (n_tok, D_MODEL), jnp.float32).astype(jnp.bfloat16)
    ln_weight = (1.0 + 0.3 * jax.random.normal(key_list[3], (D_MODEL,), jnp.float32)).astype(jnp.bfloat16)
    ln_bias = (0.3 * jax.random.normal(key_list[4], (D_MODEL,), jnp.float32)).astype(jnp.bfloat16)
    router = (1.5 * D_MODEL ** -0.5 * jax.random.normal(key_list[5], (D_MODEL, EXPERTS), jnp.float32)).astype(jnp.bfloat16)
    w_gate = (D_MODEL ** -0.5 * jax.random.normal(key_list[6], (EXPERTS, D_MODEL, FF_DIM), jnp.float32)).astype(jnp.bfloat16)
    w_up = (D_MODEL ** -0.5 * jax.random.normal(key_list[7], (EXPERTS, D_MODEL, FF_DIM), jnp.float32)).astype(jnp.bfloat16)
    w_down = (3.0 * FF_DIM ** -0.5 * jax.random.normal(key_list[8], (EXPERTS, FF_DIM, D_MODEL), jnp.float32)).astype(jnp.bfloat16)
    return {'tok_x': tok_x, 'tok_dy': tok_dy, 'exp_first': first_pick, 'exp_second': second_pick,
            'eligible': eligible, 'slot_first': slot_first, 'slot_second': slot_second,
            'ln_weight': ln_weight, 'ln_bias': ln_bias, 'router': router,
            'w_gate': w_gate, 'w_up': w_up, 'w_down': w_down}


def layer_norm(x_rows, ln_weight, ln_bias):
    x_float = x_rows.astype(jnp.float32)
    centered = x_float - jnp.mean(x_float, axis=-1, keepdims=True)
    inv_std = lax.rsqrt(jnp.mean(centered * centered, axis=-1, keepdims=True) + LN_EPS)
    x_hat = centered * inv_std
    hidden = (x_hat * ln_weight.astype(jnp.float32) + ln_bias.astype(jnp.float32)).astype(jnp.bfloat16)
    return hidden, x_hat, inv_std


def layer_norm_back(grad_h, x_hat, inv_std, ln_weight):
    scaled = grad_h * ln_weight.astype(jnp.float32)
    return inv_std * (scaled - jnp.mean(scaled, axis=-1, keepdims=True)
                      - x_hat * jnp.mean(scaled * x_hat, axis=-1, keepdims=True))


def masked_gate(logits, allowed, choice):
    expert_ids = jnp.arange(logits.shape[-1])
    prob_all = jax.nn.softmax(jnp.where(allowed, logits, -1e30), axis=-1)
    picked = (choice[:, None] == expert_ids[None, :]).astype(jnp.float32)
    return jnp.sum(prob_all * picked, axis=-1), prob_all, picked


def expert_pass(operands):
    hid_rows, grad_rows, gate_w, up_w, down_w = operands
    pre_gate = jnp.dot(hid_rows, gate_w, preferred_element_type=jnp.float32)
    pre_up = jnp.dot(hid_rows, up_w, preferred_element_type=jnp.float32)
    sig_gate = jax.nn.sigmoid(pre_gate)
    silu_gate = pre_gate * sig_gate
    inner_act = (silu_gate * pre_up).astype(jnp.bfloat16)
    exp_out = jnp.dot(inner_act, down_w, preferred_element_type=jnp.float32).astype(jnp.bfloat16)
    grad_inner = jnp.dot(grad_rows, down_w.T, preferred_element_type=jnp.float32)
    grad_pre_gate = (grad_inner * pre_up * sig_gate * (1.0 + pre_gate * (1.0 - sig_gate))).astype(jnp.bfloat16)
    grad_pre_up = (grad_inner * silu_gate).astype(jnp.bfloat16)
    grad_hid = (jnp.dot(grad_pre_gate, gate_w.T, preferred_element_type=jnp.float32)
                + jnp.dot(grad_pre_up, up_w.T, preferred_element_type=jnp.float32)).astype(jnp.bfloat16)
    dw_gate = jnp.dot(hid_rows.T, grad_pre_gate, preferred_element_type=jnp.float32)
    dw_up = jnp.dot(hid_rows.T, grad_pre_up, preferred_element_type=jnp.float32)
    dw_down = jnp.dot(inner_act.T, grad_rows, preferred_element_type=jnp.float32)
    return exp_out, grad_hid, dw_gate, dw_up, dw_down


def reference(tok_x, tok_dy, exp_first, exp_second, eligible, slot_first, slot_second,
              ln_weight, ln_bias, router, w_gate, w_up, w_down):
    n_tok = tok_x.shape[0]
    hidden, x_hat, inv_std = layer_norm(tok_x, ln_weight, ln_bias)
    logits = jnp.dot(hidden, router, preferred_element_type=jnp.float32)
    expert_ids = jnp.arange(EXPERTS)
    allowed = eligible > 0
    gate_one, prob_one, pick_one = masked_gate(logits, allowed, exp_first)
    gate_two, prob_two, pick_two = masked_gate(logits, allowed & (expert_ids[None, :] != exp_first[:, None]), exp_second)
    n_rows = EXPERTS * SHARDS * SLOT_CAP
    shard_idx = jnp.arange(n_tok) // TOK_DEV
    row_one = jnp.where(slot_first >= 0, (exp_first * SHARDS + shard_idx) * SLOT_CAP + slot_first, n_rows)
    row_two = jnp.where(slot_second >= 0, (exp_second * SHARDS + shard_idx) * SLOT_CAP + slot_second, n_rows)
    dy_float = tok_dy.astype(jnp.float32)
    grad_one = (gate_one[:, None] * dy_float).astype(jnp.bfloat16)
    grad_two = (gate_two[:, None] * dy_float).astype(jnp.bfloat16)
    empty_rows = jnp.zeros((n_rows, D_MODEL), jnp.bfloat16)
    hid_buf = empty_rows.at[row_one].set(hidden, mode='drop').at[row_two].set(hidden, mode='drop')
    grad_buf = empty_rows.at[row_one].set(grad_one, mode='drop').at[row_two].set(grad_two, mode='drop')
    exp_out, grad_hid, dw_gate, dw_up, dw_down = lax.map(
        expert_pass,
        (hid_buf.reshape(EXPERTS, SHARDS * SLOT_CAP, D_MODEL), grad_buf.reshape(EXPERTS, SHARDS * SLOT_CAP, D_MODEL),
         w_gate, w_up, w_down))
    exp_out = exp_out.reshape(n_rows, D_MODEL)
    grad_hid = grad_hid.reshape(n_rows, D_MODEL)
    out_one = jnp.take(exp_out, row_one, axis=0, mode='fill', fill_value=0).astype(jnp.float32)
    out_two = jnp.take(exp_out, row_two, axis=0, mode='fill', fill_value=0).astype(jnp.float32)
    y_mix = gate_one[:, None] * out_one + gate_two[:, None] * out_two
    out_tok = (tok_x.astype(jnp.float32) + y_mix).astype(jnp.bfloat16)
    dgate_one = jnp.sum(dy_float * out_one, axis=-1)
    dgate_two = jnp.sum(dy_float * out_two, axis=-1)
    d_logits = ((dgate_one * gate_one)[:, None] * (pick_one - prob_one)
                + (dgate_two * gate_two)[:, None] * (pick_two - prob_two)).astype(jnp.bfloat16)
    d_router = jnp.dot(hidden.T, d_logits, preferred_element_type=jnp.float32)
    grad_h = (jnp.dot(d_logits, router.T, preferred_element_type=jnp.float32)
              + jnp.take(grad_hid, row_one, axis=0, mode='fill', fill_value=0).astype(jnp.float32)
              + jnp.take(grad_hid, row_two, axis=0, mode='fill', fill_value=0).astype(jnp.float32))
    d_ln_weight = jnp.sum(grad_h * x_hat, axis=0)
    d_ln_bias = jnp.sum(grad_h, axis=0)
    dx_tok = (dy_float + layer_norm_back(grad_h, x_hat, inv_std, ln_weight)).astype(jnp.bfloat16)
    return (out_tok, dx_tok, dw_gate, dw_up, dw_down, d_router, d_ln_weight, d_ln_bias)
```

```python
import functools

import jax
import jax.numpy as jnp
from jax import lax
from jax.experimental import pallas as pl
from jax.experimental.pallas import tpu as pltpu
from jax.sharding import PartitionSpec as P


LN_EPS = 1e-5
CORES = 2
UNITS = 4
F32 = jnp.float32
BF16 = jnp.bfloat16
MESH_ID = pl.DeviceIdType.MESH
NT = (((1,), (1,)), ((), ()))


def layer_norm(x_rows, ln_weight, ln_bias):
    x_float = x_rows.astype(F32)
    centered = x_float - jnp.mean(x_float, axis=-1, keepdims=True)
    inv_std = lax.rsqrt(jnp.mean(centered * centered, axis=-1, keepdims=True) + LN_EPS)
    x_hat = centered * inv_std
    hidden = (x_hat * ln_weight.astype(F32) + ln_bias.astype(F32)).astype(BF16)
    return hidden, x_hat, inv_std


def layer_norm_back(grad_h, x_hat, inv_std, ln_weight):
    scaled = grad_h * ln_weight.astype(F32)
    return inv_std * (scaled - jnp.mean(scaled, axis=-1, keepdims=True)
                      - x_hat * jnp.mean(scaled * x_hat, axis=-1, keepdims=True))


def masked_gate(logits, allowed, choice):
    expert_ids = jnp.arange(logits.shape[-1])
    prob_all = jax.nn.softmax(jnp.where(allowed, logits, -1e30), axis=-1)
    picked = (choice[:, None] == expert_ids[None, :]).astype(F32)
    return jnp.sum(prob_all * picked, axis=-1), prob_all, picked


def ring_offsets(n_x):
    near = [d for d in (1, n_x - 1) if 0 < d < n_x]
    near = list(dict.fromkeys(near))
    far = [d for d in range(2, n_x - 1)]
    out = [(0, 1)]
    for group in (near, far):
        for core in range(CORES):
            out += [(d, core) for d in group]
    return out


class Place:
    def __init__(self, n_ep, grid):
        self.n_x, self.grid = n_ep // CORES, grid
        self.ep, self.dp = lax.axis_index('ep'), lax.axis_index('dp')
        self.x, self.core = self.ep // CORES, self.ep % CORES
        self.z, self.y = self.dp // grid, self.dp % grid
        self.offsets = ring_offsets(self.n_x)

    def ep_to(self, k):
        dx, dc = self.offsets[k]
        return lax.rem(self.x + dx, self.n_x) * CORES + lax.rem(self.core + dc, CORES)

    def ep_from(self, k):
        dx, dc = self.offsets[k]
        return lax.rem(self.x + (self.n_x - dx), self.n_x) * CORES + lax.rem(self.core + dc, CORES)

    def step(self, axis, k):
        here = self.y if axis == 'y' else self.z
        return lax.rem(here + k + self.grid, self.grid)

    def device(self, axis, k):
        if axis == 'y':
            return (self.z * self.grid + self.step('y', k), self.ep)
        return (self.step('z', k) * self.grid + self.y, self.ep)

    def flip(self, axis, bits):
        if axis == 'y':
            return (self.z * self.grid + (self.y ^ bits), self.ep)
        return ((self.z ^ bits) * self.grid + self.y, self.ep)

    def barrier(self):
        sem = pltpu.get_barrier_semaphore()
        peers = [(self.dp, self.ep_to(k)) for k in range(len(self.offsets))]
        for k in range(1, self.grid):
            peers += [self.device('y', k), self.device('z', k)]
        for peer in peers:
            pl.semaphore_signal(sem, inc=1, device_id=peer, device_id_type=MESH_ID)
        pl.semaphore_wait(sem, len(peers))


def rows_at(start, size, unit):
    return pl.ds(pl.multiple_of(start, unit), size)


class Spread:
    STAGES = ((0,), (1, 2), (3, 4, 5, 6), tuple(range(7, 15)))

    def __init__(self, here, own, held, send, recv):
        self.here, self.own, self.held, self.sems = here, own, held, (send, recv)

    def plan(self, unit, index):
        axes = ('y', 'z') if unit < UNITS // 2 else ('z', 'y')
        one, two = (1, 3) if unit % 2 == 0 else (3, 1)
        line = (0, one, two, one ^ two)
        if index < 1:
            return axes, (axes[0], one), (0, 0)
        if index < 3:
            return axes, (axes[0], two), (line[index - 1], 0)
        if index < 7:
            return axes, (axes[1], one), (line[index - 3], 0)
        return axes, (axes[1], two), (line[(index - 7) % 4], (0, one)[(index - 7) // 4])

    def copy(self, unit, index):
        axes, (axis, flip), offsets = self.plan(unit, index)
        at = dict(zip(axes, offsets))
        owner = (self.here.z ^ at['z']) * self.here.grid + (self.here.y ^ at['y'])
        held = self.held.at[owner, unit]
        source = self.own.at[unit] if self.own is not None and offsets == (0, 0) else held
        return pltpu.make_async_remote_copy(src_ref=source, dst_ref=held, send_sem=self.sems[0].at[unit, index],
                                            recv_sem=self.sems[1].at[unit, index], device_id=self.here.flip(axis, flip),
                                            device_id_type=MESH_ID)

    def each(self, stage, picks=None):
        ids = self.STAGES[stage]
        for index in ids if picks is None else [ids[p] for p in picks]:
            for unit in range(UNITS):
                yield self.copy(unit, index)

    def send(self, stage, picks=None):
        for c in self.each(stage, picks):
            c.start()

    def receive(self, stage):
        for c in self.each(stage):
            c.wait_recv()

    def sent(self, stage):
        for c in self.each(stage):
            c.wait_send()


def spread_kernel(grid, cap, held_in, o_in, dh_in, held, o_out, dh_out, sp_s, sp_r, ba_s, ba_r, loc):
    rows = o_in.shape[0]
    here = Place(rows // cap, grid)
    n_peer = len(here.offsets)
    here.barrier()
    spread = Spread(here, None, held, sp_s, sp_r)
    spread.send(3)
    pairs = ((o_in, o_out), (dh_in, dh_out))

    def block(e):
        return rows_at(e * cap, cap, 16)

    def back(j, k):
        src, dst = pairs[j]
        return pltpu.make_async_remote_copy(src_ref=src.at[block(here.ep_to(k)), :], dst_ref=dst.at[block(here.ep), :],
                                            send_sem=ba_s.at[j, k], recv_sem=ba_r.at[j, k], device_id=(here.dp, here.ep_to(k)),
                                            device_id_type=MESH_ID)

    own = [pltpu.make_async_copy(src.at[block(here.ep), :], dst.at[block(here.ep), :], loc.at[j]) for j, (src, dst) in enumerate(pairs)]
    for j in range(2):
        for k in range(n_peer):
            back(j, k).start()
        own[j].start()
    for j in range(2):
        for k in range(n_peer):
            back(j, k).wait()
        own[j].wait()
    spread.receive(3)
    spread.sent(3)


def spread_call(held, o, dh, cap, grid, collective_id):
    dma = pltpu.SemaphoreType.DMA
    n_peer = o.shape[0] // cap - 1
    hbm = pl.BlockSpec(memory_space=pl.ANY)
    return pl.pallas_call(
        functools.partial(spread_kernel, grid, cap),
        out_shape=tuple(jax.ShapeDtypeStruct(x.shape, x.dtype) for x in (held, o, dh)),
        in_specs=[hbm] * 3, out_specs=(hbm,) * 3, input_output_aliases={0: 0},
        scratch_shapes=[dma((UNITS, 15)), dma((UNITS, 15)), dma((2, n_peer)), dma((2, n_peer)), dma((2,))],
        compiler_params=pltpu.CompilerParams(collective_id=collective_id, has_side_effects=True),
        cost_estimate=pl.CostEstimate(flops=1_000_000_000, bytes_accessed=30_000_000, transcendentals=0),
        name='spread',
    )(held, o, dh)


def expert_kernel(dims, *refs):
    expert, grid, chunk, cap, first = dims
    refs = list(refs)
    take = lambda n: [refs.pop(0) for _ in range(n)]
    if first:
        sel_in, wg_h, wu_h, wd_h = take(6), *take(3)
        o_h, dh_h, sh_h, h_next, q_next, hsl_next, qsl_next = take(7)
    else:
        h_next, q_next, hsl_next, qsl_next, wg_h, wu_h, wd_h, *carry = take(9)
        done_h, = take(1)
        o_h, dh_h, sh_h, *carry_out = take(5)
        all_h, = take(1)
    h_recv, q_recv, wg, wu, wd, a_t, b_t, d_t, u_all, da_all, db_all, h_sl, q_sl, dw, rsb, act, act_b, eye = take(18)
    loc, hs_s, hs_r, qs_s, qs_r, ga_s, ga_r, rs_s, rs_r = take(9)
    if first:
        sel_h, sel_q, sel_h_next, sel_q_next, hidden, pair, h_send, q_send, h_send_next, q_send_next = take(10)
        xh_s, xh_r, xq_s, xq_r, nh_s, nh_r, nq_s, nq_r, ns_h_s, ns_h_r, ns_q_s, ns_q_r, lin = take(13)
        o_v, dh_v = h_send, q_send
    else:
        o_v, dh_v = take(2)
        ba_s, ba_r, ba_l, lin, sp_s, sp_r = take(6)
    rows, d_model = h_recv.shape
    ff = wg.shape[0]
    quarter = d_model // grid
    share = ff // grid
    here = Place(rows // cap, grid)
    n_peer = len(here.offsets)
    ep = here.ep
    remote = functools.partial(pltpu.make_async_remote_copy, device_id_type=MESH_ID)
    wide = chunk // 2

    def spot(axis):
        return here.y if axis == 'y' else here.z

    def block(e):
        return rows_at(e * cap, cap, 16)

    weights = [pltpu.make_async_copy(src.at[expert], dst, loc.at[i]) for i, (src, dst) in enumerate(((wg_h, wg), (wu_h, wu), (wd_h, wd)))]

    def x_copy(src, dst, send, recv, k):
        return remote(src_ref=src.at[block(here.ep_to(k)), :], dst_ref=dst.at[block(ep), :],
                      send_sem=send.at[k], recv_sem=recv.at[k], device_id=(here.dp, here.ep_to(k)))

    def slice_copy(axis, buf, sl, send, recv, src_ep, k):
        return remote(src_ref=buf.at[block(src_ep), rows_at(here.step(axis, k) * quarter, quarter, 128)],
                      dst_ref=sl.at[rows_at(spot(axis) * rows + src_ep * cap, cap, 16), :],
                      send_sem=send.at[k], recv_sem=recv.at[k], device_id=here.device(axis, k))

    def slices(axis, buf, sl, send, recv, k):
        return remote(src_ref=buf.at[:, pl.ds(0, quarter)], dst_ref=sl.at[pl.ds(0, rows), :],
                      send_sem=send.at[k], recv_sem=recv.at[k], device_id=here.device(axis, k))

    half = ff // 2
    gathers = [(u_all, pl.ds(0, half), 'z', 1, 3), (u_all, pl.ds(half, half), 'z', 3, 1),
               (da_all, pl.ds(0, ff), 'y', 1, 3), (db_all, pl.ds(0, ff), 'y', 3, 1)]

    def share_t(g, j):
        ref, part, axis, one, two = gathers[g]
        flip = two if j else one
        owner = spot(axis) ^ (one if j == 2 else 0)
        view = ref.at[part, rows_at(owner * rows, rows, 128)]
        return remote(src_ref=view, dst_ref=view, send_sem=ga_s.at[g, j], recv_sem=ga_r.at[g, j], device_id=here.flip(axis, flip))

    def share_on(units):
        for g in units:
            share_t(g, 0).wait_recv()
            for j in (1, 2):
                share_t(g, j).start()

    def share_done(units):
        for g in units:
            for j in (1, 2):
                share_t(g, j).wait_recv()

    reduces = [(0, pl.ds(0, quarter), 'z', 1, 3), (1, pl.ds(0, quarter), 'z', 3, 1),
               (2, pl.ds(0, quarter // 2), 'y', 1, 3), (2, pl.ds(quarter // 2, quarter // 2), 'y', 3, 1)]

    def part_at(i):
        return rows_at(i * share, share, 8)

    def reduce_copy(r, j):
        t, cols, axis, one, two = reduces[r]
        here_at = spot(axis)
        flip, chunk_at = ((one, here_at ^ one), (one, here_at ^ one ^ two), (two, here_at ^ two))[j]
        return remote(src_ref=dw.at[t, part_at(chunk_at), cols], dst_ref=rsb.at[t, j, :, cols],
                      send_sem=rs_s.at[r, j], recv_sem=rs_r.at[r, j], device_id=here.flip(axis, flip))

    def reduce_start(units):
        for r in units:
            for j in (0, 1):
                reduce_copy(r, j).start()

    def reduce_on(units):
        for r in units:
            t, cols, axis, _, two = reduces[r]
            reduce_copy(r, 0).wait_recv()
            reduce_copy(r, 1).wait_recv()
            on = part_at(spot(axis) ^ two)
            dw[t, on, cols] = dw[t, on, cols] + rsb[t, 1, :, cols]
            reduce_copy(r, 2).start()

    def reduce_end(t):
        units = [r for r in range(len(reduces)) if reduces[r][0] == t]
        axis = reduces[units[0]][2]
        for r in units:
            reduce_copy(r, 2).wait_recv()
        rsb[t, 0] = dw[t, part_at(spot(axis)), :] + rsb[t, 0] + rsb[t, 2]
        unit = quarter // UNITS
        outs = [pltpu.make_async_copy(rsb.at[t, 0, :, pl.ds(i * unit, unit)], sh_h.at[i, t], loc.at[5 + t * UNITS + i]) for i in range(UNITS)]
        for c in outs:
            c.start()
        return outs

    def own_slice(axis, buf, sl):
        sl[rows_at(spot(axis) * rows, rows, 16), :] = buf[:, rows_at(spot(axis) * quarter, quarter, 128)]

    strip = ff // 7
    u_cols = rows_at(here.z * rows, rows, 128)
    g_cols = rows_at(here.y * rows, rows, 128)

    def forward_pass():
        a_t[...] = jnp.zeros_like(a_t)
        b_t[...] = jnp.zeros_like(b_t)

        @pl.loop(0, d_model // chunk)
        def _(i):
            cols = rows_at(i * chunk, chunk, 128)
            a_t[...] += lax.dot_general(wg[:, cols], h_recv[:, cols], NT, preferred_element_type=F32)
            b_t[...] += lax.dot_general(wu[:, cols], h_recv[:, cols], NT, preferred_element_type=F32)

        @pl.loop(0, 7)
        def _(i):
            r = rows_at(i * strip, strip, 16)
            a = a_t[r, :]
            u_all[r, u_cols] = (a * jax.nn.sigmoid(a) * b_t[r, :]).astype(BF16)

    def backward_pass():
        d_t[...] = jnp.zeros_like(d_t)

        @pl.loop(0, d_model // chunk)
        def _(i):
            cols = rows_at(i * chunk, chunk, 128)
            d_t[...] += lax.dot_general(wd[:, cols], q_recv[:, cols], NT, preferred_element_type=F32)

        @pl.loop(0, 7)
        def _(i):
            r = rows_at(i * strip, strip, 16)
            a, b, du = a_t[r, :], b_t[r, :], d_t[r, :]
            sig = jax.nn.sigmoid(a)
            silu = a * sig
            da_all[r, g_cols] = (du * b * sig * (1.0 + a * (1.0 - sig))).astype(BF16)
            db_all[r, g_cols] = (du * silu).astype(BF16)

    def untranspose(out, ref, cols):
        out[...] = lax.dot_general(eye[...], ref[:, cols], NT, preferred_element_type=F32).astype(BF16)

    def o_pass():
        @pl.loop(0, d_model // wide)
        def _(i):
            cols = rows_at(i * wide, wide, 128)
            o_v[:, cols] = jnp.dot(act[...], wd[:, cols], preferred_element_type=F32).astype(BF16)

    def dh_pass():
        @pl.loop(0, d_model // wide)
        def _(i):
            cols = rows_at(i * wide, wide, 128)
            dh_v[:, cols] = (jnp.dot(act[...], wg[:, cols], preferred_element_type=F32)
                             + jnp.dot(act_b[...], wu[:, cols], preferred_element_type=F32)).astype(BF16)

    def weight_grad(t, left, right):
        @pl.loop(0, quarter // wide)
        def _(i):
            cols = rows_at(i * wide, wide, 128)
            dw[t, :, cols] = jnp.dot(left[...], right[:, cols], preferred_element_type=F32)

    def make_eye():
        eye[...] = (lax.broadcasted_iota(jnp.int32, (rows, rows), 0)
                    == lax.broadcasted_iota(jnp.int32, (rows, rows), 1)).astype(F32).astype(BF16)

    if first:
        inputs = [pltpu.make_async_copy(src, dst, lin.at[i])
                  for i, (src, dst) in enumerate(zip(sel_in, (sel_h, hidden, sel_q, pair, sel_h_next, sel_q_next)))]
        for c in inputs:
            c.start()
        here.barrier()
        for c in inputs:
            c.wait()

        def gather(sel, source, out, e):
            @pl.loop(0, d_model // chunk)
            def _(i):
                cols = rows_at(i * chunk, chunk, 128)
                out[block(e), cols] = jnp.dot(sel[block(e), :], source[:, cols], preferred_element_type=F32).astype(BF16)

        now = ((sel_h, hidden, h_send, h_recv, xh_s, xh_r), (sel_q, pair, q_send, q_recv, xq_s, xq_r))
        later = ((sel_h_next, hidden, h_send_next, h_next, nh_s, nh_r), (sel_q_next, pair, q_send_next, q_next, nq_s, nq_r))

        def copy_of(what, k):
            _, _, out, recv_buf, send, recv = what
            return x_copy(out, recv_buf, send, recv, k)

        pending = []

        def dispatch(what, k):
            gather(what[0], what[1], what[2], here.ep_to(k))
            pending.append(copy_of(what, k))
            if len(pending) > 1:
                pending.pop(0).start()

        for k in range(n_peer):
            for what in now:
                dispatch(what, k)
        for what in now:
            gather(what[0], what[1], what[3], ep)
        while pending:
            pending.pop(0).start()
        for c in weights:
            c.start()
        make_eye()

        spread = (('y', h_recv, h_sl, hs_s, hs_r), ('z', q_recv, q_sl, qs_s, qs_r))
        spread_next = (('y', h_next, hsl_next, ns_h_s, ns_h_r), ('z', q_next, qsl_next, ns_q_s, ns_q_r))

        def forward_own(spread, bufs):
            for (axis, _, sl, send, recv), buf in zip(spread, bufs):
                for k in range(1, grid):
                    slice_copy(axis, buf, sl, send, recv, ep, k).start()

        def forward(group, spread, p):
            for what, (axis, buf, sl, send, recv) in zip(group, spread):
                copy_of(what, p).wait_recv()
                for k in range(1, grid):
                    slice_copy(axis, buf, sl, send, recv, here.ep_from(p), k).start()

        forward_own(spread, (h_recv, q_recv))
        for what in later:
            gather(what[0], what[1], what[2], ep)
        own_next = [pltpu.make_async_copy(what[2].at[block(ep), :], what[3].at[block(ep), :], lin.at[6 + i]) for i, what in enumerate(later)]
        for p in range(n_peer):
            forward(now, spread, p)
            for what in later:
                dispatch(what, p)
        while pending:
            pending.pop(0).start()
        for c in own_next:
            c.start()
        own_slice('y', h_recv, h_sl)
        own_slice('z', q_recv, q_sl)
        for c in weights:
            c.wait()
        for k in range(n_peer):
            for what in now:
                copy_of(what, k).wait_send()
    else:
        loads = [pltpu.make_async_copy(h_next, h_recv, lin.at[0]), weights[0], weights[1],
                 pltpu.make_async_copy(q_next, q_recv, lin.at[1]), weights[2]]
        for i, (axis, src, dst) in enumerate((('z', qsl_next, q_sl), ('y', hsl_next, h_sl))):
            for k in range(1, grid):
                part = rows_at(here.step(axis, k) * rows, rows, 16)
                loads.append(pltpu.make_async_copy(src.at[part, :], dst.at[part, :], lin.at[2 + i * grid + k]))
        for c in loads:
            c.start()
        here.barrier()
        back = list(zip(carry, carry_out))
        spread_unit = Spread(here, done_h, all_h, sp_s, sp_r)
        own_unit = pltpu.make_async_copy(done_h, all_h.at[here.dp], lin.at[1])
        spread_unit.send(0)

        def back_copy(j, k):
            src, dst = back[j]
            return remote(src_ref=src.at[block(here.ep_to(k)), :], dst_ref=dst.at[block(ep), :],
                          send_sem=ba_s.at[j, k], recv_sem=ba_r.at[j, k], device_id=(here.dp, here.ep_to(k)))

        def back_own(j):
            src, dst = back[j]
            return pltpu.make_async_copy(src.at[block(ep), :], dst.at[block(ep), :], ba_l.at[j])

        def send_back(j):
            for k in range(n_peer):
                back_copy(j, k).start()
            back_own(j).start()

        for j in range(len(carry)):
            send_back(j)
        make_eye()
        for c in loads:
            c.wait()
        own_unit.start()
        own_slice('y', h_recv, h_sl)
        own_slice('z', q_recv, q_sl)

    forward_pass()
    share_t(0, 0).start()
    share_t(1, 0).start()
    if not first:
        spread_unit.receive(0)
        spread_unit.send(1)
    backward_pass()
    share_t(2, 0).start()
    share_t(3, 0).start()
    untranspose(act, u_all, u_cols)
    share_on((0, 1))
    o_pass()
    o_out = pltpu.make_async_copy(o_v, o_h, loc.at[3])
    o_out.start()
    untranspose(act, da_all, g_cols)
    untranspose(act_b, db_all, g_cols)
    share_on((2, 3))
    dh_pass()
    dh_out = pltpu.make_async_copy(dh_v, dh_h, loc.at[4])
    dh_out.start()
    if first:
        forward_own(spread_next, (h_send_next, q_send_next))
        forward(later, spread_next, 0)
        for k in range(1, grid):
            slices('z', q_recv, q_sl, qs_s, qs_r, k).wait_recv()
    else:
        spread_unit.receive(1)
        spread_unit.send(2, (0,))
    share_done((0, 1))
    weight_grad(2, u_all, q_sl)
    reduce_start((2, 3))
    if first:
        for k in range(1, grid):
            slices('y', h_recv, h_sl, hs_s, hs_r, k).wait_recv()
    share_done((2,))
    weight_grad(0, da_all, h_sl)
    reduce_start((0,))
    share_done((3,))
    weight_grad(1, db_all, h_sl)
    reduce_start((1,))
    if first:
        for p in range(1, (n_peer + 1) // 2):
            forward(later, spread_next, p)
    else:
        spread_unit.send(2, (1,))
    reduce_on((2, 3))
    if first:
        for p in range((n_peer + 1) // 2, n_peer - 2):
            forward(later, spread_next, p)
    reduce_on((0, 1))
    if not first:
        spread_unit.send(2, (2, 3))
    if first:
        for p in range(max((n_peer + 1) // 2, n_peer - 2), n_peer):
            forward(later, spread_next, p)
    ends = reduce_end(2) + reduce_end(0) + reduce_end(1)

    for j in range(3):
        for g in range(4):
            share_t(g, j).wait_send()
        for r in range(4):
            reduce_copy(r, j).wait_send()
    if first:
        for k in range(1, grid):
            for axis, buf, sl, send, recv in spread:
                slices(axis, buf, sl, send, recv, k).wait_send()
            for axis, buf, sl, send, recv in spread_next:
                slices(axis, buf, sl, send, recv, k).wait()
        for k in range(n_peer):
            for what in later:
                copy_of(what, k).wait_send()
        for c in own_next:
            c.wait()
    else:
        for j in range(len(back)):
            for k in range(n_peer):
                back_copy(j, k).wait()
            back_own(j).wait()
        spread_unit.receive(2)
        for stage in range(3):
            spread_unit.sent(stage)
        own_unit.wait()
    for c in ends + [o_out, dh_out]:
        c.wait()


def expert_call(inputs, w_gate, w_up, w_down, expert, cap, grid):
    first = expert == 0
    d_model = w_gate.shape[2]
    ff = w_gate.shape[1]
    rows = inputs[0].shape[0]
    quarter, share = d_model // grid, ff // grid
    n_peer = rows // cap - 1
    chunk = min(1024, d_model)
    vmem, dma = pltpu.VMEM, pltpu.SemaphoreType.DMA
    hbm = pl.BlockSpec(memory_space=pl.ANY)
    row_block, slice_block = (rows, d_model), (grid * rows, quarter)
    scratch = [
        vmem(row_block, BF16), vmem(row_block, BF16),
        vmem((ff, d_model), BF16), vmem((ff, d_model), BF16), vmem((ff, d_model), BF16),
        vmem((ff, rows), F32), vmem((ff, rows), F32), vmem((ff, rows), F32),
        vmem((ff, grid * rows), BF16), vmem((ff, grid * rows), BF16), vmem((ff, grid * rows), BF16),
        vmem(slice_block, BF16), vmem(slice_block, BF16),
        vmem((3, ff, quarter), F32), vmem((3, 3, share, quarter), F32),
        vmem((rows, ff), BF16), vmem((rows, ff), BF16), vmem((rows, rows), BF16), dma((5 + 3 * UNITS,)),
    ] + [dma((grid,))] * 4 + [dma((4, 3))] * 4
    out = lambda shape, dtype=BF16: jax.ShapeDtypeStruct(shape, dtype)
    share_block = (UNITS, 3, share, quarter // UNITS)
    outs = [out(row_block), out(row_block), out(share_block, F32)]
    if first:
        sel_h, hidden, sel_q, pair, sel_h_next, sel_q_next = inputs
        scratch += [vmem(x.shape, BF16) for x in (sel_h, sel_q, sel_h_next, sel_q_next, hidden, pair)]
        scratch += [vmem(row_block, BF16)] * 4 + [dma((n_peer,))] * 8 + [dma((grid,))] * 4 + [dma((8,))]
        operands = (*inputs, w_gate, w_up, w_down)
        outs += [out(row_block), out(row_block), out(slice_block), out(slice_block)]
    else:
        h_next, q_next, hsl_next, qsl_next, *carry, done = inputs
        scratch += [vmem(row_block, BF16)] * 2 + [dma((2, n_peer)), dma((2, n_peer)), dma((2,)), dma((2 + 2 * grid,))]
        scratch += [dma((UNITS, 15)), dma((UNITS, 15))]
        operands = (h_next, q_next, hsl_next, qsl_next, w_gate, w_up, w_down, *carry, done)
        outs += [out(row_block), out(row_block), out((grid * grid,) + share_block, F32)]
    return pl.pallas_call(
        functools.partial(expert_kernel, (expert, grid, chunk, cap, first)),
        out_shape=tuple(outs), in_specs=[hbm] * len(operands), out_specs=(hbm,) * len(outs), scratch_shapes=scratch,
        compiler_params=pltpu.CompilerParams(collective_id=expert, has_side_effects=True, vmem_limit_bytes=63 * 2 ** 20),
        cost_estimate=pl.CostEstimate(flops=2 * rows * d_model * ff * 9, bytes_accessed=30_000_000, transcendentals=0),
    )(*operands)


def small_sum_kernel(grid, val, out, first, second, third, c_one, c_two, c_three, s_one, r_one, s_two, r_two, s_three, r_three, s_four, r_four):
    n_ep, _, width = first.shape
    here = Place(n_ep, grid)
    n_peer = len(here.offsets)
    ep = here.ep
    remote = functools.partial(pltpu.make_async_remote_copy, device_id_type=MESH_ID)
    here.barrier()

    def cols(e):
        return rows_at(e * width, width, 128)

    def scatter(k):
        to = here.ep_to(k)
        return remote(src_ref=val.at[:, cols(to)], dst_ref=first.at[ep], send_sem=s_one.at[k], recv_sem=r_one.at[k],
                      device_id=(here.dp, to))

    def along(axis, src, dst, send, recv, k):
        mine = here.y if axis == 'y' else here.z
        return remote(src_ref=src, dst_ref=dst.at[mine], send_sem=send.at[k], recv_sem=recv.at[k], device_id=here.device(axis, k))

    def gather(k):
        return remote(src_ref=c_three, dst_ref=out.at[:, cols(ep)], send_sem=s_four.at[k], recv_sem=r_four.at[k],
                      device_id=(here.dp, here.ep_to(k)))

    def add_up(ref, n):
        total = ref[0]
        for i in range(1, n):
            total = total + ref[i]
        return total

    for k in range(n_peer):
        scatter(k).start()
    first[ep] = val[:, cols(ep)]
    for k in range(n_peer):
        scatter(k).wait_recv()
    c_one[...] = add_up(first, n_ep)
    second[here.y] = c_one[...]
    for k in range(1, grid):
        along('y', c_one, second, s_two, r_two, k).start()
    for k in range(1, grid):
        along('y', c_one, second, s_two, r_two, k).wait_recv()
    c_two[...] = add_up(second, grid)
    third[here.z] = c_two[...]
    for k in range(1, grid):
        along('z', c_two, third, s_three, r_three, k).start()
    for k in range(1, grid):
        along('z', c_two, third, s_three, r_three, k).wait_recv()
    c_three[...] = add_up(third, grid)
    for k in range(n_peer):
        gather(k).start()
    out[:, cols(ep)] = c_three[...]
    for k in range(n_peer):
        gather(k).wait_recv()
    for k in range(n_peer):
        scatter(k).wait_send()
        gather(k).wait_send()
    for k in range(1, grid):
        along('y', c_one, second, s_two, r_two, k).wait_send()
        along('z', c_two, third, s_three, r_three, k).wait_send()


def small_sum(val, n_ep, grid, collective_id):
    rows, d_model = val.shape
    width = d_model // n_ep
    vmem, dma = pltpu.VMEM, pltpu.SemaphoreType.DMA
    return pl.pallas_call(
        functools.partial(small_sum_kernel, grid),
        out_shape=jax.ShapeDtypeStruct(val.shape, F32),
        in_specs=[pl.BlockSpec(memory_space=pltpu.VMEM)], out_specs=pl.BlockSpec(memory_space=pltpu.VMEM),
        scratch_shapes=[vmem((n_ep, rows, width), F32), vmem((grid, rows, width), F32), vmem((grid, rows, width), F32),
                        vmem((rows, width), F32), vmem((rows, width), F32), vmem((rows, width), F32),
                        dma((n_ep - 1,)), dma((n_ep - 1,)), dma((grid,)), dma((grid,)), dma((grid,)), dma((grid,)),
                        dma((n_ep - 1,)), dma((n_ep - 1,))],
        compiler_params=pltpu.CompilerParams(collective_id=collective_id, has_side_effects=True),
        name='small_sum',
    )(val)


def assemble_kernel(gate, up, down, *refs):
    outs = refs[-3:]
    grid, unit = gate.shape[1], gate.shape[-1]
    for c in range(grid):
        for i in range(UNITS):
            at = (c * UNITS + i) * unit
            outs[0][0, :, at:at + unit] = gate[0, c, i, 0]
            outs[1][0, :, at:at + unit] = up[0, c, i, 0]
            outs[2][0, :, at:at + unit] = down[c, 0, i, 0]


def assemble(gathered, expert, n_expert, into):
    grid, _, _, _, share, unit = gathered.shape
    cut = 2
    part = share // cut
    row_first = pl.BlockSpec((1, grid, UNITS, 1, part, unit), lambda r, h: (r, 0, 0, 0, h, 0))
    up_first = pl.BlockSpec((1, grid, UNITS, 1, part, unit), lambda r, h: (r, 0, 0, 1, h, 0))
    col_first = pl.BlockSpec((grid, 1, UNITS, 1, part, unit), lambda r, h: (0, r, 0, 2, h, 0))
    out_spec = pl.BlockSpec((1, part, grid * UNITS * unit), lambda r, h: (expert, r * cut + h, 0))
    whole = jax.ShapeDtypeStruct((n_expert, grid * share, grid * UNITS * unit), F32)
    return pl.pallas_call(
        assemble_kernel, grid=(grid, cut), out_shape=(whole,) * 3,
        in_specs=[row_first, up_first, col_first] + [pl.BlockSpec(memory_space=pl.ANY)] * len(into),
        out_specs=(out_spec,) * 3, input_output_aliases={3 + i: i for i in range(len(into))},
        compiler_params=pltpu.CompilerParams(vmem_limit_bytes=40 * 2 ** 20),
        cost_estimate=pl.CostEstimate(flops=1_000_000, bytes_accessed=44_000_000, transcendentals=0),
    )(gathered, gathered, gathered, *into)


def solution(mesh):
    n_ep = mesh.shape['ep']
    grid = round(mesh.shape['dp'] ** 0.5)
    tok_spec = P(('dp', 'ep'), None)
    row_spec = P(('dp', 'ep'))
    exp_spec = P('ep', None, None)

    def local_step(tok_x, tok_dy, exp_first, exp_second, eligible, slot_first, slot_second,
                   ln_weight, ln_bias, router, w_gate, w_up, w_down):
        n_local, d_model = tok_x.shape
        n_exp = eligible.shape[1]
        local_exp = w_gate.shape[0]
        slot_cap = 3 * n_local // n_exp
        hidden, x_hat, inv_std = layer_norm(tok_x, ln_weight, ln_bias)
        logits = jnp.dot(hidden, router, preferred_element_type=F32)
        expert_ids = jnp.arange(n_exp)
        allowed = eligible > 0
        gate_one, prob_one, pick_one = masked_gate(logits, allowed, exp_first)
        gate_two, prob_two, pick_two = masked_gate(logits, allowed & (expert_ids[None, :] != exp_first[:, None]), exp_second)
        per = n_ep * slot_cap
        row_ids = jnp.arange(n_exp * slot_cap)

        def place(expert, slot):
            pos = (expert % local_exp) * per + (expert // local_exp) * slot_cap + slot
            return jnp.where(slot >= 0, pos, -1)

        pos_one = place(exp_first, slot_first)
        pos_two = place(exp_second, slot_second)
        sel_one = (pos_one[:, None] == row_ids[None, :]).astype(BF16)
        sel_two = (pos_two[:, None] == row_ids[None, :]).astype(BF16)
        sel_both = sel_one + sel_two
        dy_float = tok_dy.astype(F32)
        grad_one = (gate_one[:, None] * dy_float).astype(BF16)
        grad_two = (gate_two[:, None] * dy_float).astype(BF16)
        pair = jnp.concatenate([grad_one, grad_two], axis=0)
        pos_pair = jnp.concatenate([pos_one, pos_two])
        wg_t, wu_t = jnp.swapaxes(w_gate, 1, 2), jnp.swapaxes(w_up, 1, 2)
        cuts = [slice(e * per, (e + 1) * per) for e in range(local_exp)]
        sels = []
        for e in range(local_exp):
            ids = row_ids[cuts[e]][:, None]
            sels.append(jnp.logical_or(ids == pos_one[None, :], ids == pos_two[None, :]).astype(BF16))
            sels.append((ids == pos_pair[None, :]).astype(BF16))
        o, dh, share, *landed = expert_call((sels[0], hidden, sels[1], pair, sels[2], sels[3]), wg_t, wu_t, w_down, 0, slot_cap, grid)
        o_next, dh_next, share, o, dh, held = expert_call((*landed, o, dh, share), wg_t, wu_t, w_down, 1, slot_cap, grid)
        gathered_next = lax.all_gather(share, 'dp')
        held, o_next, dh_next = spread_call(held, o_next, dh_next, slot_cap, grid, local_exp + 1)
        gathered = [x.reshape((grid, grid) + share.shape) for x in (held, gathered_next)]
        outs, grads = [o, o_next], [dh, dh_next]
        sel_cat = [sel_one, sel_two]
        out_one, out_two = [sum(jnp.dot(s[:, c], o, preferred_element_type=F32) for c, o in zip(cuts, outs)) for s in sel_cat]
        y_mix = gate_one[:, None] * out_one + gate_two[:, None] * out_two
        out_tok = (tok_x.astype(F32) + y_mix).astype(BF16)
        grad_exp = sum(jnp.dot(sel_both[:, c], g, preferred_element_type=F32) for c, g in zip(cuts, grads))
        dgate_one = jnp.sum(dy_float * out_one, axis=-1)
        dgate_two = jnp.sum(dy_float * out_two, axis=-1)
        d_logits = ((dgate_one * gate_one)[:, None] * (pick_one - prob_one)
                    + (dgate_two * gate_two)[:, None] * (pick_two - prob_two)).astype(BF16)
        d_router = jnp.einsum('te,td->ed', d_logits, hidden, preferred_element_type=F32)
        grad_h = jnp.einsum('te,de->td', d_logits, router, preferred_element_type=F32) + grad_exp
        d_ln_weight = jnp.sum(grad_h * x_hat, axis=0)
        d_ln_bias = jnp.sum(grad_h, axis=0)
        dx_tok = (dy_float + layer_norm_back(grad_h, x_hat, inv_std, ln_weight)).astype(BF16)
        small = jnp.concatenate([d_router, d_ln_weight[None], d_ln_bias[None], jnp.zeros((6, d_model), F32)], axis=0)
        small = small_sum(small, n_ep, grid, local_exp)
        d_router, d_ln_weight, d_ln_bias = small[:n_exp].T, small[n_exp], small[n_exp + 1]

        weights = ()
        for e in range(local_exp):
            weights = assemble(gathered[e], e, local_exp, weights)
        dw_gate, dw_up, dw_down = jnp.swapaxes(weights[0], 1, 2), jnp.swapaxes(weights[1], 1, 2), weights[2]
        return out_tok, dx_tok, dw_gate, dw_up, dw_down, d_router, d_ln_weight, d_ln_bias

    return jax.shard_map(
        local_step, mesh=mesh,
        in_specs=(tok_spec, tok_spec, row_spec, row_spec, tok_spec, row_spec, row_spec,
                  P(), P(), P(), exp_spec, exp_spec, exp_spec),
        out_specs=(tok_spec, tok_spec, exp_spec, exp_spec, exp_spec, P(), P(), P()),
        check_vma=False)
```

```python
import functools

import jax
import jax.numpy as jnp
from jax import lax
from jax.experimental import pallas as pl
from jax.experimental.pallas import tpu as pltpu
from jax.sharding import PartitionSpec as P


LN_EPS = 1e-5
CORES = 2
UNITS = 4
F32 = jnp.float32
BF16 = jnp.bfloat16
MESH_ID = pl.DeviceIdType.MESH
NT = (((1,), (1,)), ((), ()))


def layer_norm(x_rows, ln_weight, ln_bias):
    x_float = x_rows.astype(F32)
    centered = x_float - jnp.mean(x_float, axis=-1, keepdims=True)
    inv_std = lax.rsqrt(jnp.mean(centered * centered, axis=-1, keepdims=True) + LN_EPS)
    x_hat = centered * inv_std
    hidden = (x_hat * ln_weight.astype(F32) + ln_bias.astype(F32)).astype(BF16)
    return hidden, jnp.mean(x_float, axis=-1, keepdims=True), inv_std


def masked_gate(logits, allowed, choice):
    expert_ids = jnp.arange(logits.shape[-1])
    prob_all = jax.nn.softmax(jnp.where(allowed, logits, -1e30), axis=-1)
    picked = (choice[:, None] == expert_ids[None, :]).astype(F32)
    return jnp.sum(prob_all * picked, axis=-1), prob_all, picked


def ring_offsets(n_x):
    near = [d for d in (1, n_x - 1) if 0 < d < n_x]
    near = list(dict.fromkeys(near))
    far = [d for d in range(2, n_x - 1)]
    out = [(0, 1)]
    for group in (near, far):
        for core in range(CORES):
            out += [(d, core) for d in group]
    return out


class Place:
    def __init__(self, n_ep, grid):
        self.n_x, self.grid = n_ep // CORES, grid
        self.ep, self.dp = lax.axis_index('ep'), lax.axis_index('dp')
        self.x, self.core = self.ep // CORES, self.ep % CORES
        self.z, self.y = self.dp // grid, self.dp % grid
        self.offsets = ring_offsets(self.n_x)

    def ep_to(self, k):
        dx, dc = self.offsets[k]
        return lax.rem(self.x + dx, self.n_x) * CORES + lax.rem(self.core + dc, CORES)

    def ep_from(self, k):
        dx, dc = self.offsets[k]
        return lax.rem(self.x + (self.n_x - dx), self.n_x) * CORES + lax.rem(self.core + dc, CORES)

    def step(self, axis, k):
        here = self.y if axis == 'y' else self.z
        return lax.rem(here + k + self.grid, self.grid)

    def device(self, axis, k):
        if axis == 'y':
            return (self.z * self.grid + self.step('y', k), self.ep)
        return (self.step('z', k) * self.grid + self.y, self.ep)

    def flip(self, axis, bits):
        if axis == 'y':
            return (self.z * self.grid + (self.y ^ bits), self.ep)
        return ((self.z ^ bits) * self.grid + self.y, self.ep)

    def barrier(self):
        sem = pltpu.get_barrier_semaphore()
        peers = [(self.dp, self.ep_to(k)) for k in range(len(self.offsets))]
        for k in range(1, self.grid):
            peers += [self.device('y', k), self.device('z', k)]
        for peer in peers:
            pl.semaphore_signal(sem, inc=1, device_id=peer, device_id_type=MESH_ID)
        pl.semaphore_wait(sem, len(peers))


def rows_at(start, size, unit):
    return pl.ds(pl.multiple_of(start, unit), size)


class Spread:
    STAGES = ((0,), (1, 2), (3, 4, 5, 6), tuple(range(7, 15)))

    def __init__(self, here, own, held, send, recv):
        self.here, self.own, self.held, self.sems = here, own, held, (send, recv)

    def plan(self, unit, index):
        axes = ('y', 'z') if unit < UNITS // 2 else ('z', 'y')
        one, two = (1, 3) if unit % 2 == 0 else (3, 1)
        line = (0, one, two, one ^ two)
        if index < 1:
            return axes, (axes[0], one), (0, 0)
        if index < 3:
            return axes, (axes[0], two), (line[index - 1], 0)
        if index < 7:
            return axes, (axes[1], one), (line[index - 3], 0)
        return axes, (axes[1], two), (line[(index - 7) % 4], (0, one)[(index - 7) // 4])

    def copy(self, unit, index):
        axes, (axis, flip), offsets = self.plan(unit, index)
        at = dict(zip(axes, offsets))
        owner = (self.here.z ^ at['z']) * self.here.grid + (self.here.y ^ at['y'])
        held = self.held.at[owner, unit]
        source = self.own.at[unit] if self.own is not None and offsets == (0, 0) else held
        return pltpu.make_async_remote_copy(src_ref=source, dst_ref=held, send_sem=self.sems[0].at[unit, index],
                                            recv_sem=self.sems[1].at[unit, index], device_id=self.here.flip(axis, flip),
                                            device_id_type=MESH_ID)

    def each(self, stage, picks=None):
        ids = self.STAGES[stage]
        for index in ids if picks is None else [ids[p] for p in picks]:
            for unit in range(UNITS):
                yield self.copy(unit, index)

    def send(self, stage, picks=None):
        for c in self.each(stage, picks):
            c.start()

    def receive(self, stage):
        for c in self.each(stage):
            c.wait_recv()

    def sent(self, stage):
        for c in self.each(stage):
            c.wait_send()


def tail_kernel(grid, cap, *refs):
    refs = list(refs)
    take = lambda n: [refs.pop(0) for _ in range(n)]
    _, o_next_h, dh_next_h, x_h, dy_h, hid_h, o_h, dh_h, stats, err_one, err_two, places, lnw, router = take(14)
    held, out, dx, small = take(4)
    x_v, dy_v, hid_v, o_v, dh_v, sel_one, sel_two, grad_h, val = take(9)
    first, second, third, c_one, c_two, c_three = take(6)
    loc, sp_s, sp_r, ba_s, ba_r, s_one, r_one, s_two, r_two, s_three, r_three, s_four, r_four = take(13)
    n_tok, d_model = x_v.shape
    rows = o_next_h.shape[0]
    n_ep, _, width = first.shape
    wide = min(512, d_model)
    here = Place(n_ep, grid)
    n_peer = len(here.offsets)
    ep = here.ep
    remote = functools.partial(pltpu.make_async_remote_copy, device_id_type=MESH_ID)
    here.barrier()
    spread = Spread(here, None, held, sp_s, sp_r)
    spread.send(3)

    def block(e, base=0):
        return rows_at(base + e * cap, cap, 16)

    pairs = ((o_next_h, o_v), (dh_next_h, dh_v))

    def back(j, k):
        src, dst = pairs[j]
        return remote(src_ref=src.at[block(here.ep_to(k)), :], dst_ref=dst.at[block(ep, rows), :],
                      send_sem=ba_s.at[j, k], recv_sem=ba_r.at[j, k], device_id=(here.dp, here.ep_to(k)))

    own = [pltpu.make_async_copy(src.at[block(ep), :], dst.at[block(ep, rows), :], loc.at[j]) for j, (src, dst) in enumerate(pairs)]
    for j in range(2):
        for k in range(n_peer):
            back(j, k).start()
        own[j].start()
    home = pl.ds(0, rows)
    loads = [pltpu.make_async_copy(src, dst, loc.at[2 + i]) for i, (src, dst) in enumerate((
        (x_h, x_v), (dy_h, dy_v), (hid_h, hid_v), (o_h, o_v.at[home, :]), (dh_h, dh_v.at[home, :])))]
    for c in loads:
        c.start()
    slots = lax.broadcasted_iota(jnp.int32, (n_tok, 2 * rows), 1)
    sel_one[...] = (slots == places[:, 0:1]).astype(F32).astype(BF16)
    sel_two[...] = (slots == places[:, 1:2]).astype(F32).astype(BF16)
    gate_one, gate_two, mean, inv_std = [stats[:, i:i + 1] for i in range(4)]
    zero = jnp.zeros((n_tok, 1), F32)
    for c in loads:
        c.wait()
    own[0].wait()
    for k in range(n_peer):
        back(0, k).wait_recv()

    def mix(i, sums):
        cols = rows_at(i * wide, wide, 128)
        one = jnp.dot(sel_one[...], o_v[:, cols], preferred_element_type=F32)
        two = jnp.dot(sel_two[...], o_v[:, cols], preferred_element_type=F32)
        dy = dy_v[:, cols].astype(F32)
        out[:, cols] = (x_v[:, cols].astype(F32) + (gate_one * one + gate_two * two)).astype(BF16)
        return sums[0] + jnp.sum(dy * one, axis=1, keepdims=True), sums[1] + jnp.sum(dy * two, axis=1, keepdims=True)

    dgate_one, dgate_two = lax.fori_loop(0, d_model // wide, mix, (zero, zero))
    d_logits = ((dgate_one * gate_one) * err_one[...] + (dgate_two * gate_two) * err_two[...]).astype(BF16)
    lanes = d_logits.shape[1]
    eye = (lax.broadcasted_iota(jnp.int32, (lanes, lanes), 0)
           == lax.broadcasted_iota(jnp.int32, (lanes, lanes), 1)).astype(F32).astype(BF16)
    d_logits_t = lax.dot_general(eye, d_logits, NT, preferred_element_type=F32).astype(BF16)[:16]
    sel_both = sel_one[...] + sel_two[...]
    row = lax.broadcasted_iota(jnp.int32, (8, wide), 0)
    own[1].wait()
    for k in range(n_peer):
        back(1, k).wait_recv()

    def gradient(i, sums):
        cols = rows_at(i * wide, wide, 128)
        grad = (jnp.dot(d_logits, router[:, cols], preferred_element_type=F32)
                + jnp.dot(sel_both, dh_v[:, cols], preferred_element_type=F32))
        x_hat = (x_v[:, cols].astype(F32) - mean) * inv_std
        grad_h[:, cols] = grad
        val[0:16, cols] = jnp.dot(d_logits_t, hid_v[:, cols], preferred_element_type=F32)
        d_weight = jnp.sum(grad * x_hat, axis=0, keepdims=True)
        d_bias = jnp.sum(grad, axis=0, keepdims=True)
        val[16:24, cols] = jnp.where(row == 0, d_weight, jnp.where(row == 1, d_bias, 0.0))
        scaled = grad * lnw[:, cols]
        return sums[0] + jnp.sum(scaled, axis=1, keepdims=True), sums[1] + jnp.sum(scaled * x_hat, axis=1, keepdims=True)

    mean_one, mean_two = lax.fori_loop(0, d_model // wide, gradient, (zero, zero))
    mean_one, mean_two = mean_one / d_model, mean_two / d_model

    def part(e):
        return rows_at(e * width, width, 128)

    def scatter(k):
        to = here.ep_to(k)
        return remote(src_ref=val.at[:, part(to)], dst_ref=first.at[ep], send_sem=s_one.at[k], recv_sem=r_one.at[k],
                      device_id=(here.dp, to))

    def along(axis, src, dst, send, recv, k):
        mine = here.y if axis == 'y' else here.z
        return remote(src_ref=src, dst_ref=dst.at[mine], send_sem=send.at[k], recv_sem=recv.at[k], device_id=here.device(axis, k))

    def gather(k):
        return remote(src_ref=c_three, dst_ref=small.at[:, part(ep)], send_sem=s_four.at[k], recv_sem=r_four.at[k],
                      device_id=(here.dp, here.ep_to(k)))

    def add_up(ref, n):
        total = ref[0]
        for i in range(1, n):
            total = total + ref[i]
        return total

    for k in range(n_peer):
        scatter(k).start()
    first[ep] = val[:, part(ep)]

    @pl.loop(0, d_model // wide)
    def _(i):
        cols = rows_at(i * wide, wide, 128)
        x_hat = (x_v[:, cols].astype(F32) - mean) * inv_std
        step = inv_std * (grad_h[:, cols] * lnw[:, cols] - mean_one - x_hat * mean_two)
        dx[:, cols] = (dy_v[:, cols].astype(F32) + step).astype(BF16)

    for k in range(n_peer):
        scatter(k).wait_recv()
    c_one[...] = add_up(first, n_ep)
    second[here.y] = c_one[...]
    for k in range(1, grid):
        along('y', c_one, second, s_two, r_two, k).start()
    for k in range(1, grid):
        along('y', c_one, second, s_two, r_two, k).wait_recv()
    c_two[...] = add_up(second, grid)
    third[here.z] = c_two[...]
    for k in range(1, grid):
        along('z', c_two, third, s_three, r_three, k).start()
    for k in range(1, grid):
        along('z', c_two, third, s_three, r_three, k).wait_recv()
    c_three[...] = add_up(third, grid)
    for k in range(n_peer):
        gather(k).start()
    small[:, part(ep)] = c_three[...]
    for k in range(n_peer):
        gather(k).wait_recv()
    for k in range(n_peer):
        scatter(k).wait_send()
        gather(k).wait_send()
        back(0, k).wait_send()
        back(1, k).wait_send()
    for k in range(1, grid):
        along('y', c_one, second, s_two, r_two, k).wait_send()
        along('z', c_two, third, s_three, r_three, k).wait_send()
    spread.receive(3)
    spread.sent(3)


def tail_call(held, o_next, dh_next, tok_x, tok_dy, hidden, o, dh, stats, err_one, err_two, places, lnw, router, cap, grid, collective_id):
    vmem, dma = pltpu.VMEM, pltpu.SemaphoreType.DMA
    n_tok, d_model = tok_x.shape
    rows = o.shape[0]
    n_ep = rows // cap
    n_peer, width = n_ep - 1, d_model // n_ep
    hbm, on_chip = pl.BlockSpec(memory_space=pl.ANY), pl.BlockSpec(memory_space=pltpu.VMEM)
    tokens = jax.ShapeDtypeStruct((n_tok, d_model), BF16)
    peers, ring = dma((n_peer,)), dma((grid,))
    return pl.pallas_call(
        functools.partial(tail_kernel, grid, cap),
        out_shape=(jax.ShapeDtypeStruct(held.shape, F32), tokens, tokens, jax.ShapeDtypeStruct((24, d_model), F32)),
        in_specs=[hbm] * 8 + [on_chip] * 6, out_specs=(hbm, on_chip, on_chip, on_chip), input_output_aliases={0: 0},
        scratch_shapes=[vmem((n_tok, d_model), BF16)] * 3 + [vmem((2 * rows, d_model), BF16)] * 2
        + [vmem((n_tok, 2 * rows), BF16)] * 2 + [vmem((n_tok, d_model), F32), vmem((24, d_model), F32)]
        + [vmem((n_ep, 24, width), F32), vmem((grid, 24, width), F32), vmem((grid, 24, width), F32)] + [vmem((24, width), F32)] * 3
        + [dma((7,)), dma((UNITS, 15)), dma((UNITS, 15)), dma((2, n_peer)), dma((2, n_peer)),
           peers, peers, ring, ring, ring, ring, peers, peers],
        compiler_params=pltpu.CompilerParams(collective_id=collective_id, has_side_effects=True, vmem_limit_bytes=50 * 2 ** 20),
        cost_estimate=pl.CostEstimate(flops=10_000_000_000, bytes_accessed=30_000_000, transcendentals=0),
        name='tail',
    )(held, o_next, dh_next, tok_x, tok_dy, hidden, o, dh, stats, err_one, err_two, places, lnw, router)


def expert_kernel(dims, *refs):
    expert, grid, chunk, cap, first = dims
    refs = list(refs)
    take = lambda n: [refs.pop(0) for _ in range(n)]
    if first:
        sel_in, wg_h, wu_h, wd_h = take(7), *take(3)
        o_h, dh_h, sh_h, h_next, q_next, hsl_next, qsl_next = take(7)
    else:
        h_next, q_next, hsl_next, qsl_next, wg_h, wu_h, wd_h, *carry = take(9)
        done_h, = take(1)
        o_h, dh_h, sh_h, *carry_out = take(5)
        all_h, = take(1)
    h_recv, q_recv, wg, wu, wd, a_t, b_t, d_t, u_all, da_all, db_all, h_sl, q_sl, dw, rsb, act, act_b, eye = take(18)
    loc, hs_s, hs_r, qs_s, qs_r, ga_s, ga_r, rs_s, rs_r = take(9)
    if first:
        sel_h, sel_q, sel_h_next, sel_q_next, hidden, grad_one, grad_two, h_send, q_send, h_send_next, q_send_next = take(11)
        xh_s, xh_r, xq_s, xq_r, nh_s, nh_r, nq_s, nq_r, ns_h_s, ns_h_r, ns_q_s, ns_q_r, lin = take(13)
        o_v, dh_v = h_send, q_send
    else:
        o_v, dh_v = take(2)
        ba_s, ba_r, ba_l, lin, sp_s, sp_r = take(6)
    rows, d_model = h_recv.shape
    ff = wg.shape[0]
    quarter = d_model // grid
    share = ff // grid
    here = Place(rows // cap, grid)
    n_peer = len(here.offsets)
    ep = here.ep
    remote = functools.partial(pltpu.make_async_remote_copy, device_id_type=MESH_ID)
    wide = chunk // 2

    def spot(axis):
        return here.y if axis == 'y' else here.z

    def block(e):
        return rows_at(e * cap, cap, 16)

    weights = [pltpu.make_async_copy(src.at[expert], dst, loc.at[i]) for i, (src, dst) in enumerate(((wg_h, wg), (wu_h, wu), (wd_h, wd)))]

    def x_copy(src, dst, send, recv, k):
        return remote(src_ref=src.at[block(here.ep_to(k)), :], dst_ref=dst.at[block(ep), :],
                      send_sem=send.at[k], recv_sem=recv.at[k], device_id=(here.dp, here.ep_to(k)))

    def slice_copy(axis, buf, sl, send, recv, src_ep, k):
        return remote(src_ref=buf.at[block(src_ep), rows_at(here.step(axis, k) * quarter, quarter, 128)],
                      dst_ref=sl.at[rows_at(spot(axis) * rows + src_ep * cap, cap, 16), :],
                      send_sem=send.at[k], recv_sem=recv.at[k], device_id=here.device(axis, k))

    def slices(axis, buf, sl, send, recv, k):
        return remote(src_ref=buf.at[:, pl.ds(0, quarter)], dst_ref=sl.at[pl.ds(0, rows), :],
                      send_sem=send.at[k], recv_sem=recv.at[k], device_id=here.device(axis, k))

    half = ff // 2
    gathers = [(u_all, pl.ds(0, half), 'z', 1, 3), (u_all, pl.ds(half, half), 'z', 3, 1),
               (da_all, pl.ds(0, ff), 'y', 1, 3), (db_all, pl.ds(0, ff), 'y', 3, 1)]

    def share_t(g, j):
        ref, part, axis, one, two = gathers[g]
        flip = two if j else one
        owner = spot(axis) ^ (one if j == 2 else 0)
        view = ref.at[part, rows_at(owner * rows, rows, 128)]
        return remote(src_ref=view, dst_ref=view, send_sem=ga_s.at[g, j], recv_sem=ga_r.at[g, j], device_id=here.flip(axis, flip))

    def share_on(units):
        for g in units:
            share_t(g, 0).wait_recv()
            for j in (1, 2):
                share_t(g, j).start()

    def share_done(units):
        for g in units:
            for j in (1, 2):
                share_t(g, j).wait_recv()

    reduces = [(0, pl.ds(0, quarter), 'z', 1, 3), (1, pl.ds(0, quarter), 'z', 3, 1),
               (2, pl.ds(0, quarter // 2), 'y', 1, 3), (2, pl.ds(quarter // 2, quarter // 2), 'y', 3, 1)]

    def part_at(i):
        return rows_at(i * share, share, 8)

    def reduce_copy(r, j):
        t, cols, axis, one, two = reduces[r]
        here_at = spot(axis)
        flip, chunk_at = ((one, here_at ^ one), (one, here_at ^ one ^ two), (two, here_at ^ two))[j]
        return remote(src_ref=dw.at[t, part_at(chunk_at), cols], dst_ref=rsb.at[t, j, :, cols],
                      send_sem=rs_s.at[r, j], recv_sem=rs_r.at[r, j], device_id=here.flip(axis, flip))

    def reduce_start(units):
        for r in units:
            for j in (0, 1):
                reduce_copy(r, j).start()

    def reduce_on(units):
        for r in units:
            t, cols, axis, _, two = reduces[r]
            reduce_copy(r, 0).wait_recv()
            reduce_copy(r, 1).wait_recv()
            on = part_at(spot(axis) ^ two)
            dw[t, on, cols] = dw[t, on, cols] + rsb[t, 1, :, cols]
            reduce_copy(r, 2).start()

    def reduce_end(t):
        units = [r for r in range(len(reduces)) if reduces[r][0] == t]
        axis = reduces[units[0]][2]
        for r in units:
            reduce_copy(r, 2).wait_recv()
        rsb[t, 0] = dw[t, part_at(spot(axis)), :] + rsb[t, 0] + rsb[t, 2]
        unit = quarter // UNITS
        outs = [pltpu.make_async_copy(rsb.at[t, 0, :, pl.ds(i * unit, unit)], sh_h.at[i, t], loc.at[5 + t * UNITS + i]) for i in range(UNITS)]
        for c in outs:
            c.start()
        return outs

    def own_slice(axis, buf, sl):
        sl[rows_at(spot(axis) * rows, rows, 16), :] = buf[:, rows_at(spot(axis) * quarter, quarter, 128)]

    strip = ff // 7
    u_cols = rows_at(here.z * rows, rows, 128)
    g_cols = rows_at(here.y * rows, rows, 128)

    def forward_pass():
        a_t[...] = jnp.zeros_like(a_t)
        b_t[...] = jnp.zeros_like(b_t)

        @pl.loop(0, d_model // chunk)
        def _(i):
            cols = rows_at(i * chunk, chunk, 128)
            a_t[...] += lax.dot_general(wg[:, cols], h_recv[:, cols], NT, preferred_element_type=F32)
            b_t[...] += lax.dot_general(wu[:, cols], h_recv[:, cols], NT, preferred_element_type=F32)

        @pl.loop(0, 7)
        def _(i):
            r = rows_at(i * strip, strip, 16)
            a = a_t[r, :]
            u_all[r, u_cols] = (a * jax.nn.sigmoid(a) * b_t[r, :]).astype(BF16)

    def backward_pass():
        d_t[...] = jnp.zeros_like(d_t)

        @pl.loop(0, d_model // chunk)
        def _(i):
            cols = rows_at(i * chunk, chunk, 128)
            d_t[...] += lax.dot_general(wd[:, cols], q_recv[:, cols], NT, preferred_element_type=F32)

        @pl.loop(0, 7)
        def _(i):
            r = rows_at(i * strip, strip, 16)
            a, b, du = a_t[r, :], b_t[r, :], d_t[r, :]
            sig = jax.nn.sigmoid(a)
            silu = a * sig
            da_all[r, g_cols] = (du * b * sig * (1.0 + a * (1.0 - sig))).astype(BF16)
            db_all[r, g_cols] = (du * silu).astype(BF16)

    def untranspose(out, ref, cols):
        out[...] = lax.dot_general(eye[...], ref[:, cols], NT, preferred_element_type=F32).astype(BF16)

    def o_pass():
        @pl.loop(0, d_model // wide)
        def _(i):
            cols = rows_at(i * wide, wide, 128)
            o_v[:, cols] = jnp.dot(act[...], wd[:, cols], preferred_element_type=F32).astype(BF16)

    def dh_pass():
        @pl.loop(0, d_model // wide)
        def _(i):
            cols = rows_at(i * wide, wide, 128)
            dh_v[:, cols] = (jnp.dot(act[...], wg[:, cols], preferred_element_type=F32)
                             + jnp.dot(act_b[...], wu[:, cols], preferred_element_type=F32)).astype(BF16)

    def weight_grad(t, left, right):
        @pl.loop(0, quarter // wide)
        def _(i):
            cols = rows_at(i * wide, wide, 128)
            dw[t, :, cols] = jnp.dot(left[...], right[:, cols], preferred_element_type=F32)

    def make_eye():
        eye[...] = (lax.broadcasted_iota(jnp.int32, (rows, rows), 0)
                    == lax.broadcasted_iota(jnp.int32, (rows, rows), 1)).astype(F32).astype(BF16)

    if first:
        inputs = [pltpu.make_async_copy(src, dst, lin.at[i])
                  for i, (src, dst) in enumerate(zip(sel_in, (sel_h, hidden, sel_q, grad_one, grad_two, sel_h_next, sel_q_next)))]
        for c in inputs:
            c.start()
        here.barrier()
        for c in inputs:
            c.wait()

        def gather(sel, source, out, e):
            @pl.loop(0, d_model // chunk)
            def _(i):
                cols = rows_at(i * chunk, chunk, 128)
                total = jnp.dot(sel[block(e), :n_tok], source[0][:, cols], preferred_element_type=F32)
                for j in range(1, len(source)):
                    total += jnp.dot(sel[block(e), j * n_tok:(j + 1) * n_tok], source[j][:, cols], preferred_element_type=F32)
                out[block(e), cols] = total.astype(BF16)

        n_tok = hidden.shape[0]
        rows_h, rows_q = (hidden,), (grad_one, grad_two)
        now = ((sel_h, rows_h, h_send, h_recv, xh_s, xh_r), (sel_q, rows_q, q_send, q_recv, xq_s, xq_r))
        later = ((sel_h_next, rows_h, h_send_next, h_next, nh_s, nh_r), (sel_q_next, rows_q, q_send_next, q_next, nq_s, nq_r))

        def copy_of(what, k):
            _, _, out, recv_buf, send, recv = what
            return x_copy(out, recv_buf, send, recv, k)

        pending = []

        def dispatch(what, k):
            gather(what[0], what[1], what[2], here.ep_to(k))
            pending.append(copy_of(what, k))
            if len(pending) > 1:
                pending.pop(0).start()

        for k in range(n_peer):
            for what in now:
                dispatch(what, k)
        for what in now:
            gather(what[0], what[1], what[3], ep)
        while pending:
            pending.pop(0).start()
        for c in weights:
            c.start()
        make_eye()

        spread = (('y', h_recv, h_sl, hs_s, hs_r), ('z', q_recv, q_sl, qs_s, qs_r))
        spread_next = (('y', h_next, hsl_next, ns_h_s, ns_h_r), ('z', q_next, qsl_next, ns_q_s, ns_q_r))

        def forward_own(spread, bufs):
            for (axis, _, sl, send, recv), buf in zip(spread, bufs):
                for k in range(1, grid):
                    slice_copy(axis, buf, sl, send, recv, ep, k).start()

        def forward(group, spread, p):
            for what, (axis, buf, sl, send, recv) in zip(group, spread):
                copy_of(what, p).wait_recv()
                for k in range(1, grid):
                    slice_copy(axis, buf, sl, send, recv, here.ep_from(p), k).start()

        forward_own(spread, (h_recv, q_recv))
        for what in later:
            gather(what[0], what[1], what[2], ep)
        own_next = [pltpu.make_async_copy(what[2].at[block(ep), :], what[3].at[block(ep), :], lin.at[7 + i]) for i, what in enumerate(later)]
        for p in range(n_peer):
            forward(now, spread, p)
            for what in later:
                dispatch(what, p)
            if p == min(3, n_peer - 1):
                while pending:
                    pending.pop(0).start()
                forward_own(spread_next, (h_send_next, q_send_next))
                forward(later, spread_next, 0)
        while pending:
            pending.pop(0).start()
        for c in own_next:
            c.start()
        own_slice('y', h_recv, h_sl)
        own_slice('z', q_recv, q_sl)
        for c in weights:
            c.wait()
        for k in range(n_peer):
            for what in now:
                copy_of(what, k).wait_send()
    else:
        loads = [pltpu.make_async_copy(h_next, h_recv, lin.at[0]), weights[0], weights[1],
                 pltpu.make_async_copy(q_next, q_recv, lin.at[1]), weights[2]]
        for i, (axis, src, dst) in enumerate((('z', qsl_next, q_sl), ('y', hsl_next, h_sl))):
            for k in range(1, grid):
                part = rows_at(here.step(axis, k) * rows, rows, 16)
                loads.append(pltpu.make_async_copy(src.at[part, :], dst.at[part, :], lin.at[2 + i * grid + k]))
        for c in loads:
            c.start()
        here.barrier()
        back = list(zip(carry, carry_out))
        spread_unit = Spread(here, done_h, all_h, sp_s, sp_r)
        own_unit = pltpu.make_async_copy(done_h, all_h.at[here.dp], lin.at[1])
        spread_unit.send(0)

        def back_copy(j, k):
            src, dst = back[j]
            return remote(src_ref=src.at[block(here.ep_to(k)), :], dst_ref=dst.at[block(ep), :],
                          send_sem=ba_s.at[j, k], recv_sem=ba_r.at[j, k], device_id=(here.dp, here.ep_to(k)))

        def back_own(j):
            src, dst = back[j]
            return pltpu.make_async_copy(src.at[block(ep), :], dst.at[block(ep), :], ba_l.at[j])

        def send_back(j):
            for k in range(n_peer):
                back_copy(j, k).start()
            back_own(j).start()

        for j in range(len(carry)):
            send_back(j)
        make_eye()
        for c in loads:
            c.wait()
        own_unit.start()
        own_slice('y', h_recv, h_sl)
        own_slice('z', q_recv, q_sl)

    forward_pass()
    share_t(0, 0).start()
    share_t(1, 0).start()
    if not first:
        spread_unit.receive(0)
        spread_unit.send(1)
    backward_pass()
    share_t(2, 0).start()
    share_t(3, 0).start()
    untranspose(act, u_all, u_cols)
    share_on((0, 1))
    o_pass()
    o_out = pltpu.make_async_copy(o_v, o_h, loc.at[3])
    o_out.start()
    untranspose(act, da_all, g_cols)
    untranspose(act_b, db_all, g_cols)
    share_on((2, 3))
    dh_pass()
    dh_out = pltpu.make_async_copy(dh_v, dh_h, loc.at[4])
    dh_out.start()
    if first:
        for k in range(1, grid):
            slices('z', q_recv, q_sl, qs_s, qs_r, k).wait_recv()
    else:
        spread_unit.receive(1)
        spread_unit.send(2, (0,))
    share_done((0, 1))
    weight_grad(2, u_all, q_sl)
    reduce_start((2, 3))
    if first:
        for k in range(1, grid):
            slices('y', h_recv, h_sl, hs_s, hs_r, k).wait_recv()
    share_done((2,))
    weight_grad(0, da_all, h_sl)
    reduce_start((0,))
    share_done((3,))
    weight_grad(1, db_all, h_sl)
    reduce_start((1,))
    if first:
        for p in range(1, (n_peer + 1) // 2):
            forward(later, spread_next, p)
    else:
        spread_unit.send(2, (1,))
    reduce_on((2, 3))
    if first:
        for p in range((n_peer + 1) // 2, n_peer - 2):
            forward(later, spread_next, p)
    reduce_on((0, 1))
    if not first:
        spread_unit.send(2, (2, 3))
    if first:
        for p in range(max((n_peer + 1) // 2, n_peer - 2), n_peer):
            forward(later, spread_next, p)
    ends = reduce_end(2) + reduce_end(0) + reduce_end(1)

    for j in range(3):
        for g in range(4):
            share_t(g, j).wait_send()
        for r in range(4):
            reduce_copy(r, j).wait_send()
    if first:
        for k in range(1, grid):
            for axis, buf, sl, send, recv in spread:
                slices(axis, buf, sl, send, recv, k).wait_send()
            for axis, buf, sl, send, recv in spread_next:
                slices(axis, buf, sl, send, recv, k).wait()
        for k in range(n_peer):
            for what in later:
                copy_of(what, k).wait_send()
        for c in own_next:
            c.wait()
    else:
        for j in range(len(back)):
            for k in range(n_peer):
                back_copy(j, k).wait()
            back_own(j).wait()
        spread_unit.receive(2)
        for stage in range(3):
            spread_unit.sent(stage)
        own_unit.wait()
    for c in ends + [o_out, dh_out]:
        c.wait()


def expert_call(inputs, w_gate, w_up, w_down, expert, cap, grid):
    first = expert == 0
    d_model = w_gate.shape[2]
    ff = w_gate.shape[1]
    rows = inputs[0].shape[0]
    quarter, share = d_model // grid, ff // grid
    n_peer = rows // cap - 1
    chunk = min(1024, d_model)
    vmem, dma = pltpu.VMEM, pltpu.SemaphoreType.DMA
    hbm = pl.BlockSpec(memory_space=pl.ANY)
    row_block, slice_block = (rows, d_model), (grid * rows, quarter)
    scratch = [
        vmem(row_block, BF16), vmem(row_block, BF16),
        vmem((ff, d_model), BF16), vmem((ff, d_model), BF16), vmem((ff, d_model), BF16),
        vmem((ff, rows), F32), vmem((ff, rows), F32), vmem((ff, rows), F32),
        vmem((ff, grid * rows), BF16), vmem((ff, grid * rows), BF16), vmem((ff, grid * rows), BF16),
        vmem(slice_block, BF16), vmem(slice_block, BF16),
        vmem((3, ff, quarter), F32), vmem((3, 3, share, quarter), F32),
        vmem((rows, ff), BF16), vmem((rows, ff), BF16), vmem((rows, rows), BF16), dma((5 + 3 * UNITS,)),
    ] + [dma((grid,))] * 4 + [dma((4, 3))] * 4
    out = lambda shape, dtype=BF16: jax.ShapeDtypeStruct(shape, dtype)
    share_block = (UNITS, 3, share, quarter // UNITS)
    outs = [out(row_block), out(row_block), out(share_block, F32)]
    if first:
        sel_h, hidden, sel_q, grad_one, grad_two, sel_h_next, sel_q_next = inputs
        scratch += [vmem(x.shape, BF16) for x in (sel_h, sel_q, sel_h_next, sel_q_next, hidden, grad_one, grad_two)]
        scratch += [vmem(row_block, BF16)] * 4 + [dma((n_peer,))] * 8 + [dma((grid,))] * 4 + [dma((9,))]
        operands = (*inputs, w_gate, w_up, w_down)
        outs += [out(row_block), out(row_block), out(slice_block), out(slice_block)]
    else:
        h_next, q_next, hsl_next, qsl_next, *carry, done = inputs
        scratch += [vmem(row_block, BF16)] * 2 + [dma((2, n_peer)), dma((2, n_peer)), dma((2,)), dma((2 + 2 * grid,))]
        scratch += [dma((UNITS, 15)), dma((UNITS, 15))]
        operands = (h_next, q_next, hsl_next, qsl_next, w_gate, w_up, w_down, *carry, done)
        outs += [out(row_block), out(row_block), out((grid * grid,) + share_block, F32)]
    return pl.pallas_call(
        functools.partial(expert_kernel, (expert, grid, chunk, cap, first)),
        out_shape=tuple(outs), in_specs=[hbm] * len(operands), out_specs=(hbm,) * len(outs), scratch_shapes=scratch,
        compiler_params=pltpu.CompilerParams(collective_id=expert, has_side_effects=True, vmem_limit_bytes=63 * 2 ** 20),
        cost_estimate=pl.CostEstimate(flops=2 * rows * d_model * ff * 9, bytes_accessed=30_000_000, transcendentals=0),
    )(*operands)


def assemble_kernel(gate, up, down, *refs):
    n_pass = (len(refs) - 3) // 2 if len(refs) > 6 else 0
    outs = refs[-3 - n_pass:][:3]
    for j in range(n_pass):
        refs[-n_pass + j][...] = refs[j][...]
    grid, unit = gate.shape[1], gate.shape[-1]
    for c in range(grid):
        for i in range(UNITS):
            at = (c * UNITS + i) * unit
            outs[0][0, :, at:at + unit] = gate[0, c, i, 0]
            outs[1][0, :, at:at + unit] = up[0, c, i, 0]
            outs[2][0, :, at:at + unit] = down[c, 0, i, 0]


def assemble(gathered, expert, n_expert, into, through=()):
    grid, _, _, _, share, unit = gathered.shape
    cut = 2
    part = share // cut
    row_first = pl.BlockSpec((1, grid, UNITS, 1, part, unit), lambda r, h: (r, 0, 0, 0, h, 0))
    up_first = pl.BlockSpec((1, grid, UNITS, 1, part, unit), lambda r, h: (r, 0, 0, 1, h, 0))
    col_first = pl.BlockSpec((grid, 1, UNITS, 1, part, unit), lambda r, h: (0, r, 0, 2, h, 0))
    out_spec = pl.BlockSpec((1, part, grid * UNITS * unit), lambda r, h: (expert, r * cut + h, 0))
    whole = jax.ShapeDtypeStruct((n_expert, grid * share, grid * UNITS * unit), F32)
    strips = [pl.BlockSpec((x.shape[0] // (grid * cut), x.shape[1]), lambda r, h: (r * cut + h, 0)) for x in through]
    return pl.pallas_call(
        assemble_kernel, grid=(grid, cut), out_shape=(whole,) * 3 + tuple(jax.ShapeDtypeStruct(x.shape, x.dtype) for x in through),
        in_specs=[row_first, up_first, col_first] + strips + [pl.BlockSpec(memory_space=pl.ANY)] * len(into),
        out_specs=(out_spec,) * 3 + tuple(strips), input_output_aliases={3 + i: i for i in range(len(into))},
        compiler_params=pltpu.CompilerParams(vmem_limit_bytes=40 * 2 ** 20),
        cost_estimate=pl.CostEstimate(flops=1_000_000, bytes_accessed=44_000_000, transcendentals=0),
    )(gathered, gathered, gathered, *through, *into)


def solution(mesh):
    n_ep = mesh.shape['ep']
    grid = round(mesh.shape['dp'] ** 0.5)
    tok_spec = P(('dp', 'ep'), None)
    row_spec = P(('dp', 'ep'))
    exp_spec = P('ep', None, None)

    def local_step(tok_x, tok_dy, exp_first, exp_second, eligible, slot_first, slot_second,
                   ln_weight, ln_bias, router, w_gate, w_up, w_down):
        n_local, _ = tok_x.shape
        n_exp = eligible.shape[1]
        local_exp = w_gate.shape[0]
        slot_cap = 3 * n_local // n_exp
        hidden, mean, inv_std = layer_norm(tok_x, ln_weight, ln_bias)
        logits = jnp.dot(hidden, router, preferred_element_type=F32)
        expert_ids = jnp.arange(n_exp)
        allowed = eligible > 0
        gate_one, prob_one, pick_one = masked_gate(logits, allowed, exp_first)
        gate_two, prob_two, pick_two = masked_gate(logits, allowed & (expert_ids[None, :] != exp_first[:, None]), exp_second)
        per = n_ep * slot_cap
        row_ids = jnp.arange(n_exp * slot_cap)

        def place(expert, slot):
            pos = (expert % local_exp) * per + (expert // local_exp) * slot_cap + slot
            return jnp.where(slot >= 0, pos, -1)

        pos_one = place(exp_first, slot_first)
        pos_two = place(exp_second, slot_second)
        dy_float = tok_dy.astype(F32)
        grad_one = (gate_one[:, None] * dy_float).astype(BF16)
        grad_two = (gate_two[:, None] * dy_float).astype(BF16)
        pos_pair = jnp.concatenate([pos_one, pos_two])
        wg_t, wu_t = jnp.swapaxes(w_gate, 1, 2), jnp.swapaxes(w_up, 1, 2)

        def lanes(columns):
            flat = jnp.concatenate(columns, axis=1)
            return jnp.pad(flat, ((0, 0), (0, 128 - flat.shape[1])))

        stats = lanes([gate_one[:, None], gate_two[:, None], mean, inv_std])
        err_one, err_two = lanes([pick_one - prob_one]), lanes([pick_two - prob_two])
        places = lanes([pos_one[:, None], pos_two[:, None]])
        router_t = jnp.pad(router.T, ((0, 128 - n_exp), (0, 0)))
        cuts = [slice(e * per, (e + 1) * per) for e in range(local_exp)]
        sels = []
        for e in range(local_exp):
            ids = row_ids[cuts[e]][:, None]
            sels.append(jnp.logical_or(ids == pos_one[None, :], ids == pos_two[None, :]).astype(BF16))
            sels.append((ids == pos_pair[None, :]).astype(BF16))
        o, dh, share, *landed = expert_call((sels[0], hidden, sels[1], grad_one, grad_two, sels[2], sels[3]), wg_t, wu_t, w_down, 0, slot_cap, grid)
        o_next, dh_next, share, o, dh, held = expert_call((*landed, o, dh, share), wg_t, wu_t, w_down, 1, slot_cap, grid)
        gathered_next = lax.all_gather(share, 'dp')
        held, out_tok, dx_tok, small = tail_call(
            held, o_next, dh_next, tok_x, tok_dy, hidden, o, dh, stats, err_one, err_two, places,
            ln_weight.astype(F32)[None], router_t, slot_cap, grid, local_exp + 1)
        gathered = [x.reshape((grid, grid) + share.shape) for x in (held, gathered_next)]
        d_router, d_ln_weight, d_ln_bias = small[:n_exp].T, small[16], small[17]
        *weights, out_tok, dx_tok = assemble(gathered[0], 0, local_exp, (), (out_tok, dx_tok))
        weights = assemble(gathered[1], 1, local_exp, weights)
        dw_gate, dw_up, dw_down = jnp.swapaxes(weights[0], 1, 2), jnp.swapaxes(weights[1], 1, 2), weights[2]
        return out_tok, dx_tok, dw_gate, dw_up, dw_down, d_router, d_ln_weight, d_ln_bias

    return jax.shard_map(
        local_step, mesh=mesh,
        in_specs=(tok_spec, tok_spec, row_spec, row_spec, tok_spec, row_spec, row_spec,
                  P(), P(), P(), exp_spec, exp_spec, exp_spec),
        out_specs=(tok_spec, tok_spec, exp_spec, exp_spec, exp_spec, P(), P(), P()),
        check_vma=False)
```

```python
import functools

import jax
import jax.numpy as jnp
from jax import lax
from jax.experimental import pallas as pl
from jax.experimental.pallas import tpu as pltpu
from jax.sharding import PartitionSpec as P


LN_EPS = 1e-5
CORES = 2
UNITS = 4
NEAR, FAR = (1, 3), (3, 1)
LANES = 128
PACK = 16
SMALL = 24
STREAM = 30_000_000
KEEP = {'keepdims': True}
F32 = jnp.float32
BF16 = jnp.bfloat16
ALL = Ellipsis
MESH_ID = pl.DeviceIdType.MESH
NT = (((1,), (1,)), ((), ()))


def layer_norm(x_rows, ln_weight, ln_bias):
    x_float = x_rows.astype(F32)
    centered = x_float - jnp.mean(x_float, axis=-1, **KEEP)
    inv_std = lax.rsqrt(jnp.mean(centered * centered, axis=-1, **KEEP) + LN_EPS)
    x_hat = centered * inv_std
    hidden = (x_hat * ln_weight.astype(F32) + ln_bias.astype(F32)).astype(BF16)
    return hidden, jnp.mean(x_float, axis=-1, **KEEP), inv_std


def masked_gate(logits, allowed, choice):
    expert_ids = jnp.arange(logits.shape[-1])
    prob_all = jax.nn.softmax(jnp.where(allowed, logits, -1e30), axis=-1)
    picked = (choice[:, None] == expert_ids[None, :]).astype(F32)
    return jnp.sum(prob_all * picked, axis=-1), prob_all, picked


def ring_offsets(n_x):
    near = [d for d in (1, n_x - 1) if 0 < d < n_x]
    near = list(dict.fromkeys(near))
    far = [d for d in range(2, n_x - 1)]
    out = [(0, 1)]
    for group in (near, far):
        for core in range(CORES):
            out += [(d, core) for d in group]
    return out


class Place:
    def __init__(self, n_ep, grid):
        self.n_x, self.grid = n_ep // CORES, grid
        self.ep, self.dp = lax.axis_index('ep'), lax.axis_index('dp')
        self.x, self.core = self.ep // CORES, self.ep % CORES
        self.z, self.y = self.dp // grid, self.dp % grid
        self.offsets = ring_offsets(self.n_x)

    def ep_to(self, k):
        dx, dc = self.offsets[k]
        return lax.rem(self.x + dx, self.n_x) * CORES + lax.rem(self.core + dc, CORES)

    def ep_from(self, k):
        dx, dc = self.offsets[k]
        return lax.rem(self.x + (self.n_x - dx), self.n_x) * CORES + lax.rem(self.core + dc, CORES)

    def step(self, axis, k):
        here = self.y if axis == 'y' else self.z
        return lax.rem(here + k + self.grid, self.grid)

    def device(self, axis, k):
        if axis == 'y':
            return (self.z * self.grid + self.step('y', k), self.ep)
        return (self.step('z', k) * self.grid + self.y, self.ep)

    def flip(self, axis, bits):
        if axis == 'y':
            return (self.z * self.grid + (self.y ^ bits), self.ep)
        return ((self.z ^ bits) * self.grid + self.y, self.ep)

    def arrive(self):
        sem = pltpu.get_barrier_semaphore()
        peers = [(self.dp, self.ep_to(k)) for k in range(len(self.offsets))]
        for k in range(1, self.grid):
            peers += [self.device('y', k), self.device('z', k)]
        for peer in peers:
            pl.semaphore_signal(sem, inc=1, device_id=peer, device_id_type=MESH_ID)
        return len(peers)

    def barrier(self, signals=None):
        pl.semaphore_wait(pltpu.get_barrier_semaphore(), self.arrive() if signals is None else signals)


def rows_at(start, size, unit):
    return pl.ds(pl.multiple_of(start, unit), size)


class Spread:
    STAGES = [range(2 ** i - 1, 2 ** (i + 1) - 1) for i in range(UNITS)]

    def __init__(self, here, own, held, send, recv):
        self.here, self.own, self.held, self.sems = here, own, held, (send, recv)

    def plan(self, unit, index):
        axes = ('y', 'z') if unit < UNITS // 2 else ('z', 'y')
        one, two = FAR if unit % 2 else NEAR
        line = (0, one, two, one ^ two)
        if index < 1:
            return axes, (axes[0], one), (0, 0)
        if index < 3:
            return axes, (axes[0], two), (line[index - 1], 0)
        if index < 7:
            return axes, (axes[1], one), (line[index - 3], 0)
        return axes, (axes[1], two), (line[(index - 7) % 4], (0, one)[(index - 7) // 4])

    def copy(self, unit, index):
        axes, (axis, flip), offsets = self.plan(unit, index)
        at = dict(zip(axes, offsets))
        owner = (self.here.z ^ at['z']) * self.here.grid + (self.here.y ^ at['y'])
        held = self.held.at[owner, unit]
        source = self.own.at[unit] if self.own is not None and offsets == (0, 0) else held
        return pltpu.make_async_remote_copy(src_ref=source, dst_ref=held, send_sem=self.sems[0].at[unit, index],
                                            recv_sem=self.sems[1].at[unit, index], device_id=self.here.flip(axis, flip),
                                            device_id_type=MESH_ID)

    def each(self, stage, picks=None):
        ids = self.STAGES[stage]
        for index in ids if picks is None else [ids[p] for p in picks]:
            for unit in range(UNITS):
                yield self.copy(unit, index)

    def send(self, stage, picks=None):
        for c in self.each(stage, picks):
            c.start()

    def receive(self, stage):
        for c in self.each(stage):
            c.wait_recv()

    def sent(self, stage):
        for c in self.each(stage):
            c.wait_send()


def tail_kernel(grid, cap, *refs):
    refs = list(refs)
    take = lambda n: [refs.pop(0) for _ in range(n)]
    _, o_next_h, dh_next_h, x_h, dy_h, hid_h, o_h, dh_h, stats, err_one, err_two, places, lnw, router = take(14)
    held, out, dx, small = take(4)
    x_v, dy_v, hid_v, o_v, dh_v, sel_one, sel_two, grad_h, val = take(9)
    first, second, third, c_one, c_two, c_three = take(6)
    loc, sp_s, sp_r, ba_s, ba_r, s_one, r_one, s_two, r_two, s_three, r_three, s_four, r_four = take(13)
    n_tok, d_model = x_v.shape
    rows = o_next_h.shape[0]
    n_ep, _, width = first.shape
    wide = min(512, d_model)
    here = Place(n_ep, grid)
    n_peer = len(here.offsets)
    ep = here.ep
    remote = functools.partial(pltpu.make_async_remote_copy, device_id_type=MESH_ID)
    here.barrier()
    spread = Spread(here, None, held, sp_s, sp_r)
    spread.send(3)

    def block(e, base=0):
        return rows_at(base + e * cap, cap, PACK)

    pairs = ((o_next_h, o_v), (dh_next_h, dh_v))

    def back(j, k):
        src, dst = pairs[j]
        return remote(src_ref=src.at[block(here.ep_to(k)), :], dst_ref=dst.at[block(ep, rows), :],
                      send_sem=ba_s.at[j, k], recv_sem=ba_r.at[j, k], device_id=(here.dp, here.ep_to(k)))

    own = [pltpu.make_async_copy(src.at[block(ep), :], dst.at[block(ep, rows), :], loc.at[j]) for j, (src, dst) in enumerate(pairs)]
    for j in range(2):
        for k in range(n_peer):
            back(j, k).start()
        own[j].start()
    home = pl.ds(0, rows)
    loads = [pltpu.make_async_copy(src, dst, loc.at[2 + i]) for i, (src, dst) in enumerate((
        (x_h, x_v), (dy_h, dy_v), (hid_h, hid_v), (o_h, o_v.at[home, :]), (dh_h, dh_v.at[home, :])))]
    for c in loads:
        c.start()
    slots = lax.broadcasted_iota(jnp.int32, (n_tok, 2 * rows), 1)
    sel_one[ALL] = (slots == places[:, 0:1]).astype(F32).astype(BF16)
    sel_two[ALL] = (slots == places[:, 1:2]).astype(F32).astype(BF16)
    gate_one, gate_two, mean, inv_std = [stats[:, i:i + 1] for i in range(4)]
    zero = jnp.zeros((n_tok, 1), F32)
    for c in loads:
        c.wait()
    own[0].wait()
    for k in range(n_peer):
        back(0, k).wait_recv()

    def mix(i, sums):
        cols = rows_at(i * wide, wide, LANES)
        one = jnp.dot(sel_one[ALL], o_v[:, cols], preferred_element_type=F32)
        two = jnp.dot(sel_two[ALL], o_v[:, cols], preferred_element_type=F32)
        dy = dy_v[:, cols].astype(F32)
        out[:, cols] = (x_v[:, cols].astype(F32) + (gate_one * one + gate_two * two)).astype(BF16)
        return sums[0] + jnp.sum(dy * one, axis=1, **KEEP), sums[1] + jnp.sum(dy * two, axis=1, **KEEP)

    dgate_one, dgate_two = lax.fori_loop(0, d_model // wide, mix, (zero, zero))
    d_logits = ((dgate_one * gate_one) * err_one[ALL] + (dgate_two * gate_two) * err_two[ALL]).astype(BF16)
    lanes = d_logits.shape[1]
    eye = (lax.broadcasted_iota(jnp.int32, (lanes, lanes), 0)
           == lax.broadcasted_iota(jnp.int32, (lanes, lanes), 1)).astype(F32).astype(BF16)
    d_logits_t = lax.dot_general(eye, d_logits, NT, preferred_element_type=F32).astype(BF16)[:16]
    sel_both = sel_one[ALL] + sel_two[ALL]
    row = lax.broadcasted_iota(jnp.int32, (8, wide), 0)
    own[1].wait()
    for k in range(n_peer):
        back(1, k).wait_recv()

    def gradient(i, sums):
        cols = rows_at(i * wide, wide, LANES)
        grad = (jnp.dot(d_logits, router[:, cols], preferred_element_type=F32)
                + jnp.dot(sel_both, dh_v[:, cols], preferred_element_type=F32))
        x_hat = (x_v[:, cols].astype(F32) - mean) * inv_std
        grad_h[:, cols] = grad
        val[0:16, cols] = jnp.dot(d_logits_t, hid_v[:, cols], preferred_element_type=F32)
        d_weight = jnp.sum(grad * x_hat, axis=0, **KEEP)
        d_bias = jnp.sum(grad, axis=0, **KEEP)
        val[16:SMALL, cols] = jnp.where(row == 0, d_weight, jnp.where(row == 1, d_bias, 0.0))
        scaled = grad * lnw[:, cols]
        return sums[0] + jnp.sum(scaled, axis=1, **KEEP), sums[1] + jnp.sum(scaled * x_hat, axis=1, **KEEP)

    mean_one, mean_two = lax.fori_loop(0, d_model // wide, gradient, (zero, zero))
    mean_one, mean_two = mean_one / d_model, mean_two / d_model

    def part(e):
        return rows_at(e * width, width, LANES)

    def scatter(k):
        to = here.ep_to(k)
        return remote(src_ref=val.at[:, part(to)], dst_ref=first.at[ep], send_sem=s_one.at[k], recv_sem=r_one.at[k],
                      device_id=(here.dp, to))

    def along(axis, src, dst, send, recv, k):
        mine = here.y if axis == 'y' else here.z
        return remote(src_ref=src, dst_ref=dst.at[mine], send_sem=send.at[k], recv_sem=recv.at[k], device_id=here.device(axis, k))

    def gather(k):
        return remote(src_ref=c_three, dst_ref=small.at[:, part(ep)], send_sem=s_four.at[k], recv_sem=r_four.at[k],
                      device_id=(here.dp, here.ep_to(k)))

    def add_up(ref, n):
        total = ref[0]
        for i in range(1, n):
            total = total + ref[i]
        return total

    for k in range(n_peer):
        scatter(k).start()
    first[ep] = val[:, part(ep)]

    @pl.loop(0, d_model // wide)
    def _(i):
        cols = rows_at(i * wide, wide, LANES)
        x_hat = (x_v[:, cols].astype(F32) - mean) * inv_std
        step = inv_std * (grad_h[:, cols] * lnw[:, cols] - mean_one - x_hat * mean_two)
        dx[:, cols] = (dy_v[:, cols].astype(F32) + step).astype(BF16)

    for k in range(n_peer):
        scatter(k).wait_recv()
    c_one[ALL] = add_up(first, n_ep)
    second[here.y] = c_one[ALL]
    for k in range(1, grid):
        along('y', c_one, second, s_two, r_two, k).start()
    for k in range(1, grid):
        along('y', c_one, second, s_two, r_two, k).wait_recv()
    c_two[ALL] = add_up(second, grid)
    third[here.z] = c_two[ALL]
    for k in range(1, grid):
        along('z', c_two, third, s_three, r_three, k).start()
    for k in range(1, grid):
        along('z', c_two, third, s_three, r_three, k).wait_recv()
    c_three[ALL] = add_up(third, grid)
    for k in range(n_peer):
        gather(k).start()
    small[:, part(ep)] = c_three[ALL]
    for k in range(n_peer):
        gather(k).wait_recv()
    for k in range(n_peer):
        scatter(k).wait_send()
        gather(k).wait_send()
        back(0, k).wait_send()
        back(1, k).wait_send()
    for k in range(1, grid):
        along('y', c_one, second, s_two, r_two, k).wait_send()
        along('z', c_two, third, s_three, r_three, k).wait_send()
    spread.receive(3)
    spread.sent(3)


def tail_call(held, o_next, dh_next, tok_x, tok_dy, hidden, o, dh, stats, err_one, err_two, places, lnw, router, cap, grid, collective_id):
    vmem, dma = pltpu.VMEM, pltpu.SemaphoreType.DMA
    n_tok, d_model = tok_x.shape
    rows = o.shape[0]
    n_ep = rows // cap
    n_peer, width = n_ep - 1, d_model // n_ep
    hbm, on_chip = pl.BlockSpec(memory_space=pl.ANY), pl.BlockSpec(memory_space=pltpu.VMEM)
    tokens = jax.ShapeDtypeStruct((n_tok, d_model), BF16)
    peers, ring = dma((n_peer,)), dma((grid,))
    return pl.pallas_call(
        functools.partial(tail_kernel, grid, cap),
        out_shape=(jax.ShapeDtypeStruct(held.shape, F32), tokens, tokens, jax.ShapeDtypeStruct((SMALL, d_model), F32)),
        in_specs=[hbm] * 8 + [on_chip] * 6, out_specs=(hbm, on_chip, on_chip, on_chip), input_output_aliases={0: 0},
        scratch_shapes=[vmem((n_tok, d_model), BF16)] * 3 + [vmem((2 * rows, d_model), BF16)] * 2
        + [vmem((n_tok, 2 * rows), BF16)] * 2 + [vmem((n_tok, d_model), F32), vmem((SMALL, d_model), F32)]
        + [vmem((n_ep, SMALL, width), F32), vmem((grid, SMALL, width), F32), vmem((grid, SMALL, width), F32)] + [vmem((SMALL, width), F32)] * 3
        + [dma((7,)), dma((UNITS, 15)), dma((UNITS, 15)), dma((2, n_peer)), dma((2, n_peer)),
           peers, peers, ring, ring, ring, ring, peers, peers],
        compiler_params=pltpu.CompilerParams(collective_id=collective_id, has_side_effects=True, vmem_limit_bytes=50 * 2 ** 20),
        cost_estimate=pl.CostEstimate(flops=10_000_000_000, bytes_accessed=STREAM, transcendentals=0),
        name='tail',
    )(held, o_next, dh_next, tok_x, tok_dy, hidden, o, dh, stats, err_one, err_two, places, lnw, router)


def expert_kernel(dims, *refs):
    expert, grid, chunk, cap, first = dims
    refs = list(refs)
    take = lambda n: [refs.pop(0) for _ in range(n)]
    if first:
        sel_in, wg_h, wu_h, wd_h = take(7), *take(3)
        o_h, dh_h, sh_h, h_next, q_next, hsl_next, qsl_next = take(7)
    else:
        h_next, q_next, hsl_next, qsl_next, wg_h, wu_h, wd_h, *carry = take(9)
        done_h, = take(1)
        o_h, dh_h, sh_h, *carry_out = take(5)
        all_h, = take(1)
    h_recv, q_recv, wg, wu, wd, a_t, b_t, d_t, u_all, da_all, db_all, h_sl, q_sl, dw, rsb, act, act_b, eye = take(18)
    loc, hs_s, hs_r, qs_s, qs_r, ga_s, ga_r, rs_s, rs_r = take(9)
    if first:
        sel_h, sel_q, sel_h_next, sel_q_next, hidden, grad_one, grad_two, h_send, q_send, h_send_next, q_send_next = take(11)
        xh_s, xh_r, xq_s, xq_r, nh_s, nh_r, nq_s, nq_r, ns_h_s, ns_h_r, ns_q_s, ns_q_r, lin = take(13)
        o_v, dh_v = h_send, q_send
    else:
        o_v, dh_v = take(2)
        ba_s, ba_r, ba_l, lin, sp_s, sp_r = take(6)
    rows, d_model = h_recv.shape
    ff = wg.shape[0]
    quarter = d_model // grid
    share = ff // grid
    here = Place(rows // cap, grid)
    n_peer = len(here.offsets)
    ep = here.ep
    remote = functools.partial(pltpu.make_async_remote_copy, device_id_type=MESH_ID)
    wide = chunk // 2

    def spot(axis):
        return here.y if axis == 'y' else here.z

    def block(e):
        return rows_at(e * cap, cap, PACK)

    weights = [pltpu.make_async_copy(src.at[expert], dst, loc.at[i]) for i, (src, dst) in enumerate(((wg_h, wg), (wu_h, wu), (wd_h, wd)))]

    def x_copy(src, dst, send, recv, k):
        return remote(src_ref=src.at[block(here.ep_to(k)), :], dst_ref=dst.at[block(ep), :],
                      send_sem=send.at[k], recv_sem=recv.at[k], device_id=(here.dp, here.ep_to(k)))

    def slice_copy(axis, buf, sl, send, recv, src_ep, k):
        return remote(src_ref=buf.at[block(src_ep), rows_at(here.step(axis, k) * quarter, quarter, LANES)],
                      dst_ref=sl.at[rows_at(spot(axis) * rows + src_ep * cap, cap, PACK), :],
                      send_sem=send.at[k], recv_sem=recv.at[k], device_id=here.device(axis, k))

    def slices(axis, buf, sl, send, recv, k):
        return remote(src_ref=buf.at[:, pl.ds(0, quarter)], dst_ref=sl.at[pl.ds(0, rows), :],
                      send_sem=send.at[k], recv_sem=recv.at[k], device_id=here.device(axis, k))

    half = ff // 2
    gathers = [(u_all, pl.ds(0, half), 'z', *NEAR), (u_all, pl.ds(half, half), 'z', *FAR),
               (da_all, pl.ds(0, ff), 'y', *NEAR), (db_all, pl.ds(0, ff), 'y', *FAR)]

    def share_t(g, j):
        ref, part, axis, one, two = gathers[g]
        flip = two if j else one
        owner = spot(axis) ^ (one if j == 2 else 0)
        view = ref.at[part, rows_at(owner * rows, rows, LANES)]
        return remote(src_ref=view, dst_ref=view, send_sem=ga_s.at[g, j], recv_sem=ga_r.at[g, j], device_id=here.flip(axis, flip))

    def share_on(units):
        for g in units:
            share_t(g, 0).wait_recv()
            for j in (1, 2):
                share_t(g, j).start()

    def share_done(units):
        for g in units:
            for j in (1, 2):
                share_t(g, j).wait_recv()

    reduces = [(0, pl.ds(0, quarter), 'z', *NEAR), (1, pl.ds(0, quarter), 'z', *FAR),
               (2, pl.ds(0, quarter // 2), 'y', *NEAR), (2, pl.ds(quarter // 2, quarter // 2), 'y', *FAR)]

    def part_at(i):
        return rows_at(i * share, share, 8)

    def reduce_copy(r, j):
        t, cols, axis, one, two = reduces[r]
        here_at = spot(axis)
        flip, chunk_at = ((one, here_at ^ one), (one, here_at ^ one ^ two), (two, here_at ^ two))[j]
        return remote(src_ref=dw.at[t, part_at(chunk_at), cols], dst_ref=rsb.at[t, j, :, cols],
                      send_sem=rs_s.at[r, j], recv_sem=rs_r.at[r, j], device_id=here.flip(axis, flip))

    def reduce_start(units):
        for r in units:
            for j in (0, 1):
                reduce_copy(r, j).start()

    def reduce_on(units):
        for r in units:
            t, cols, axis, _, two = reduces[r]
            reduce_copy(r, 0).wait_recv()
            reduce_copy(r, 1).wait_recv()
            on = part_at(spot(axis) ^ two)
            dw[t, on, cols] = dw[t, on, cols] + rsb[t, 1, :, cols]
            reduce_copy(r, 2).start()

    def reduce_end(t):
        units = [r for r in range(len(reduces)) if reduces[r][0] == t]
        axis = reduces[units[0]][2]
        for r in units:
            reduce_copy(r, 2).wait_recv()
        rsb[t, 0] = dw[t, part_at(spot(axis)), :] + rsb[t, 0] + rsb[t, 2]
        unit = quarter // UNITS
        outs = [pltpu.make_async_copy(rsb.at[t, 0, :, pl.ds(i * unit, unit)], sh_h.at[i, t], loc.at[5 + t * UNITS + i]) for i in range(UNITS)]
        for c in outs:
            c.start()
        return outs

    def own_slice(axis, buf, sl):
        sl[rows_at(spot(axis) * rows, rows, PACK), :] = buf[:, rows_at(spot(axis) * quarter, quarter, LANES)]

    strip = ff // 7
    u_cols = rows_at(here.z * rows, rows, LANES)
    g_cols = rows_at(here.y * rows, rows, LANES)

    def forward_pass():
        a_t[ALL] = jnp.zeros_like(a_t)
        b_t[ALL] = jnp.zeros_like(b_t)

        @pl.loop(0, d_model // chunk)
        def _(i):
            cols = rows_at(i * chunk, chunk, LANES)
            a_t[ALL] += lax.dot_general(wg[:, cols], h_recv[:, cols], NT, preferred_element_type=F32)
            b_t[ALL] += lax.dot_general(wu[:, cols], h_recv[:, cols], NT, preferred_element_type=F32)

        @pl.loop(0, 7)
        def _(i):
            r = rows_at(i * strip, strip, PACK)
            a = a_t[r, :]
            u_all[r, u_cols] = (a * jax.nn.sigmoid(a) * b_t[r, :]).astype(BF16)

    def backward_pass():
        d_t[ALL] = jnp.zeros_like(d_t)

        @pl.loop(0, d_model // chunk)
        def _(i):
            cols = rows_at(i * chunk, chunk, LANES)
            d_t[ALL] += lax.dot_general(wd[:, cols], q_recv[:, cols], NT, preferred_element_type=F32)

        @pl.loop(0, 7)
        def _(i):
            r = rows_at(i * strip, strip, PACK)
            a, b, du = a_t[r, :], b_t[r, :], d_t[r, :]
            sig = jax.nn.sigmoid(a)
            silu = a * sig
            da_all[r, g_cols] = (du * b * sig * (1.0 + a * (1.0 - sig))).astype(BF16)
            db_all[r, g_cols] = (du * silu).astype(BF16)

    def untranspose(out, ref, cols):
        out[ALL] = lax.dot_general(eye[ALL], ref[:, cols], NT, preferred_element_type=F32).astype(BF16)

    def o_pass():
        @pl.loop(0, d_model // wide)
        def _(i):
            cols = rows_at(i * wide, wide, LANES)
            o_v[:, cols] = jnp.dot(act[ALL], wd[:, cols], preferred_element_type=F32).astype(BF16)

    def dh_pass():
        @pl.loop(0, d_model // wide)
        def _(i):
            cols = rows_at(i * wide, wide, LANES)
            dh_v[:, cols] = (jnp.dot(act[ALL], wg[:, cols], preferred_element_type=F32)
                             + jnp.dot(act_b[ALL], wu[:, cols], preferred_element_type=F32)).astype(BF16)

    def weight_grad(t, left, right):
        @pl.loop(0, quarter // wide)
        def _(i):
            cols = rows_at(i * wide, wide, LANES)
            dw[t, :, cols] = jnp.dot(left[ALL], right[:, cols], preferred_element_type=F32)

    def forward_part():
        weights[0].wait()
        weights[1].wait()
        forward_pass()
        share_t(0, 0).start()
        share_t(1, 0).start()
        untranspose(act, u_all, u_cols)
        weights[2].wait()
        o_pass()
        o_out = pltpu.make_async_copy(o_v, o_h, loc.at[3])
        o_out.start()
        return o_out

    def make_eye():
        eye[ALL] = (lax.broadcasted_iota(jnp.int32, (rows, rows), 0)
                    == lax.broadcasted_iota(jnp.int32, (rows, rows), 1)).astype(F32).astype(BF16)

    if first:
        inputs = [pltpu.make_async_copy(src, dst, lin.at[i])
                  for i, (src, dst) in enumerate(zip(sel_in, (sel_h, hidden, sel_q, grad_one, grad_two, sel_h_next, sel_q_next)))]
        for c in inputs:
            c.start()
        signals = here.arrive()
        for c in inputs:
            c.wait()

        def gather(sel, source, out, e):
            @pl.loop(0, d_model // chunk)
            def _(i):
                cols = rows_at(i * chunk, chunk, LANES)
                total = jnp.dot(sel[block(e), :n_tok], source[0][:, cols], preferred_element_type=F32)
                for j in range(1, len(source)):
                    total += jnp.dot(sel[block(e), j * n_tok:(j + 1) * n_tok], source[j][:, cols], preferred_element_type=F32)
                out[block(e), cols] = total.astype(BF16)

        n_tok = hidden.shape[0]
        rows_h, rows_q = (hidden,), (grad_one, grad_two)
        now = ((sel_h, rows_h, h_send, h_recv, xh_s, xh_r), (sel_q, rows_q, q_send, q_recv, xq_s, xq_r))
        later = ((sel_h_next, rows_h, h_send_next, h_next, nh_s, nh_r), (sel_q_next, rows_q, q_send_next, q_next, nq_s, nq_r))

        def copy_of(what, k):
            _, _, out, recv_buf, send, recv = what
            return x_copy(out, recv_buf, send, recv, k)

        others = range(1, n_peer)
        pairs = list(zip(others[::2], others[1::2]))
        steps = [(group, i, ks) for group, order in ((now, (0, 1)), (later, (1, 0))) for i in order for ks in pairs]
        ahead = 2 * len(pairs)

        def gather_step(n):
            if n < len(steps):
                group, i, ks = steps[n]
                for k in ks:
                    gather(group[i][0], group[i][1], group[i][2], here.ep_to(k))

        def send_step(n):
            if n < len(steps):
                group, i, ks = steps[n]
                for k in ks:
                    copy_of(group[i], k).start()

        def sent_step(n):
            if n < len(steps):
                group, i, ks = steps[n]
                for k in ks:
                    copy_of(group[i], k).wait_send()

        def partner(group):
            for what in group:
                gather(what[0], what[1], what[2], here.ep_to(0))

        def partner_send(group):
            for what in group:
                copy_of(what, 0).start()

        gather_step(0)
        here.barrier(signals)
        send_step(0)
        gather_step(1)
        send_step(1)
        partner(now)
        partner_send(now)
        for c in weights:
            c.start()
        for what in now:
            gather(what[0], what[1], what[3], ep)
        make_eye()

        spread = (('y', h_recv, h_sl, hs_s, hs_r), ('z', q_recv, q_sl, qs_s, qs_r))
        spread_next = (('y', h_next, hsl_next, ns_h_s, ns_h_r), ('z', q_next, qsl_next, ns_q_s, ns_q_r))

        def forward_own(spread, bufs):
            for (axis, _, sl, send, recv), buf in zip(spread, bufs):
                for k in range(1, grid):
                    slice_copy(axis, buf, sl, send, recv, ep, k).start()

        def forward(group, spread, i, p):
            axis, buf, sl, send, recv = spread[i]
            copy_of(group[i], p).wait_recv()
            for k in range(1, grid):
                slice_copy(axis, buf, sl, send, recv, here.ep_from(p), k).start()

        def forward_step(n):
            if n < len(steps):
                group, i, ks = steps[n]
                for k in ks:
                    forward(group, spread if group is now else spread_next, i, k)

        forward_own(spread, (h_recv, q_recv))
        for i in range(2):
            forward(now, spread, i, 0)
        for what in later:
            gather(what[0], what[1], what[2], ep)
        own_next = [pltpu.make_async_copy(what[2].at[block(ep), :], what[3].at[block(ep), :], lin.at[7 + i]) for i, what in enumerate(later)]
        partner(later)
        partner_send(later)
        middle, last = max(len(pairs) - 1, 0), max(ahead - 1, 0)
        for n in range(last + 1):
            gather_step(n + 2)
            sent_step(n)
            send_step(n + 2)
            forward_step(n)
            if n == middle:
                own_slice('y', h_recv, h_sl)
                copy_of(now[0], 0).wait_send()
                o_out = forward_part()
            if n == min(middle + 2, last):
                share_on((0, 1))
            if n >= 2:
                gather_step(n + ahead)
            if n == min(1, last):
                forward_own(spread_next, (h_send_next, q_send_next))
                for i in range(2):
                    forward(later, spread_next, i, 0)
        send_step(ahead + 2)
        send_step(ahead + 3)
        for c in own_next:
            c.start()
        own_slice('z', q_recv, q_sl)
        copy_of(now[1], 0).wait_send()
    else:
        load_h, load_q = [pltpu.make_async_copy(src, dst, lin.at[2 + i * grid]) for i, (src, dst) in enumerate(((h_next, h_recv), (q_next, q_recv)))]
        load_slices = []
        for i, (axis, src, dst) in enumerate((('z', qsl_next, q_sl), ('y', hsl_next, h_sl))):
            for k in range(1, grid):
                part = rows_at(here.step(axis, k) * rows, rows, PACK)
                load_slices.append(pltpu.make_async_copy(src.at[part, :], dst.at[part, :], lin.at[2 + i * grid + k]))
        for c in [load_h] + weights + [load_q] + load_slices:
            c.start()
        here.barrier()
        back = list(zip(carry, carry_out))
        spread_unit = Spread(here, done_h, all_h, sp_s, sp_r)
        own_unit = pltpu.make_async_copy(done_h, all_h.at[here.dp], lin.at[1])
        spread_unit.send(0)

        def back_copy(j, k):
            src, dst = back[j]
            return remote(src_ref=src.at[block(here.ep_to(k)), :], dst_ref=dst.at[block(ep), :],
                          send_sem=ba_s.at[j, k], recv_sem=ba_r.at[j, k], device_id=(here.dp, here.ep_to(k)))

        def back_own(j):
            src, dst = back[j]
            return pltpu.make_async_copy(src.at[block(ep), :], dst.at[block(ep), :], ba_l.at[j])

        def send_back(j):
            for k in range(n_peer):
                back_copy(j, k).start()
            back_own(j).start()

        for j in range(len(carry)):
            send_back(j)
        make_eye()
        load_h.wait()
        o_out = forward_part()
        spread_unit.receive(0)
        spread_unit.send(1)
        load_q.wait()
        own_slice('y', h_recv, h_sl)
        own_slice('z', q_recv, q_sl)
        own_unit.start()

    backward_pass()
    share_t(2, 0).start()
    share_t(3, 0).start()
    if first:
        sent_step(ahead)
        send_step(ahead + 4)
    else:
        share_on((0, 1))
    untranspose(act, da_all, g_cols)
    untranspose(act_b, db_all, g_cols)
    share_on((2, 3))
    dh_pass()
    dh_out = pltpu.make_async_copy(dh_v, dh_h, loc.at[4])
    dh_out.start()
    if first:
        sent_step(ahead + 1)
        send_step(ahead + 5)
        forward_step(ahead)
        forward_step(ahead + 1)
        for k in range(1, grid):
            slices('z', q_recv, q_sl, qs_s, qs_r, k).wait_recv()
    else:
        spread_unit.receive(1)
        spread_unit.send(2, (0,))
        for c in load_slices:
            c.wait()
    share_done((0, 1))
    weight_grad(2, u_all, q_sl)
    reduce_start((2, 3))
    if first:
        for k in range(1, grid):
            slices('y', h_recv, h_sl, hs_s, hs_r, k).wait_recv()
    share_done((2,))
    weight_grad(0, da_all, h_sl)
    reduce_start((0,))
    share_done((3,))
    weight_grad(1, db_all, h_sl)
    reduce_start((1,))
    if first:
        forward_step(ahead + 2)
        forward_step(ahead + 3)
    else:
        spread_unit.send(2, (1,))
    reduce_on((2, 3))
    if first:
        forward_step(ahead + 4)
    reduce_on((0, 1))
    if first:
        forward_step(ahead + 5)
    else:
        spread_unit.send(2, (2, 3))
    ends = reduce_end(2) + reduce_end(0) + reduce_end(1)

    for j in range(3):
        for g in range(4):
            share_t(g, j).wait_send()
            reduce_copy(g, j).wait_send()
    if first:
        for k in range(1, grid):
            for axis, buf, sl, send, recv in spread:
                slices(axis, buf, sl, send, recv, k).wait_send()
            for axis, buf, sl, send, recv in spread_next:
                slices(axis, buf, sl, send, recv, k).wait()
        for what in later:
            copy_of(what, 0).wait_send()
        for n in range(2, 6):
            sent_step(ahead + n)
        for c in own_next:
            c.wait()
    else:
        for j in range(len(back)):
            for k in range(n_peer):
                back_copy(j, k).wait()
            back_own(j).wait()
        spread_unit.receive(2)
        for stage in range(3):
            spread_unit.sent(stage)
        own_unit.wait()
    for c in ends + [o_out, dh_out]:
        c.wait()


def expert_call(inputs, w_gate, w_up, w_down, expert, cap, grid):
    first = expert == 0
    d_model = w_gate.shape[2]
    ff = w_gate.shape[1]
    rows = inputs[0].shape[0]
    quarter, share = d_model // grid, ff // grid
    n_peer = rows // cap - 1
    chunk = min(1024, d_model)
    vmem, dma = pltpu.VMEM, pltpu.SemaphoreType.DMA
    hbm = pl.BlockSpec(memory_space=pl.ANY)
    row_block, slice_block = (rows, d_model), (grid * rows, quarter)
    scratch = [
        vmem(row_block, BF16), vmem(row_block, BF16),
        vmem((ff, d_model), BF16), vmem((ff, d_model), BF16), vmem((ff, d_model), BF16),
        vmem((ff, rows), F32), vmem((ff, rows), F32), vmem((ff, rows), F32),
        vmem((ff, grid * rows), BF16), vmem((ff, grid * rows), BF16), vmem((ff, grid * rows), BF16),
        vmem(slice_block, BF16), vmem(slice_block, BF16),
        vmem((3, ff, quarter), F32), vmem((3, 3, share, quarter), F32),
        vmem((rows, ff), BF16), vmem((rows, ff), BF16), vmem((rows, rows), BF16), dma((5 + 3 * UNITS,)),
    ] + [dma((grid,))] * 4 + [dma((4, 3))] * 4
    out = lambda shape, dtype=BF16: jax.ShapeDtypeStruct(shape, dtype)
    share_block = (UNITS, 3, share, quarter // UNITS)
    outs = [out(row_block), out(row_block), out(share_block, F32)]
    if first:
        sel_h, hidden, sel_q, grad_one, grad_two, sel_h_next, sel_q_next = inputs
        scratch += [vmem(x.shape, BF16) for x in (sel_h, sel_q, sel_h_next, sel_q_next, hidden, grad_one, grad_two)]
        scratch += [vmem(row_block, BF16)] * 4 + [dma((n_peer,))] * 8 + [dma((grid,))] * 4 + [dma((9,))]
        operands = (*inputs, w_gate, w_up, w_down)
        outs += [out(row_block), out(row_block), out(slice_block), out(slice_block)]
    else:
        h_next, q_next, hsl_next, qsl_next, *carry, done = inputs
        scratch += [vmem(row_block, BF16)] * 2 + [dma((2, n_peer)), dma((2, n_peer)), dma((2,)), dma((2 + 2 * grid,))]
        scratch += [dma((UNITS, 15)), dma((UNITS, 15))]
        operands = (h_next, q_next, hsl_next, qsl_next, w_gate, w_up, w_down, *carry, done)
        outs += [out(row_block), out(row_block), out((grid * grid,) + share_block, F32)]
    return pl.pallas_call(
        functools.partial(expert_kernel, (expert, grid, chunk, cap, first)),
        out_shape=tuple(outs), in_specs=[hbm] * len(operands), out_specs=(hbm,) * len(outs), scratch_shapes=scratch,
        compiler_params=pltpu.CompilerParams(collective_id=expert, has_side_effects=True, vmem_limit_bytes=63 * 2 ** 20),
        cost_estimate=pl.CostEstimate(flops=2 * rows * d_model * ff * 9, bytes_accessed=STREAM, transcendentals=0),
    )(*operands)


def assemble_kernel(gate, up, down, *refs):
    n_pass = (len(refs) - 3) // 2 if len(refs) > 6 else 0
    outs = refs[-3 - n_pass:][:3]
    for j in range(n_pass):
        refs[-n_pass + j][ALL] = refs[j][ALL]
    grid, unit = gate.shape[1], gate.shape[-1]
    for c in range(grid):
        for i in range(UNITS):
            at = (c * UNITS + i) * unit
            outs[0][0, :, at:at + unit] = gate[0, c, i, 0]
            outs[1][0, :, at:at + unit] = up[0, c, i, 0]
            outs[2][0, :, at:at + unit] = down[c, 0, i, 0]


def assemble(gathered, expert, n_expert, into, through=()):
    grid, _, _, _, share, unit = gathered.shape
    cut = 2
    part = share // cut
    row_first = pl.BlockSpec((1, grid, UNITS, 1, part, unit), lambda r, h: (r, 0, 0, 0, h, 0))
    up_first = pl.BlockSpec((1, grid, UNITS, 1, part, unit), lambda r, h: (r, 0, 0, 1, h, 0))
    col_first = pl.BlockSpec((grid, 1, UNITS, 1, part, unit), lambda r, h: (0, r, 0, 2, h, 0))
    out_spec = pl.BlockSpec((1, part, grid * UNITS * unit), lambda r, h: (expert, r * cut + h, 0))
    whole = jax.ShapeDtypeStruct((n_expert, grid * share, grid * UNITS * unit), F32)
    strips = [pl.BlockSpec((x.shape[0] // (grid * cut), x.shape[1]), lambda r, h: (r * cut + h, 0)) for x in through]
    return pl.pallas_call(
        assemble_kernel, grid=(grid, cut), out_shape=(whole,) * 3 + tuple(jax.ShapeDtypeStruct(x.shape, x.dtype) for x in through),
        in_specs=[row_first, up_first, col_first] + strips + [pl.BlockSpec(memory_space=pl.ANY)] * len(into),
        out_specs=(out_spec,) * 3 + tuple(strips), input_output_aliases={3 + i: i for i in range(len(into))},
        compiler_params=pltpu.CompilerParams(vmem_limit_bytes=40 * 2 ** 20),
        cost_estimate=pl.CostEstimate(flops=1_000_000, bytes_accessed=44_000_000, transcendentals=0),
    )(gathered, gathered, gathered, *through, *into)


def solution(mesh):
    n_ep = mesh.shape['ep']
    grid = round(mesh.shape['dp'] ** 0.5)
    tok_spec = P(('dp', 'ep'), None)
    row_spec = P(('dp', 'ep'))
    exp_spec = P('ep', None, None)

    def local_step(tok_x, tok_dy, exp_first, exp_second, eligible, slot_first, slot_second,
                   ln_weight, ln_bias, router, w_gate, w_up, w_down):
        n_local, _ = tok_x.shape
        n_exp = eligible.shape[1]
        local_exp = w_gate.shape[0]
        slot_cap = 3 * n_local // n_exp
        hidden, mean, inv_std = layer_norm(tok_x, ln_weight, ln_bias)
        logits = jnp.dot(hidden, router, preferred_element_type=F32)
        expert_ids = jnp.arange(n_exp)
        allowed = eligible > 0
        gate_one, prob_one, pick_one = masked_gate(logits, allowed, exp_first)
        gate_two, prob_two, pick_two = masked_gate(logits, allowed & (expert_ids[None, :] != exp_first[:, None]), exp_second)
        per = n_ep * slot_cap
        row_ids = jnp.arange(n_exp * slot_cap)

        def place(expert, slot):
            pos = (expert % local_exp) * per + (expert // local_exp) * slot_cap + slot
            return jnp.where(slot >= 0, pos, -1)

        pos_one = place(exp_first, slot_first)
        pos_two = place(exp_second, slot_second)
        dy_float = tok_dy.astype(F32)
        grad_one = (gate_one[:, None] * dy_float).astype(BF16)
        grad_two = (gate_two[:, None] * dy_float).astype(BF16)
        pos_pair = jnp.concatenate([pos_one, pos_two])
        wg_t, wu_t = jnp.swapaxes(w_gate, 1, 2), jnp.swapaxes(w_up, 1, 2)

        def lanes(columns):
            flat = jnp.concatenate(columns, axis=1)
            return jnp.pad(flat, ((0, 0), (0, LANES - flat.shape[1])))

        stats = lanes([gate_one[:, None], gate_two[:, None], mean, inv_std])
        err_one, err_two = lanes([pick_one - prob_one]), lanes([pick_two - prob_two])
        places = lanes([pos_one[:, None], pos_two[:, None]])
        router_t = jnp.pad(router.T, ((0, LANES - n_exp), (0, 0)))
        cuts = [slice(e * per, (e + 1) * per) for e in range(local_exp)]
        sels = []
        for e in range(local_exp):
            ids = row_ids[cuts[e]][:, None]
            sels.append(jnp.logical_or(ids == pos_one[None, :], ids == pos_two[None, :]).astype(BF16))
            sels.append((ids == pos_pair[None, :]).astype(BF16))
        o, dh, share, *landed = expert_call((sels[0], hidden, sels[1], grad_one, grad_two, sels[2], sels[3]), wg_t, wu_t, w_down, 0, slot_cap, grid)
        o_next, dh_next, share, o, dh, held = expert_call((*landed, o, dh, share), wg_t, wu_t, w_down, 1, slot_cap, grid)
        gathered_next = lax.all_gather(share, 'dp')
        held, out_tok, dx_tok, small = tail_call(
            held, o_next, dh_next, tok_x, tok_dy, hidden, o, dh, stats, err_one, err_two, places,
            ln_weight.astype(F32)[None], router_t, slot_cap, grid, local_exp + 1)
        gathered = [x.reshape((grid, grid) + share.shape) for x in (held, gathered_next)]
        d_router, d_ln_weight, d_ln_bias = small[:n_exp].T, small[16], small[17]
        *weights, out_tok, dx_tok = assemble(gathered[0], 0, local_exp, (), (out_tok, dx_tok))
        weights = assemble(gathered[1], 1, local_exp, weights)
        dw_gate, dw_up, dw_down = jnp.swapaxes(weights[0], 1, 2), jnp.swapaxes(weights[1], 1, 2), weights[2]
        return out_tok, dx_tok, dw_gate, dw_up, dw_down, d_router, d_ln_weight, d_ln_bias

    return jax.shard_map(
        local_step, mesh=mesh,
        in_specs=(tok_spec, tok_spec, row_spec, row_spec, tok_spec, row_spec, row_spec,
                  P(), P(), P(), exp_spec, exp_spec, exp_spec),
        out_specs=(tok_spec, tok_spec, exp_spec, exp_spec, exp_spec, P(), P(), P()),
        check_vma=False)
```

```python
import functools

import jax
import jax.numpy as jnp
from jax import lax
from jax.experimental import pallas as pl
from jax.experimental.pallas import tpu as pltpu
from jax.sharding import PartitionSpec as P


LN_EPS = 1e-5
CORES = 2
UNITS = 4
NEAR, FAR = (1, 3), (3, 1)
LANES = 128
PACK = 16
SMALL = 24
STREAM = 30_000_000
KEEP = {'keepdims': True}
F32 = jnp.float32
BF16 = jnp.bfloat16
ALL = Ellipsis
MESH_ID = pl.DeviceIdType.MESH
NT = (((1,), (1,)), ((), ()))


def layer_norm(x_rows, ln_weight, ln_bias):
    x_float = x_rows.astype(F32)
    centered = x_float - jnp.mean(x_float, axis=-1, **KEEP)
    inv_std = lax.rsqrt(jnp.mean(centered * centered, axis=-1, **KEEP) + LN_EPS)
    x_hat = centered * inv_std
    hidden = (x_hat * ln_weight.astype(F32) + ln_bias.astype(F32)).astype(BF16)
    return hidden, jnp.mean(x_float, axis=-1, **KEEP), inv_std


def masked_gate(logits, allowed, choice):
    expert_ids = jnp.arange(logits.shape[-1])
    prob_all = jax.nn.softmax(jnp.where(allowed, logits, -1e30), axis=-1)
    picked = (choice[:, None] == expert_ids[None, :]).astype(F32)
    return jnp.sum(prob_all * picked, axis=-1), prob_all, picked


def ring_offsets(n_x):
    near = [d for d in (1, n_x - 1) if 0 < d < n_x]
    near = list(dict.fromkeys(near))
    far = [d for d in range(2, n_x - 1)]
    out = [(0, 1)]
    for group in (near, far):
        for core in range(CORES):
            out += [(d, core) for d in group]
    return out


class Place:
    def __init__(self, n_ep, grid):
        self.n_x, self.grid = n_ep // CORES, grid
        self.ep, self.dp = lax.axis_index('ep'), lax.axis_index('dp')
        self.x, self.core = self.ep // CORES, self.ep % CORES
        self.z, self.y = self.dp // grid, self.dp % grid
        self.offsets = ring_offsets(self.n_x)

    def ep_to(self, k):
        dx, dc = self.offsets[k]
        return lax.rem(self.x + dx, self.n_x) * CORES + lax.rem(self.core + dc, CORES)

    def ep_from(self, k):
        dx, dc = self.offsets[k]
        return lax.rem(self.x + (self.n_x - dx), self.n_x) * CORES + lax.rem(self.core + dc, CORES)

    def step(self, axis, k):
        here = self.y if axis == 'y' else self.z
        return lax.rem(here + k + self.grid, self.grid)

    def device(self, axis, k):
        if axis == 'y':
            return (self.z * self.grid + self.step('y', k), self.ep)
        return (self.step('z', k) * self.grid + self.y, self.ep)

    def flip(self, axis, bits):
        if axis == 'y':
            return (self.z * self.grid + (self.y ^ bits), self.ep)
        return ((self.z ^ bits) * self.grid + self.y, self.ep)

    def arrive(self):
        sem = pltpu.get_barrier_semaphore()
        peers = [(self.dp, self.ep_to(k)) for k in range(len(self.offsets))]
        for k in range(1, self.grid):
            peers += [self.device('y', k), self.device('z', k)]
        for peer in peers:
            pl.semaphore_signal(sem, inc=1, device_id=peer, device_id_type=MESH_ID)
        return len(peers)

    def barrier(self, signals=None):
        pl.semaphore_wait(pltpu.get_barrier_semaphore(), self.arrive() if signals is None else signals)


def rows_at(start, size, unit):
    return pl.ds(pl.multiple_of(start, unit), size)


class Spread:
    STAGES = [range(2 ** i - 1, 2 ** (i + 1) - 1) for i in range(UNITS)]

    def __init__(self, here, own, held, send, recv):
        self.here, self.own, self.held, self.sems = here, own, held, (send, recv)

    def plan(self, unit, index):
        axes = ('y', 'z') if unit < UNITS // 2 else ('z', 'y')
        one, two = FAR if unit % 2 else NEAR
        line = (0, one, two, one ^ two)
        if index < 1:
            return axes, (axes[0], one), (0, 0)
        if index < 3:
            return axes, (axes[0], two), (line[index - 1], 0)
        if index < 7:
            return axes, (axes[1], one), (line[index - 3], 0)
        return axes, (axes[1], two), (line[(index - 7) % 4], (0, one)[(index - 7) // 4])

    def copy(self, unit, index):
        axes, (axis, flip), offsets = self.plan(unit, index)
        at = dict(zip(axes, offsets))
        owner = (self.here.z ^ at['z']) * self.here.grid + (self.here.y ^ at['y'])
        held = self.held.at[owner, unit]
        source = self.own.at[unit] if self.own is not None and offsets == (0, 0) else held
        return pltpu.make_async_remote_copy(src_ref=source, dst_ref=held, send_sem=self.sems[0].at[unit, index],
                                            recv_sem=self.sems[1].at[unit, index], device_id=self.here.flip(axis, flip),
                                            device_id_type=MESH_ID)

    def each(self, stage, picks=None):
        ids = self.STAGES[stage]
        for index in ids if picks is None else [ids[p] for p in picks]:
            for unit in range(UNITS):
                yield self.copy(unit, index)

    def send(self, stage, picks=None):
        for c in self.each(stage, picks):
            c.start()

    def receive(self, stage):
        for c in self.each(stage):
            c.wait_recv()

    def sent(self, stage):
        for c in self.each(stage):
            c.wait_send()


def tail_kernel(grid, cap, *refs):
    refs = list(refs)
    take = lambda n: [refs.pop(0) for _ in range(n)]
    _, o_next_h, dh_next_h, x_h, dy_h, hid_h, o_h, dh_h, stats, err_one, err_two, places, lnw, router = take(14)
    held, out, dx, small = take(4)
    x_v, dy_v, hid_v, o_v, dh_v, sel_one, sel_two, grad_h, val = take(9)
    first, second, third, c_one, c_two, c_three = take(6)
    loc, sp_s, sp_r, ba_s, ba_r, s_one, r_one, s_two, r_two, s_three, r_three, s_four, r_four = take(13)
    n_tok, d_model = x_v.shape
    rows = o_next_h.shape[0]
    n_ep, _, width = first.shape
    wide = min(512, d_model)
    here = Place(n_ep, grid)
    n_peer = len(here.offsets)
    ep = here.ep
    remote = functools.partial(pltpu.make_async_remote_copy, device_id_type=MESH_ID)
    here.barrier()
    spread = Spread(here, None, held, sp_s, sp_r)
    spread.send(3)

    def block(e, base=0):
        return rows_at(base + e * cap, cap, PACK)

    pairs = ((o_next_h, o_v), (dh_next_h, dh_v))

    def back(j, k):
        src, dst = pairs[j]
        return remote(src_ref=src.at[block(here.ep_to(k)), :], dst_ref=dst.at[block(ep, rows), :],
                      send_sem=ba_s.at[j, k], recv_sem=ba_r.at[j, k], device_id=(here.dp, here.ep_to(k)))

    own = [pltpu.make_async_copy(src.at[block(ep), :], dst.at[block(ep, rows), :], loc.at[j]) for j, (src, dst) in enumerate(pairs)]
    for j in range(2):
        for k in range(n_peer):
            back(j, k).start()
        own[j].start()
    home = pl.ds(0, rows)
    loads = [pltpu.make_async_copy(src, dst, loc.at[2 + i]) for i, (src, dst) in enumerate((
        (x_h, x_v), (dy_h, dy_v), (hid_h, hid_v), (o_h, o_v.at[home, :]), (dh_h, dh_v.at[home, :])))]
    for c in loads:
        c.start()
    slots = lax.broadcasted_iota(jnp.int32, (n_tok, 2 * rows), 1)
    sel_one[ALL] = (slots == places[:, 0:1]).astype(F32).astype(BF16)
    sel_two[ALL] = (slots == places[:, 1:2]).astype(F32).astype(BF16)
    gate_one, gate_two, mean, inv_std = [stats[:, i:i + 1] for i in range(4)]
    zero = jnp.zeros((n_tok, 1), F32)
    for c in loads:
        c.wait()
    own[0].wait()
    for k in range(n_peer):
        back(0, k).wait_recv()

    def mix(i, sums):
        cols = rows_at(i * wide, wide, LANES)
        one = jnp.dot(sel_one[ALL], o_v[:, cols], preferred_element_type=F32)
        two = jnp.dot(sel_two[ALL], o_v[:, cols], preferred_element_type=F32)
        dy = dy_v[:, cols].astype(F32)
        out[:, cols] = (x_v[:, cols].astype(F32) + (gate_one * one + gate_two * two)).astype(BF16)
        return sums[0] + jnp.sum(dy * one, axis=1, **KEEP), sums[1] + jnp.sum(dy * two, axis=1, **KEEP)

    dgate_one, dgate_two = lax.fori_loop(0, d_model // wide, mix, (zero, zero))
    d_logits = ((dgate_one * gate_one) * err_one[ALL] + (dgate_two * gate_two) * err_two[ALL]).astype(BF16)
    lanes = d_logits.shape[1]
    eye = (lax.broadcasted_iota(jnp.int32, (lanes, lanes), 0)
           == lax.broadcasted_iota(jnp.int32, (lanes, lanes), 1)).astype(F32).astype(BF16)
    d_logits_t = lax.dot_general(eye, d_logits, NT, preferred_element_type=F32).astype(BF16)[:16]
    sel_both = sel_one[ALL] + sel_two[ALL]
    row = lax.broadcasted_iota(jnp.int32, (8, wide), 0)
    own[1].wait()
    for k in range(n_peer):
        back(1, k).wait_recv()

    def gradient(i, sums):
        cols = rows_at(i * wide, wide, LANES)
        grad = (jnp.dot(d_logits, router[:, cols], preferred_element_type=F32)
                + jnp.dot(sel_both, dh_v[:, cols], preferred_element_type=F32))
        x_hat = (x_v[:, cols].astype(F32) - mean) * inv_std
        grad_h[:, cols] = grad
        val[0:16, cols] = jnp.dot(d_logits_t, hid_v[:, cols], preferred_element_type=F32)
        d_weight = jnp.sum(grad * x_hat, axis=0, **KEEP)
        d_bias = jnp.sum(grad, axis=0, **KEEP)
        val[16:SMALL, cols] = jnp.where(row == 0, d_weight, jnp.where(row == 1, d_bias, 0.0))
        scaled = grad * lnw[:, cols]
        return sums[0] + jnp.sum(scaled, axis=1, **KEEP), sums[1] + jnp.sum(scaled * x_hat, axis=1, **KEEP)

    mean_one, mean_two = lax.fori_loop(0, d_model // wide, gradient, (zero, zero))
    mean_one, mean_two = mean_one / d_model, mean_two / d_model

    def part(e):
        return rows_at(e * width, width, LANES)

    def scatter(k):
        to = here.ep_to(k)
        return remote(src_ref=val.at[:, part(to)], dst_ref=first.at[ep], send_sem=s_one.at[k], recv_sem=r_one.at[k],
                      device_id=(here.dp, to))

    def along(axis, src, dst, send, recv, k):
        mine = here.y if axis == 'y' else here.z
        return remote(src_ref=src, dst_ref=dst.at[mine], send_sem=send.at[k], recv_sem=recv.at[k], device_id=here.device(axis, k))

    def gather(k):
        return remote(src_ref=c_three, dst_ref=small.at[:, part(ep)], send_sem=s_four.at[k], recv_sem=r_four.at[k],
                      device_id=(here.dp, here.ep_to(k)))

    def add_up(ref, n):
        total = ref[0]
        for i in range(1, n):
            total = total + ref[i]
        return total

    for k in range(n_peer):
        scatter(k).start()
    first[ep] = val[:, part(ep)]

    @pl.loop(0, d_model // wide)
    def _(i):
        cols = rows_at(i * wide, wide, LANES)
        x_hat = (x_v[:, cols].astype(F32) - mean) * inv_std
        step = inv_std * (grad_h[:, cols] * lnw[:, cols] - mean_one - x_hat * mean_two)
        dx[:, cols] = (dy_v[:, cols].astype(F32) + step).astype(BF16)

    for k in range(n_peer):
        scatter(k).wait_recv()
    c_one[ALL] = add_up(first, n_ep)
    second[here.y] = c_one[ALL]
    for k in range(1, grid):
        along('y', c_one, second, s_two, r_two, k).start()
    for k in range(1, grid):
        along('y', c_one, second, s_two, r_two, k).wait_recv()
    c_two[ALL] = add_up(second, grid)
    third[here.z] = c_two[ALL]
    for k in range(1, grid):
        along('z', c_two, third, s_three, r_three, k).start()
    for k in range(1, grid):
        along('z', c_two, third, s_three, r_three, k).wait_recv()
    c_three[ALL] = add_up(third, grid)
    for k in range(n_peer):
        gather(k).start()
    small[:, part(ep)] = c_three[ALL]
    for k in range(n_peer):
        gather(k).wait_recv()
    for k in range(n_peer):
        scatter(k).wait_send()
        gather(k).wait_send()
        back(0, k).wait_send()
        back(1, k).wait_send()
    for k in range(1, grid):
        along('y', c_one, second, s_two, r_two, k).wait_send()
        along('z', c_two, third, s_three, r_three, k).wait_send()
    spread.receive(3)
    spread.sent(3)


def tail_call(held, o_next, dh_next, tok_x, tok_dy, hidden, o, dh, stats, err_one, err_two, places, lnw, router, cap, grid, collective_id):
    vmem, dma = pltpu.VMEM, pltpu.SemaphoreType.DMA
    n_tok, d_model = tok_x.shape
    rows = o.shape[0]
    n_ep = rows // cap
    n_peer, width = n_ep - 1, d_model // n_ep
    hbm, on_chip = pl.BlockSpec(memory_space=pl.ANY), pl.BlockSpec(memory_space=pltpu.VMEM)
    tokens = jax.ShapeDtypeStruct((n_tok, d_model), BF16)
    peers, ring = dma((n_peer,)), dma((grid,))
    return pl.pallas_call(
        functools.partial(tail_kernel, grid, cap),
        out_shape=(jax.ShapeDtypeStruct(held.shape, F32), tokens, tokens, jax.ShapeDtypeStruct((SMALL, d_model), F32)),
        in_specs=[hbm] * 8 + [on_chip] * 6, out_specs=(hbm, on_chip, on_chip, on_chip), input_output_aliases={0: 0},
        scratch_shapes=[vmem((n_tok, d_model), BF16)] * 3 + [vmem((2 * rows, d_model), BF16)] * 2
        + [vmem((n_tok, 2 * rows), BF16)] * 2 + [vmem((n_tok, d_model), F32), vmem((SMALL, d_model), F32)]
        + [vmem((n_ep, SMALL, width), F32), vmem((grid, SMALL, width), F32), vmem((grid, SMALL, width), F32)] + [vmem((SMALL, width), F32)] * 3
        + [dma((7,)), dma((UNITS, 15)), dma((UNITS, 15)), dma((2, n_peer)), dma((2, n_peer)),
           peers, peers, ring, ring, ring, ring, peers, peers],
        compiler_params=pltpu.CompilerParams(collective_id=collective_id, has_side_effects=True, vmem_limit_bytes=50 * 2 ** 20),
        cost_estimate=pl.CostEstimate(flops=10_000_000_000, bytes_accessed=STREAM, transcendentals=0),
        name='tail',
    )(held, o_next, dh_next, tok_x, tok_dy, hidden, o, dh, stats, err_one, err_two, places, lnw, router)


def expert_kernel(dims, *refs):
    expert, grid, chunk, cap, first = dims
    refs = list(refs)
    take = lambda n: [refs.pop(0) for _ in range(n)]
    if first:
        sel_in, wg_h, wu_h, wd_h = take(7), *take(3)
        o_h, dh_h, sh_h, h_next, q_next, hsl_next, qsl_next = take(7)
    else:
        h_next, q_next, hsl_next, qsl_next, wg_h, wu_h, wd_h, *carry = take(9)
        done_h, = take(1)
        o_h, dh_h, sh_h, *carry_out = take(5)
        all_h, = take(1)
    h_recv, q_recv, wg, wu, wd, a_t, b_t, d_t, u_all, da_all, db_all, h_sl, q_sl, dw, rsb, act, act_b, eye = take(18)
    loc, hs_s, hs_r, qs_s, qs_r, ga_s, ga_r, rs_s, rs_r = take(9)
    if first:
        sel_h, sel_q, sel_h_next, sel_q_next, hidden, grad_one, grad_two, h_send, q_send, h_send_next, q_send_next = take(11)
        xh_s, xh_r, xq_s, xq_r, nh_s, nh_r, nq_s, nq_r, ns_h_s, ns_h_r, ns_q_s, ns_q_r, lin = take(13)
        o_v, dh_v = h_send, q_send
    else:
        o_v, dh_v = take(2)
        ba_s, ba_r, ba_l, lin, sp_s, sp_r = take(6)
    rows, d_model = h_recv.shape
    ff = wg.shape[0]
    quarter = d_model // grid
    share = ff // grid
    here = Place(rows // cap, grid)
    n_peer = len(here.offsets)
    ep = here.ep
    remote = functools.partial(pltpu.make_async_remote_copy, device_id_type=MESH_ID)
    wide = chunk // 2

    def spot(axis):
        return here.y if axis == 'y' else here.z

    def block(e):
        return rows_at(e * cap, cap, PACK)

    weights = [pltpu.make_async_copy(src.at[expert], dst, loc.at[i]) for i, (src, dst) in enumerate(((wg_h, wg), (wu_h, wu), (wd_h, wd)))]

    def x_copy(src, dst, send, recv, k):
        return remote(src_ref=src.at[block(here.ep_to(k)), :], dst_ref=dst.at[block(ep), :],
                      send_sem=send.at[k], recv_sem=recv.at[k], device_id=(here.dp, here.ep_to(k)))

    def slice_copy(axis, buf, sl, send, recv, src_ep, k):
        return remote(src_ref=buf.at[block(src_ep), rows_at(here.step(axis, k) * quarter, quarter, LANES)],
                      dst_ref=sl.at[rows_at(spot(axis) * rows + src_ep * cap, cap, PACK), :],
                      send_sem=send.at[k], recv_sem=recv.at[k], device_id=here.device(axis, k))

    def slices(axis, buf, sl, send, recv, k):
        return remote(src_ref=buf.at[:, pl.ds(0, quarter)], dst_ref=sl.at[pl.ds(0, rows), :],
                      send_sem=send.at[k], recv_sem=recv.at[k], device_id=here.device(axis, k))

    half = ff // 2
    halves = ((pl.ds(0, half), NEAR), (pl.ds(half, half), FAR))
    gathers = [(ref, part, axis, *order) for ref, axis in ((u_all, 'z'), (da_all, 'y'), (db_all, 'y')) for part, order in halves]

    def share_t(g, j):
        ref, part, axis, one, two = gathers[g]
        flip = two if j else one
        owner = spot(axis) ^ (one if j == 2 else 0)
        view = ref.at[part, rows_at(owner * rows, rows, LANES)]
        return remote(src_ref=view, dst_ref=view, send_sem=ga_s.at[g, j], recv_sem=ga_r.at[g, j], device_id=here.flip(axis, flip))

    def share_start(t):
        for g in (2 * t, 2 * t + 1):
            share_t(g, 0).start()

    def share_on(t):
        for g in (2 * t, 2 * t + 1):
            share_t(g, 0).wait_recv()
            for j in (1, 2):
                share_t(g, j).start()

    def share_done(t):
        for g in (2 * t, 2 * t + 1):
            for j in (1, 2):
                share_t(g, j).wait_recv()

    wing = quarter // 2
    wings = ((pl.ds(0, wing), NEAR), (pl.ds(wing, wing), FAR))
    reduces = [(t, cols, axis, *order) for t, axis in enumerate('zzy') for cols, order in wings]

    def part_at(i):
        return rows_at(i * share, share, 8)

    def reduce_copy(r, j):
        t, cols, axis, one, two = reduces[r]
        here_at = spot(axis)
        flip, chunk_at = ((one, here_at ^ one), (one, here_at ^ one ^ two), (two, here_at ^ two))[j]
        return remote(src_ref=dw.at[t, part_at(chunk_at), cols], dst_ref=rsb.at[t, j, :, cols],
                      send_sem=rs_s.at[r, j], recv_sem=rs_r.at[r, j], device_id=here.flip(axis, flip))

    def reduce_start(t):
        for r in (2 * t, 2 * t + 1):
            for j in (0, 1):
                reduce_copy(r, j).start()

    def reduce_on(t):
        for r in (2 * t, 2 * t + 1):
            _, cols, axis, _, two = reduces[r]
            reduce_copy(r, 0).wait_recv()
            reduce_copy(r, 1).wait_recv()
            on = part_at(spot(axis) ^ two)
            dw[t, on, cols] = dw[t, on, cols] + rsb[t, 1, :, cols]
            reduce_copy(r, 2).start()

    def reduce_end(t):
        axis = 'zzy'[t]
        for r in (2 * t, 2 * t + 1):
            reduce_copy(r, 2).wait_recv()
        rsb[t, 0] = dw[t, part_at(spot(axis)), :] + rsb[t, 0] + rsb[t, 2]
        unit = quarter // UNITS
        outs = [pltpu.make_async_copy(rsb.at[t, 0, :, pl.ds(i * unit, unit)], sh_h.at[i, t], loc.at[5 + t * UNITS + i]) for i in range(UNITS)]
        for c in outs:
            c.start()
        return outs

    def own_slice(axis, buf, sl):
        sl[rows_at(spot(axis) * rows, rows, PACK), :] = buf[:, rows_at(spot(axis) * quarter, quarter, LANES)]

    strip = ff // 7
    u_cols = rows_at(here.z * rows, rows, LANES)
    g_cols = rows_at(here.y * rows, rows, LANES)

    def forward_pass():
        a_t[ALL] = jnp.zeros_like(a_t)
        b_t[ALL] = jnp.zeros_like(b_t)

        @pl.loop(0, d_model // chunk)
        def _(i):
            cols = rows_at(i * chunk, chunk, LANES)
            a_t[ALL] += lax.dot_general(wg[:, cols], h_recv[:, cols], NT, preferred_element_type=F32)
            b_t[ALL] += lax.dot_general(wu[:, cols], h_recv[:, cols], NT, preferred_element_type=F32)

        @pl.loop(0, 7)
        def _(i):
            r = rows_at(i * strip, strip, PACK)
            a = a_t[r, :]
            u_all[r, u_cols] = (a * jax.nn.sigmoid(a) * b_t[r, :]).astype(BF16)

    def backward_pass():
        d_t[ALL] = jnp.zeros_like(d_t)

        @pl.loop(0, d_model // chunk)
        def _(i):
            cols = rows_at(i * chunk, chunk, LANES)
            d_t[ALL] += lax.dot_general(wd[:, cols], q_recv[:, cols], NT, preferred_element_type=F32)

        @pl.loop(0, 7)
        def _(i):
            r = rows_at(i * strip, strip, PACK)
            a, b, du = a_t[r, :], b_t[r, :], d_t[r, :]
            sig = jax.nn.sigmoid(a)
            silu = a * sig
            da_all[r, g_cols] = (du * b * sig * (1.0 + a * (1.0 - sig))).astype(BF16)
            db_all[r, g_cols] = (du * silu).astype(BF16)

    def untranspose(out, ref, cols):
        out[ALL] = lax.dot_general(eye[ALL], ref[:, cols], NT, preferred_element_type=F32).astype(BF16)

    def o_pass():
        @pl.loop(0, d_model // wide)
        def _(i):
            cols = rows_at(i * wide, wide, LANES)
            o_v[:, cols] = jnp.dot(act[ALL], wd[:, cols], preferred_element_type=F32).astype(BF16)

    def dh_pass():
        @pl.loop(0, d_model // wide)
        def _(i):
            cols = rows_at(i * wide, wide, LANES)
            dh_v[:, cols] = (jnp.dot(act[ALL], wg[:, cols], preferred_element_type=F32)
                             + jnp.dot(act_b[ALL], wu[:, cols], preferred_element_type=F32)).astype(BF16)

    def weight_grad(t, left, right):
        @pl.loop(0, quarter // wide)
        def _(i):
            cols = rows_at(i * wide, wide, LANES)
            dw[t, :, cols] = jnp.dot(left[ALL], right[:, cols], preferred_element_type=F32)

    def forward_part():
        weights[0].wait()
        weights[1].wait()
        forward_pass()
        share_start(0)
        untranspose(act, u_all, u_cols)
        weights[2].wait()
        o_pass()
        o_out = pltpu.make_async_copy(o_v, o_h, loc.at[3])
        o_out.start()
        return o_out

    def make_eye():
        eye[ALL] = (lax.broadcasted_iota(jnp.int32, (rows, rows), 0)
                    == lax.broadcasted_iota(jnp.int32, (rows, rows), 1)).astype(F32).astype(BF16)

    if first:
        inputs = [pltpu.make_async_copy(src, dst, lin.at[i])
                  for i, (src, dst) in enumerate(zip(sel_in, (sel_h, hidden, sel_q, grad_one, grad_two, sel_h_next, sel_q_next)))]
        for c in inputs:
            c.start()
        signals = here.arrive()
        for c in inputs:
            c.wait()

        def gather(sel, source, out, e):
            @pl.loop(0, d_model // chunk)
            def _(i):
                cols = rows_at(i * chunk, chunk, LANES)
                total = jnp.dot(sel[block(e), :n_tok], source[0][:, cols], preferred_element_type=F32)
                for j in range(1, len(source)):
                    total += jnp.dot(sel[block(e), j * n_tok:(j + 1) * n_tok], source[j][:, cols], preferred_element_type=F32)
                out[block(e), cols] = total.astype(BF16)

        n_tok = hidden.shape[0]
        rows_h, rows_q = (hidden,), (grad_one, grad_two)
        now = ((sel_h, rows_h, h_send, h_recv, xh_s, xh_r), (sel_q, rows_q, q_send, q_recv, xq_s, xq_r))
        later = ((sel_h_next, rows_h, h_send_next, h_next, nh_s, nh_r), (sel_q_next, rows_q, q_send_next, q_next, nq_s, nq_r))

        def copy_of(what, k):
            _, _, out, recv_buf, send, recv = what
            return x_copy(out, recv_buf, send, recv, k)

        others = range(1, n_peer)
        pairs = list(zip(others[::2], others[1::2]))
        steps = [(group, i, ks) for group, order in ((now, (0, 1)), (later, (1, 0))) for i in order for ks in pairs]
        ahead = 2 * len(pairs)

        def gather_step(n):
            if n < len(steps):
                group, i, ks = steps[n]
                for k in ks:
                    gather(group[i][0], group[i][1], group[i][2], here.ep_to(k))

        def send_step(n):
            if n < len(steps):
                group, i, ks = steps[n]
                for k in ks:
                    copy_of(group[i], k).start()

        def sent_step(n):
            if n < len(steps):
                group, i, ks = steps[n]
                for k in ks:
                    copy_of(group[i], k).wait_send()

        def partner(group):
            for what in group:
                gather(what[0], what[1], what[2], here.ep_to(0))

        def partner_send(group):
            for what in group:
                copy_of(what, 0).start()

        gather_step(0)
        here.barrier(signals)
        send_step(0)
        gather_step(1)
        send_step(1)
        partner(now)
        partner_send(now)
        for c in weights:
            c.start()
        for what in now:
            gather(what[0], what[1], what[3], ep)
        make_eye()

        spread = (('y', h_recv, h_sl, hs_s, hs_r), ('z', q_recv, q_sl, qs_s, qs_r))
        spread_next = (('y', h_next, hsl_next, ns_h_s, ns_h_r), ('z', q_next, qsl_next, ns_q_s, ns_q_r))

        def forward_own(spread, bufs):
            for (axis, _, sl, send, recv), buf in zip(spread, bufs):
                for k in range(1, grid):
                    slice_copy(axis, buf, sl, send, recv, ep, k).start()

        def forward(group, spread, i, p):
            axis, buf, sl, send, recv = spread[i]
            copy_of(group[i], p).wait_recv()
            for k in range(1, grid):
                slice_copy(axis, buf, sl, send, recv, here.ep_from(p), k).start()

        def forward_step(n):
            if n < len(steps):
                group, i, ks = steps[n]
                for k in ks:
                    forward(group, spread if group is now else spread_next, i, k)

        forward_own(spread, (h_recv, q_recv))
        for i in range(2):
            forward(now, spread, i, 0)
        for what in later:
            gather(what[0], what[1], what[2], ep)
        own_next = [pltpu.make_async_copy(what[2].at[block(ep), :], what[3].at[block(ep), :], lin.at[7 + i]) for i, what in enumerate(later)]
        partner(later)
        partner_send(later)
        middle, last = max(len(pairs) - 1, 0), max(ahead - 1, 0)
        for n in range(last + 1):
            gather_step(n + 2)
            sent_step(n)
            send_step(n + 2)
            forward_step(n)
            if n == middle:
                own_slice('y', h_recv, h_sl)
                copy_of(now[0], 0).wait_send()
                o_out = forward_part()
            if n == min(middle + 2, last):
                share_on(0)
            if n >= 2:
                gather_step(n + ahead)
            if n == min(1, last):
                forward_own(spread_next, (h_send_next, q_send_next))
                for i in range(2):
                    forward(later, spread_next, i, 0)
        send_step(ahead + 2)
        send_step(ahead + 3)
        for c in own_next:
            c.start()
        own_slice('z', q_recv, q_sl)
        copy_of(now[1], 0).wait_send()
    else:
        load_h, load_q = [pltpu.make_async_copy(src, dst, lin.at[2 + i * grid]) for i, (src, dst) in enumerate(((h_next, h_recv), (q_next, q_recv)))]
        load_slices = []
        for i, (axis, src, dst) in enumerate((('z', qsl_next, q_sl), ('y', hsl_next, h_sl))):
            for k in range(1, grid):
                part = rows_at(here.step(axis, k) * rows, rows, PACK)
                load_slices.append(pltpu.make_async_copy(src.at[part, :], dst.at[part, :], lin.at[2 + i * grid + k]))
        for c in [load_h] + weights + [load_q] + load_slices:
            c.start()
        here.barrier()
        back = list(zip(carry, carry_out))
        spread_unit = Spread(here, done_h, all_h, sp_s, sp_r)
        own_unit = pltpu.make_async_copy(done_h, all_h.at[here.dp], lin.at[1])
        spread_unit.send(0)
        spread_unit.send(1, (0,))

        def back_copy(j, k):
            src, dst = back[j]
            return remote(src_ref=src.at[block(here.ep_to(k)), :], dst_ref=dst.at[block(ep), :],
                          send_sem=ba_s.at[j, k], recv_sem=ba_r.at[j, k], device_id=(here.dp, here.ep_to(k)))

        def back_own(j):
            src, dst = back[j]
            return pltpu.make_async_copy(src.at[block(ep), :], dst.at[block(ep), :], ba_l.at[j])

        def send_back(j):
            for k in range(n_peer):
                back_copy(j, k).start()
            back_own(j).start()

        for j in range(len(carry)):
            send_back(j)
        make_eye()
        load_h.wait()
        o_out = forward_part()
        load_q.wait()
        own_slice('y', h_recv, h_sl)
        own_slice('z', q_recv, q_sl)
        own_unit.start()

    backward_pass()
    share_start(1)
    share_start(2)
    if first:
        sent_step(ahead)
        send_step(ahead + 4)
    else:
        share_on(0)
    untranspose(act, da_all, g_cols)
    untranspose(act_b, db_all, g_cols)
    share_on(1)
    share_on(2)
    if not first:
        spread_unit.receive(0)
        spread_unit.send(1, (1,))
    dh_pass()
    dh_out = pltpu.make_async_copy(dh_v, dh_h, loc.at[4])
    dh_out.start()
    if first:
        sent_step(ahead + 1)
        send_step(ahead + 5)
        forward_step(ahead)
        for k in range(1, grid):
            slices('z', q_recv, q_sl, qs_s, qs_r, k).wait_recv()
            slices('y', h_recv, h_sl, hs_s, hs_r, k).wait_recv()
    else:
        for c in load_slices:
            c.wait()
    share_done(1)
    weight_grad(0, da_all, h_sl)
    reduce_start(0)
    if not first:
        spread_unit.send(2, (0,))
    share_done(0)
    weight_grad(2, u_all, q_sl)
    share_done(2)
    weight_grad(1, db_all, h_sl)
    reduce_start(1)
    reduce_start(2)
    if first:
        forward_step(ahead + 1)
    else:
        spread_unit.receive(1)
    reduce_on(0)
    if not first:
        spread_unit.send(2, (1,))
    reduce_on(1)
    reduce_on(2)
    if first:
        for n in range(2, 5):
            forward_step(ahead + n)
    else:
        spread_unit.send(2, (2, 3))
    ends = reduce_end(0) + reduce_end(1) + reduce_end(2)
    if first:
        forward_step(ahead + 5)

    for j in range(3):
        for g in range(len(gathers)):
            share_t(g, j).wait_send()
            reduce_copy(g, j).wait_send()
    if first:
        for k in range(1, grid):
            for axis, buf, sl, send, recv in spread:
                slices(axis, buf, sl, send, recv, k).wait_send()
            for axis, buf, sl, send, recv in spread_next:
                slices(axis, buf, sl, send, recv, k).wait()
        for what in later:
            copy_of(what, 0).wait_send()
        for n in range(2, 6):
            sent_step(ahead + n)
        for c in own_next:
            c.wait()
    else:
        for j in range(len(back)):
            for k in range(n_peer):
                back_copy(j, k).wait()
            back_own(j).wait()
        spread_unit.receive(2)
        for stage in range(3):
            spread_unit.sent(stage)
        own_unit.wait()
    for c in ends + [o_out, dh_out]:
        c.wait()


def expert_call(inputs, w_gate, w_up, w_down, expert, cap, grid):
    first = expert == 0
    d_model = w_gate.shape[2]
    ff = w_gate.shape[1]
    rows = inputs[0].shape[0]
    quarter, share = d_model // grid, ff // grid
    n_peer = rows // cap - 1
    chunk = min(1024, d_model)
    vmem, dma = pltpu.VMEM, pltpu.SemaphoreType.DMA
    hbm = pl.BlockSpec(memory_space=pl.ANY)
    row_block, slice_block = (rows, d_model), (grid * rows, quarter)
    scratch = [
        vmem(row_block, BF16), vmem(row_block, BF16),
        vmem((ff, d_model), BF16), vmem((ff, d_model), BF16), vmem((ff, d_model), BF16),
        vmem((ff, rows), F32), vmem((ff, rows), F32), vmem((ff, rows), F32),
        vmem((ff, grid * rows), BF16), vmem((ff, grid * rows), BF16), vmem((ff, grid * rows), BF16),
        vmem(slice_block, BF16), vmem(slice_block, BF16),
        vmem((3, ff, quarter), F32), vmem((3, 3, share, quarter), F32),
        vmem((rows, ff), BF16), vmem((rows, ff), BF16), vmem((rows, rows), BF16), dma((5 + 3 * UNITS,)),
    ] + [dma((grid,))] * 4 + [dma((6, 3))] * 4
    out = lambda shape, dtype=BF16: jax.ShapeDtypeStruct(shape, dtype)
    share_block = (UNITS, 3, share, quarter // UNITS)
    outs = [out(row_block), out(row_block), out(share_block, F32)]
    if first:
        sel_h, hidden, sel_q, grad_one, grad_two, sel_h_next, sel_q_next = inputs
        scratch += [vmem(x.shape, BF16) for x in (sel_h, sel_q, sel_h_next, sel_q_next, hidden, grad_one, grad_two)]
        scratch += [vmem(row_block, BF16)] * 4 + [dma((n_peer,))] * 8 + [dma((grid,))] * 4 + [dma((9,))]
        operands = (*inputs, w_gate, w_up, w_down)
        outs += [out(row_block), out(row_block), out(slice_block), out(slice_block)]
    else:
        h_next, q_next, hsl_next, qsl_next, *carry, done = inputs
        scratch += [vmem(row_block, BF16)] * 2 + [dma((2, n_peer)), dma((2, n_peer)), dma((2,)), dma((2 + 2 * grid,))]
        scratch += [dma((UNITS, 15)), dma((UNITS, 15))]
        operands = (h_next, q_next, hsl_next, qsl_next, w_gate, w_up, w_down, *carry, done)
        outs += [out(row_block), out(row_block), out((grid * grid,) + share_block, F32)]
    return pl.pallas_call(
        functools.partial(expert_kernel, (expert, grid, chunk, cap, first)),
        out_shape=tuple(outs), in_specs=[hbm] * len(operands), out_specs=(hbm,) * len(outs), scratch_shapes=scratch,
        compiler_params=pltpu.CompilerParams(collective_id=expert, has_side_effects=True, vmem_limit_bytes=63 * 2 ** 20),
        cost_estimate=pl.CostEstimate(flops=2 * rows * d_model * ff * 9, bytes_accessed=STREAM, transcendentals=0),
    )(*operands)


def assemble_kernel(gate, up, down, *refs):
    n_pass = (len(refs) - 3) // 2 if len(refs) > 6 else 0
    outs = refs[-3 - n_pass:][:3]
    for j in range(n_pass):
        refs[-n_pass + j][ALL] = refs[j][ALL]
    grid, unit = gate.shape[1], gate.shape[-1]
    for c in range(grid):
        for i in range(UNITS):
            at = (c * UNITS + i) * unit
            outs[0][0, :, at:at + unit] = gate[0, c, i, 0]
            outs[1][0, :, at:at + unit] = up[0, c, i, 0]
            outs[2][0, :, at:at + unit] = down[c, 0, i, 0]


def assemble(gathered, expert, n_expert, into, through=()):
    grid, _, _, _, share, unit = gathered.shape
    cut = 2
    part = share // cut
    row_first = pl.BlockSpec((1, grid, UNITS, 1, part, unit), lambda r, h: (r, 0, 0, 0, h, 0))
    up_first = pl.BlockSpec((1, grid, UNITS, 1, part, unit), lambda r, h: (r, 0, 0, 1, h, 0))
    col_first = pl.BlockSpec((grid, 1, UNITS, 1, part, unit), lambda r, h: (0, r, 0, 2, h, 0))
    out_spec = pl.BlockSpec((1, part, grid * UNITS * unit), lambda r, h: (expert, r * cut + h, 0))
    whole = jax.ShapeDtypeStruct((n_expert, grid * share, grid * UNITS * unit), F32)
    strips = [pl.BlockSpec((x.shape[0] // (grid * cut), x.shape[1]), lambda r, h: (r * cut + h, 0)) for x in through]
    return pl.pallas_call(
        assemble_kernel, grid=(grid, cut), out_shape=(whole,) * 3 + tuple(jax.ShapeDtypeStruct(x.shape, x.dtype) for x in through),
        in_specs=[row_first, up_first, col_first] + strips + [pl.BlockSpec(memory_space=pl.ANY)] * len(into),
        out_specs=(out_spec,) * 3 + tuple(strips), input_output_aliases={3 + i: i for i in range(len(into))},
        compiler_params=pltpu.CompilerParams(vmem_limit_bytes=40 * 2 ** 20),
        cost_estimate=pl.CostEstimate(flops=1_000_000, bytes_accessed=44_000_000, transcendentals=0),
    )(gathered, gathered, gathered, *through, *into)


def solution(mesh):
    n_ep = mesh.shape['ep']
    grid = round(mesh.shape['dp'] ** 0.5)
    tok_spec = P(('dp', 'ep'), None)
    row_spec = P(('dp', 'ep'))
    exp_spec = P('ep', None, None)

    def local_step(tok_x, tok_dy, exp_first, exp_second, eligible, slot_first, slot_second,
                   ln_weight, ln_bias, router, w_gate, w_up, w_down):
        n_local, _ = tok_x.shape
        n_exp = eligible.shape[1]
        local_exp = w_gate.shape[0]
        slot_cap = 3 * n_local // n_exp
        hidden, mean, inv_std = layer_norm(tok_x, ln_weight, ln_bias)
        logits = jnp.dot(hidden, router, preferred_element_type=F32)
        expert_ids = jnp.arange(n_exp)
        allowed = eligible > 0
        gate_one, prob_one, pick_one = masked_gate(logits, allowed, exp_first)
        gate_two, prob_two, pick_two = masked_gate(logits, allowed & (expert_ids[None, :] != exp_first[:, None]), exp_second)
        per = n_ep * slot_cap
        row_ids = jnp.arange(n_exp * slot_cap)

        def place(expert, slot):
            pos = (expert % local_exp) * per + (expert // local_exp) * slot_cap + slot
            return jnp.where(slot >= 0, pos, -1)

        pos_one = place(exp_first, slot_first)
        pos_two = place(exp_second, slot_second)
        dy_float = tok_dy.astype(F32)
        grad_one = (gate_one[:, None] * dy_float).astype(BF16)
        grad_two = (gate_two[:, None] * dy_float).astype(BF16)
        pos_pair = jnp.concatenate([pos_one, pos_two])
        wg_t, wu_t = jnp.swapaxes(w_gate, 1, 2), jnp.swapaxes(w_up, 1, 2)

        def lanes(columns):
            flat = jnp.concatenate(columns, axis=1)
            return jnp.pad(flat, ((0, 0), (0, LANES - flat.shape[1])))

        stats = lanes([gate_one[:, None], gate_two[:, None], mean, inv_std])
        err_one, err_two = lanes([pick_one - prob_one]), lanes([pick_two - prob_two])
        places = lanes([pos_one[:, None], pos_two[:, None]])
        router_t = jnp.pad(router.T, ((0, LANES - n_exp), (0, 0)))
        cuts = [slice(e * per, (e + 1) * per) for e in range(local_exp)]
        sels = []
        for e in range(local_exp):
            ids = row_ids[cuts[e]][:, None]
            sels.append(jnp.logical_or(ids == pos_one[None, :], ids == pos_two[None, :]).astype(BF16))
            sels.append((ids == pos_pair[None, :]).astype(BF16))
        o, dh, share, *landed = expert_call((sels[0], hidden, sels[1], grad_one, grad_two, sels[2], sels[3]), wg_t, wu_t, w_down, 0, slot_cap, grid)
        o_next, dh_next, share, o, dh, held = expert_call((*landed, o, dh, share), wg_t, wu_t, w_down, 1, slot_cap, grid)
        gathered_next = lax.all_gather(share, 'dp')
        held, out_tok, dx_tok, small = tail_call(
            held, o_next, dh_next, tok_x, tok_dy, hidden, o, dh, stats, err_one, err_two, places,
            ln_weight.astype(F32)[None], router_t, slot_cap, grid, local_exp + 1)
        gathered = [x.reshape((grid, grid) + share.shape) for x in (held, gathered_next)]
        d_router, d_ln_weight, d_ln_bias = small[:n_exp].T, small[16], small[17]
        *weights, out_tok, dx_tok = assemble(gathered[0], 0, local_exp, (), (out_tok, dx_tok))
        weights = assemble(gathered[1], 1, local_exp, weights)
        dw_gate, dw_up, dw_down = jnp.swapaxes(weights[0], 1, 2), jnp.swapaxes(weights[1], 1, 2), weights[2]
        return out_tok, dx_tok, dw_gate, dw_up, dw_down, d_router, d_ln_weight, d_ln_bias

    return jax.shard_map(
        local_step, mesh=mesh,
        in_specs=(tok_spec, tok_spec, row_spec, row_spec, tok_spec, row_spec, row_spec,
                  P(), P(), P(), exp_spec, exp_spec, exp_spec),
        out_specs=(tok_spec, tok_spec, exp_spec, exp_spec, exp_spec, P(), P(), P()),
        check_vma=False)
```

```python
import functools

import jax
import jax.numpy as jnp
from jax import lax
from jax.experimental import pallas as pl
from jax.experimental.pallas import tpu as pltpu
from jax.sharding import PartitionSpec as P


LN_EPS = 1e-5
CORES = 2
UNITS = 4
NEAR, FAR = (1, 3), (3, 1)
LANES = 128
PACK = 16
STRIPS = 7
SMALL = 24
STREAM = 30_000_000
KEEP = {'keepdims': True}
F32 = jnp.float32
BF16 = jnp.bfloat16
ALL = Ellipsis
MESH_ID = pl.DeviceIdType.MESH
NT = (((1,), (1,)), ((), ()))


def ring_offsets(n_x):
    near = [d for d in (1, n_x - 1) if 0 < d < n_x]
    near = list(dict.fromkeys(near))
    far = [d for d in range(2, n_x - 1)]
    out = [(0, 1)]
    for group in (near, far):
        for core in range(CORES):
            out += [(d, core) for d in group]
    return out


class Place:
    def __init__(self, n_ep, grid):
        self.n_x, self.grid = n_ep // CORES, grid
        self.ep, self.dp = lax.axis_index('ep'), lax.axis_index('dp')
        self.x, self.core = self.ep // CORES, self.ep % CORES
        self.z, self.y = self.dp // grid, self.dp % grid
        self.offsets = ring_offsets(self.n_x)

    def ep_to(self, k):
        dx, dc = self.offsets[k]
        return lax.rem(self.x + dx, self.n_x) * CORES + lax.rem(self.core + dc, CORES)

    def ep_from(self, k):
        dx, dc = self.offsets[k]
        return lax.rem(self.x + (self.n_x - dx), self.n_x) * CORES + lax.rem(self.core + dc, CORES)

    def step(self, axis, k):
        here = self.y if axis == 'y' else self.z
        return lax.rem(here + k + self.grid, self.grid)

    def device(self, axis, k):
        if axis == 'y':
            return (self.z * self.grid + self.step('y', k), self.ep)
        return (self.step('z', k) * self.grid + self.y, self.ep)

    def flip(self, axis, bits):
        if axis == 'y':
            return (self.z * self.grid + (self.y ^ bits), self.ep)
        return ((self.z ^ bits) * self.grid + self.y, self.ep)

    def arrive(self):
        sem = pltpu.get_barrier_semaphore()
        peers = [(self.dp, self.ep_to(k)) for k in range(len(self.offsets))]
        for k in range(1, self.grid):
            peers += [self.device('y', k), self.device('z', k)]
        for peer in peers:
            pl.semaphore_signal(sem, inc=1, device_id=peer, device_id_type=MESH_ID)
        return len(peers)

    def barrier(self, signals=None):
        pl.semaphore_wait(pltpu.get_barrier_semaphore(), self.arrive() if signals is None else signals)


def cost(flops, size):
    return pl.CostEstimate(flops=flops, bytes_accessed=size, transcendentals=0)


def rows_at(start, size, unit):
    return pl.ds(pl.multiple_of(start, unit), size)


class Spread:
    STAGES = [range(2 ** i - 1, 2 ** (i + 1) - 1) for i in range(UNITS)]

    def __init__(self, here, own, held, send, recv):
        self.here, self.own, self.held, self.sems = here, own, held, (send, recv)

    def plan(self, unit, index):
        axes = ('y', 'z') if unit < UNITS // 2 else ('z', 'y')
        one, two = FAR if unit % 2 else NEAR
        line = (0, one, two, one ^ two)
        if index < 1:
            return axes, (axes[0], one), (0, 0)
        if index < 3:
            return axes, (axes[0], two), (line[index - 1], 0)
        if index < 7:
            return axes, (axes[1], one), (line[index - 3], 0)
        return axes, (axes[1], two), (line[(index - 7) % 4], (0, one)[(index - 7) // 4])

    def copy(self, unit, index):
        axes, (axis, flip), offsets = self.plan(unit, index)
        at = dict(zip(axes, offsets))
        owner = (self.here.z ^ at['z']) * self.here.grid + (self.here.y ^ at['y'])
        held = self.held.at[owner, unit]
        source = self.own.at[unit] if self.own is not None and offsets == (0, 0) else held
        return pltpu.make_async_remote_copy(src_ref=source, dst_ref=held, send_sem=self.sems[0].at[unit, index],
                                            recv_sem=self.sems[1].at[unit, index], device_id=self.here.flip(axis, flip),
                                            device_id_type=MESH_ID)

    def each(self, stage, picks=None):
        ids = self.STAGES[stage]
        for index in ids if picks is None else [ids[p] for p in picks]:
            for unit in range(UNITS):
                yield self.copy(unit, index)

    def send(self, stage, picks=None):
        for c in self.each(stage, picks):
            c.start()

    def receive(self, stage):
        for c in self.each(stage):
            c.wait_recv()

    def sent(self, stage):
        for c in self.each(stage):
            c.wait_send()


def tail_kernel(grid, cap, *refs):
    refs = list(refs)
    take = lambda n: [refs.pop(0) for _ in range(n)]
    _, o_next_h, dh_next_h, x_h, dy_h, hid_h, o_h, dh_h, stats, err_one, err_two, lnw, router = take(13)
    held, out, dx, small = take(4)
    x_v, dy_v, hid_v, o_v, dh_v, sel_one, sel_two, grad_h, val = take(9)
    first, second, third, c_one, c_two, c_three = take(6)
    loc, sp_s, sp_r, ba_s, ba_r, s_one, r_one, s_two, r_two, s_three, r_three, s_four, r_four = take(13)
    n_tok, d_model = x_v.shape
    rows = o_next_h.shape[0]
    n_ep, _, width = first.shape
    wide = min(512, d_model)
    here = Place(n_ep, grid)
    n_peer = len(here.offsets)
    ep = here.ep
    remote = functools.partial(pltpu.make_async_remote_copy, device_id_type=MESH_ID)
    here.barrier()
    spread = Spread(here, None, held, sp_s, sp_r)
    spread.send(3)

    def block(e, base=0):
        return rows_at(base + e * cap, cap, PACK)

    pairs = ((o_next_h, o_v), (dh_next_h, dh_v))

    def back(j, k):
        src, dst = pairs[j]
        return remote(src_ref=src.at[block(here.ep_to(k)), :], dst_ref=dst.at[block(ep, rows), :],
                      send_sem=ba_s.at[j, k], recv_sem=ba_r.at[j, k], device_id=(here.dp, here.ep_to(k)))

    own = [pltpu.make_async_copy(src.at[block(ep), :], dst.at[block(ep, rows), :], loc.at[j]) for j, (src, dst) in enumerate(pairs)]
    for j in range(2):
        for k in range(n_peer):
            back(j, k).start()
        own[j].start()
    home = pl.ds(0, rows)
    loads = [pltpu.make_async_copy(src, dst, loc.at[2 + i]) for i, (src, dst) in enumerate((
        (x_h, x_v), (dy_h, dy_v), (hid_h, hid_v), (o_h, o_v.at[home, :]), (dh_h, dh_v.at[home, :])))]
    for c in loads:
        c.start()
    slots = lax.broadcasted_iota(jnp.int32, (n_tok, 2 * rows), 1)
    sel_one[ALL] = (slots == stats[:, 4:5].astype(jnp.int32)).astype(F32).astype(BF16)
    sel_two[ALL] = (slots == stats[:, 5:6].astype(jnp.int32)).astype(F32).astype(BF16)
    gate_one, gate_two, mean, inv_std = [stats[:, i:i + 1] for i in range(4)]
    zero = jnp.zeros((n_tok, 1), F32)
    for c in loads:
        c.wait()
    own[0].wait()
    for k in range(n_peer):
        back(0, k).wait_recv()

    def mix(i, sums):
        cols = rows_at(i * wide, wide, LANES)
        one = jnp.dot(sel_one[ALL], o_v[:, cols], preferred_element_type=F32)
        two = jnp.dot(sel_two[ALL], o_v[:, cols], preferred_element_type=F32)
        dy = dy_v[:, cols].astype(F32)
        out[:, cols] = (x_v[:, cols].astype(F32) + (gate_one * one + gate_two * two)).astype(BF16)
        return sums[0] + jnp.sum(dy * one, axis=1, **KEEP), sums[1] + jnp.sum(dy * two, axis=1, **KEEP)

    dgate_one, dgate_two = lax.fori_loop(0, d_model // wide, mix, (zero, zero))
    d_logits = ((dgate_one * gate_one) * err_one[ALL] + (dgate_two * gate_two) * err_two[ALL]).astype(BF16)
    lanes = d_logits.shape[1]
    eye = (lax.broadcasted_iota(jnp.int32, (lanes, lanes), 0)
           == lax.broadcasted_iota(jnp.int32, (lanes, lanes), 1)).astype(F32).astype(BF16)
    d_logits_t = lax.dot_general(eye, d_logits, NT, preferred_element_type=F32).astype(BF16)[:PACK]
    sel_both = sel_one[ALL] + sel_two[ALL]
    row = lax.broadcasted_iota(jnp.int32, (8, wide), 0)
    own[1].wait()
    for k in range(n_peer):
        back(1, k).wait_recv()

    def gradient(i, sums):
        cols = rows_at(i * wide, wide, LANES)
        grad = (jnp.dot(d_logits, router[:, cols], preferred_element_type=F32)
                + jnp.dot(sel_both, dh_v[:, cols], preferred_element_type=F32))
        x_hat = (x_v[:, cols].astype(F32) - mean) * inv_std
        grad_h[:, cols] = grad
        val[:PACK, cols] = jnp.dot(d_logits_t, hid_v[:, cols], preferred_element_type=F32)
        d_weight = jnp.sum(grad * x_hat, axis=0, **KEEP)
        d_bias = jnp.sum(grad, axis=0, **KEEP)
        val[PACK:SMALL, cols] = jnp.where(row == 0, d_weight, jnp.where(row == 1, d_bias, 0.0))
        scaled = grad * lnw[0:1, cols]
        return sums[0] + jnp.sum(scaled, axis=1, **KEEP), sums[1] + jnp.sum(scaled * x_hat, axis=1, **KEEP)

    mean_one, mean_two = lax.fori_loop(0, d_model // wide, gradient, (zero, zero))
    mean_one, mean_two = mean_one / d_model, mean_two / d_model

    def part(e):
        return rows_at(e * width, width, LANES)

    def scatter(k):
        to = here.ep_to(k)
        return remote(src_ref=val.at[:, part(to)], dst_ref=first.at[ep], send_sem=s_one.at[k], recv_sem=r_one.at[k],
                      device_id=(here.dp, to))

    def along(axis, src, dst, send, recv, k):
        mine = here.y if axis == 'y' else here.z
        return remote(src_ref=src, dst_ref=dst.at[mine], send_sem=send.at[k], recv_sem=recv.at[k], device_id=here.device(axis, k))

    def gather(k):
        return remote(src_ref=c_three, dst_ref=small.at[:, part(ep)], send_sem=s_four.at[k], recv_sem=r_four.at[k],
                      device_id=(here.dp, here.ep_to(k)))

    def add_up(ref, n):
        total = ref[0]
        for i in range(1, n):
            total = total + ref[i]
        return total

    for k in range(n_peer):
        scatter(k).start()
    first[ep] = val[:, part(ep)]

    @pl.loop(0, d_model // wide)
    def _(i):
        cols = rows_at(i * wide, wide, LANES)
        x_hat = (x_v[:, cols].astype(F32) - mean) * inv_std
        step = inv_std * (grad_h[:, cols] * lnw[0:1, cols] - mean_one - x_hat * mean_two)
        dx[:, cols] = (dy_v[:, cols].astype(F32) + step).astype(BF16)

    for k in range(n_peer):
        scatter(k).wait_recv()
    c_one[ALL] = add_up(first, n_ep)
    second[here.y] = c_one[ALL]
    for k in range(1, grid):
        along('y', c_one, second, s_two, r_two, k).start()
    for k in range(1, grid):
        along('y', c_one, second, s_two, r_two, k).wait_recv()
    c_two[ALL] = add_up(second, grid)
    third[here.z] = c_two[ALL]
    for k in range(1, grid):
        along('z', c_two, third, s_three, r_three, k).start()
    for k in range(1, grid):
        along('z', c_two, third, s_three, r_three, k).wait_recv()
    c_three[ALL] = add_up(third, grid)
    for k in range(n_peer):
        gather(k).start()
    small[:, part(ep)] = c_three[ALL]
    for k in range(n_peer):
        gather(k).wait_recv()
    for k in range(n_peer):
        scatter(k).wait_send()
        gather(k).wait_send()
        back(0, k).wait_send()
        back(1, k).wait_send()
    for k in range(1, grid):
        along('y', c_one, second, s_two, r_two, k).wait_send()
        along('z', c_two, third, s_three, r_three, k).wait_send()
    spread.receive(3)
    spread.sent(3)


def tail_call(held, o_next, dh_next, tok_x, tok_dy, hidden, o, dh, stats, err_one, err_two, lnw, router, cap, grid, collective_id):
    vmem, dma = pltpu.VMEM, pltpu.SemaphoreType.DMA
    n_tok, d_model = tok_x.shape
    rows = o.shape[0]
    n_ep = rows // cap
    n_peer, width = n_ep - 1, d_model // n_ep
    hbm, on_chip = pl.BlockSpec(memory_space=pl.ANY), pl.BlockSpec(memory_space=pltpu.VMEM)
    tokens = jax.ShapeDtypeStruct((n_tok, d_model), BF16)
    peers, ring = dma((n_peer,)), dma((grid,))
    deep, both = dma((UNITS, 15)), dma((2, n_peer))
    return pl.pallas_call(
        functools.partial(tail_kernel, grid, cap),
        out_shape=(jax.ShapeDtypeStruct(held.shape, F32), tokens, tokens, jax.ShapeDtypeStruct((SMALL, d_model), F32)),
        in_specs=[hbm] * 8 + [on_chip] * 5, out_specs=(hbm, on_chip, on_chip, on_chip), input_output_aliases={0: 0},
        scratch_shapes=[vmem((n_tok, d_model), BF16)] * 3 + [vmem((2 * rows, d_model), BF16)] * 2
        + [vmem((n_tok, 2 * rows), BF16)] * 2 + [vmem((n_tok, d_model), F32), vmem((SMALL, d_model), F32)]
        + [vmem((n_ep, SMALL, width), F32), vmem((grid, SMALL, width), F32), vmem((grid, SMALL, width), F32)] + [vmem((SMALL, width), F32)] * 3
        + [dma((7,)), deep, deep, both, both,
           peers, peers, ring, ring, ring, ring, peers, peers],
        compiler_params=pltpu.CompilerParams(collective_id=collective_id, has_side_effects=True, vmem_limit_bytes=50 * 2 ** 20),
        cost_estimate=cost(10_000_000_000, STREAM),
        name='tail',
    )(held, o_next, dh_next, tok_x, tok_dy, hidden, o, dh, stats, err_one, err_two, lnw, router)


def expert_kernel(dims, *refs):
    expert, grid, chunk, cap, first = dims
    refs = list(refs)
    take = lambda n: [refs.pop(0) for _ in range(n)]
    if first:
        marks, columns, picks, norm, router, x_h, dy_h, wg_h, wu_h, wd_h = take(10)
        o_h, dh_h, sh_h, h_next, q_next, hsl_next, qsl_next, hid_h, stats, err_one, err_two = take(11)
    else:
        h_next, q_next, hsl_next, qsl_next, wg_h, wu_h, wd_h, *carry = take(9)
        done_h, = take(1)
        o_h, dh_h, sh_h, *carry_out = take(5)
        all_h, = take(1)
    h_recv, q_recv, wg, wu, wd, a_t, b_t, d_t, u_all, da_all, db_all, h_sl, q_sl, dw, rsb, act, act_b, eye = take(18)
    loc, hs_s, hs_r, qs_s, qs_r, ga_s, ga_r, rs_s, rs_r = take(9)
    if first:
        sel_h, sel_q, sel_h_next, sel_q_next, hidden, grad_one, grad_two, h_send, q_send, h_send_next, q_send_next = take(11)
        xh_s, xh_r, xq_s, xq_r, nh_s, nh_r, nq_s, nq_r, ns_h_s, ns_h_r, ns_q_s, ns_q_r, lin = take(13)
        o_v, dh_v = h_send, q_send
    else:
        o_v, dh_v = take(2)
        ba_s, ba_r, ba_l, lin, sp_s, sp_r = take(6)
    rows, d_model = h_recv.shape
    ff = wg.shape[0]
    quarter = d_model // grid
    share = ff // grid
    here = Place(rows // cap, grid)
    n_peer = len(here.offsets)
    ep = here.ep
    remote = functools.partial(pltpu.make_async_remote_copy, device_id_type=MESH_ID)
    wide = chunk // 2

    def spot(axis):
        return here.y if axis == 'y' else here.z

    def block(e):
        return rows_at(e * cap, cap, PACK)

    weights = [pltpu.make_async_copy(src.at[expert], dst, loc.at[i]) for i, (src, dst) in enumerate(((wg_h, wg), (wu_h, wu), (wd_h, wd)))]

    def x_copy(src, dst, send, recv, k):
        return remote(src_ref=src.at[block(here.ep_to(k)), :], dst_ref=dst.at[block(ep), :],
                      send_sem=send.at[k], recv_sem=recv.at[k], device_id=(here.dp, here.ep_to(k)))

    def slice_copy(axis, buf, sl, send, recv, src_ep, k):
        return remote(src_ref=buf.at[block(src_ep), rows_at(here.step(axis, k) * quarter, quarter, LANES)],
                      dst_ref=sl.at[rows_at(spot(axis) * rows + src_ep * cap, cap, PACK), :],
                      send_sem=send.at[k], recv_sem=recv.at[k], device_id=here.device(axis, k))

    def slices(axis, buf, sl, send, recv, k):
        return remote(src_ref=buf.at[:, pl.ds(0, quarter)], dst_ref=sl.at[pl.ds(0, rows), :],
                      send_sem=send.at[k], recv_sem=recv.at[k], device_id=here.device(axis, k))

    half = ff // 2
    halves = ((pl.ds(0, half), NEAR), (pl.ds(half, half), FAR))
    gathers = [(ref, part, axis, *order) for ref, axis in ((u_all, 'z'), (da_all, 'y'), (db_all, 'y')) for part, order in halves]

    def share_t(g, j):
        ref, part, axis, one, two = gathers[g]
        flip = two if j else one
        owner = spot(axis) ^ (one if j == 2 else 0)
        view = ref.at[part, rows_at(owner * rows, rows, LANES)]
        return remote(src_ref=view, dst_ref=view, send_sem=ga_s.at[g, j], recv_sem=ga_r.at[g, j], device_id=here.flip(axis, flip))

    def share_start(t):
        for g in (2 * t, 2 * t + 1):
            share_t(g, 0).start()

    def share_on(t):
        for g in (2 * t, 2 * t + 1):
            share_t(g, 0).wait_recv()
            for j in (1, 2):
                share_t(g, j).start()

    def share_done(t):
        for g in (2 * t, 2 * t + 1):
            for j in (1, 2):
                share_t(g, j).wait_recv()

    wing = quarter // 2
    wings = ((pl.ds(0, wing), NEAR), (pl.ds(wing, wing), FAR))
    reduces = [(t, cols, axis, *order) for t, axis in enumerate('zzy') for cols, order in wings]

    def part_at(i):
        return rows_at(i * share, share, 8)

    def reduce_copy(r, j):
        t, cols, axis, one, two = reduces[r]
        here_at = spot(axis)
        flip, chunk_at = ((one, here_at ^ one), (one, here_at ^ one ^ two), (two, here_at ^ two))[j]
        return remote(src_ref=dw.at[t, part_at(chunk_at), cols], dst_ref=rsb.at[t, j, :, cols],
                      send_sem=rs_s.at[r, j], recv_sem=rs_r.at[r, j], device_id=here.flip(axis, flip))

    def reduce_start(t):
        for r in (2 * t, 2 * t + 1):
            for j in (0, 1):
                reduce_copy(r, j).start()

    def reduce_on(t):
        for r in (2 * t, 2 * t + 1):
            _, cols, axis, _, two = reduces[r]
            reduce_copy(r, 0).wait_recv()
            reduce_copy(r, 1).wait_recv()
            on = part_at(spot(axis) ^ two)
            dw[t, on, cols] = dw[t, on, cols] + rsb[t, 1, :, cols]
            reduce_copy(r, 2).start()

    def reduce_end(t):
        axis = 'zzy'[t]
        for r in (2 * t, 2 * t + 1):
            reduce_copy(r, 2).wait_recv()
        rsb[t, 0] = dw[t, part_at(spot(axis)), :] + rsb[t, 0] + rsb[t, 2]
        unit = quarter // UNITS
        outs = [pltpu.make_async_copy(rsb.at[t, 0, :, pl.ds(i * unit, unit)], sh_h.at[i, t], loc.at[5 + t * UNITS + i]) for i in range(UNITS)]
        for c in outs:
            c.start()
        return outs

    def own_slice(axis, buf, sl):
        sl[rows_at(spot(axis) * rows, rows, PACK), :] = buf[:, rows_at(spot(axis) * quarter, quarter, LANES)]

    strip = ff // STRIPS
    u_cols = rows_at(here.z * rows, rows, LANES)
    g_cols = rows_at(here.y * rows, rows, LANES)

    def forward_pass():
        a_t[ALL] = jnp.zeros_like(a_t)
        b_t[ALL] = jnp.zeros_like(b_t)

        @pl.loop(0, d_model // chunk)
        def _(i):
            cols = rows_at(i * chunk, chunk, LANES)
            a_t[ALL] += lax.dot_general(wg[:, cols], h_recv[:, cols], NT, preferred_element_type=F32)
            b_t[ALL] += lax.dot_general(wu[:, cols], h_recv[:, cols], NT, preferred_element_type=F32)

        @pl.loop(0, STRIPS)
        def _(i):
            r = rows_at(i * strip, strip, PACK)
            a = a_t[r, :]
            u_all[r, u_cols] = (a * jax.nn.sigmoid(a) * b_t[r, :]).astype(BF16)

    def backward_pass():
        d_t[ALL] = jnp.zeros_like(d_t)

        @pl.loop(0, d_model // chunk)
        def _(i):
            cols = rows_at(i * chunk, chunk, LANES)
            d_t[ALL] += lax.dot_general(wd[:, cols], q_recv[:, cols], NT, preferred_element_type=F32)

        @pl.loop(0, STRIPS)
        def _(i):
            r = rows_at(i * strip, strip, PACK)
            a, b, du = a_t[r, :], b_t[r, :], d_t[r, :]
            sig = jax.nn.sigmoid(a)
            silu = a * sig
            da_all[r, g_cols] = (du * b * sig * (1.0 + a * (1.0 - sig))).astype(BF16)
            db_all[r, g_cols] = (du * silu).astype(BF16)

    def untranspose(out, ref, cols):
        out[ALL] = lax.dot_general(eye[ALL], ref[:, cols], NT, preferred_element_type=F32).astype(BF16)

    def o_pass():
        @pl.loop(0, d_model // wide)
        def _(i):
            cols = rows_at(i * wide, wide, LANES)
            o_v[:, cols] = jnp.dot(act[ALL], wd[:, cols], preferred_element_type=F32).astype(BF16)

    def dh_pass():
        @pl.loop(0, d_model // wide)
        def _(i):
            cols = rows_at(i * wide, wide, LANES)
            dh_v[:, cols] = (jnp.dot(act[ALL], wg[:, cols], preferred_element_type=F32)
                             + jnp.dot(act_b[ALL], wu[:, cols], preferred_element_type=F32)).astype(BF16)

    def weight_grad(t, left, right):
        @pl.loop(0, quarter // wide)
        def _(i):
            cols = rows_at(i * wide, wide, LANES)
            dw[t, :, cols] = jnp.dot(left[ALL], right[:, cols], preferred_element_type=F32)

    def forward_part():
        weights[0].wait()
        weights[1].wait()
        forward_pass()
        share_start(0)
        untranspose(act, u_all, u_cols)
        weights[2].wait()
        o_pass()
        o_out = pltpu.make_async_copy(o_v, o_h, loc.at[3])
        o_out.start()
        return o_out

    def make_eye():
        eye[ALL] = (lax.broadcasted_iota(jnp.int32, (rows, rows), 0)
                    == lax.broadcasted_iota(jnp.int32, (rows, rows), 1)).astype(F32).astype(BF16)

    if first:
        inputs = [pltpu.make_async_copy(src, dst, lin.at[i]) for i, (src, dst) in enumerate(((x_h, hidden), (dy_h, grad_two)))]
        n_tok = hidden.shape[0]
        lane = lax.broadcasted_iota(jnp.int32, stats.shape, 1)
        for c in inputs:
            c.start()
        signals = here.arrive()

        def place(table, i):
            ids, slots = [table[j:j + 1, :] if table is picks else table[:, j:j + 1] for j in (i, i + 2)]
            local = jnp.bitwise_and(ids, 1)
            return jnp.where(slots >= 0, local * rows + jnp.right_shift(ids, 1) * cap + slots, -1)

        for e, (one, two) in enumerate(((sel_h, sel_q), (sel_h_next, sel_q_next))):
            slot = lax.broadcasted_iota(jnp.int32, one.shape, 0) + e * rows
            hits = [(slot == place(picks, i)).astype(F32).astype(BF16) for i in range(2)]
            one[ALL] = hits[0] + hits[1]
            for i in range(2):
                two[:, i * n_tok:(i + 1) * n_tok] = hits[i]
        inputs[0].wait()
        strip_rows = 2 * PACK

        @pl.loop(0, n_tok // strip_rows)
        def _(i):
            r = rows_at(i * strip_rows, strip_rows, PACK)
            x = hidden[r, :].astype(F32)
            mean = jnp.mean(x, axis=1, **KEEP)
            centered = x - mean
            inv_std = lax.rsqrt(jnp.mean(centered * centered, axis=1, **KEEP) + LN_EPS)
            hidden[r, :] = (centered * inv_std * norm[0:1, :] + norm[1:, :]).astype(BF16)
            at = lane[:strip_rows]
            stats[r, :] = jnp.where(at == 2, mean, jnp.where(at == 3, inv_std, 0.0))

        hid_out = pltpu.make_async_copy(hidden, hid_h, lin.at[2])
        hid_out.start()

        def gates():
            logits = lax.dot_general(hidden[ALL], router[ALL], NT, preferred_element_type=F32)
            choices = [columns[:, i:i + 1] for i in range(2)]
            err_one[ALL] = jnp.zeros_like(err_one)
            err_one[:, :marks.shape[1]] = marks[ALL].astype(F32)
            allowed = err_one[ALL] > 0
            found = [place(columns, i).astype(F32) for i in range(2)]
            for choice, err in zip(choices, (err_one, err_two)):
                masked = jnp.where(allowed, logits, -1e30)
                weight = jnp.exp(masked - jnp.max(masked, axis=1, **KEEP))
                prob = weight / jnp.sum(weight, axis=1, **KEEP)
                pick = (lane == choice).astype(F32)
                found.append(jnp.sum(prob * pick, axis=1, **KEEP))
                err[ALL] = pick - prob
                allowed = jnp.logical_and(allowed, lane != choice)
            total = stats[ALL]
            for i, value in zip((4, 5, 0, 1), found):
                total = jnp.where(lane == i, value, total)
            stats[ALL] = total
            inputs[1].wait()

            @pl.loop(0, d_model // wide)
            def _(i):
                cols = rows_at(i * wide, wide, LANES)
                dy = grad_two[:, cols].astype(F32)
                grad_one[:, cols] = (stats[:, 0:1] * dy).astype(BF16)
                grad_two[:, cols] = (stats[:, 1:2] * dy).astype(BF16)

        def gather(sel, source, out, e):
            @pl.loop(0, d_model // chunk)
            def _(i):
                cols = rows_at(i * chunk, chunk, LANES)
                total = jnp.dot(sel[block(e), :n_tok], source[0][:, cols], preferred_element_type=F32)
                for j in range(1, len(source)):
                    total += jnp.dot(sel[block(e), j * n_tok:(j + 1) * n_tok], source[j][:, cols], preferred_element_type=F32)
                out[block(e), cols] = total.astype(BF16)

        rows_h, rows_q = (hidden,), (grad_one, grad_two)
        now = ((sel_h, rows_h, h_send, h_recv, xh_s, xh_r), (sel_q, rows_q, q_send, q_recv, xq_s, xq_r))
        later = ((sel_h_next, rows_h, h_send_next, h_next, nh_s, nh_r), (sel_q_next, rows_q, q_send_next, q_next, nq_s, nq_r))

        def copy_of(what, k):
            _, _, out, recv_buf, send, recv = what
            return x_copy(out, recv_buf, send, recv, k)

        others = range(1, n_peer)
        pairs = list(zip(others[::2], others[1::2]))
        steps = [(group, i, ks) for group, order in ((now, (0, 1)), (later, (1, 0))) for i in order for ks in pairs]
        ahead = 2 * len(pairs)

        def gather_step(n):
            if n < len(steps):
                group, i, ks = steps[n]
                for k in ks:
                    gather(group[i][0], group[i][1], group[i][2], here.ep_to(k))

        def send_step(n):
            if n < len(steps):
                group, i, ks = steps[n]
                for k in ks:
                    copy_of(group[i], k).start()

        def sent_step(n):
            if n < len(steps):
                group, i, ks = steps[n]
                for k in ks:
                    copy_of(group[i], k).wait_send()

        def partner(what):
            gather(what[0], what[1], what[2], here.ep_to(0))
            copy_of(what, 0).start()

        gather_step(0)
        here.barrier(signals)
        send_step(0)
        gather_step(1)
        send_step(1)
        for c in weights:
            c.start()
        for i, what in enumerate(now):
            partner(what)
            gather(what[0], what[1], what[3], ep)
            if not i:
                gates()
        make_eye()

        spread = (('y', h_recv, h_sl, hs_s, hs_r), ('z', q_recv, q_sl, qs_s, qs_r))
        spread_next = (('y', h_next, hsl_next, ns_h_s, ns_h_r), ('z', q_next, qsl_next, ns_q_s, ns_q_r))

        def forward_own(spread, bufs):
            for (axis, _, sl, send, recv), buf in zip(spread, bufs):
                for k in range(1, grid):
                    slice_copy(axis, buf, sl, send, recv, ep, k).start()

        def forward(group, spread, i, p):
            axis, buf, sl, send, recv = spread[i]
            copy_of(group[i], p).wait_recv()
            for k in range(1, grid):
                slice_copy(axis, buf, sl, send, recv, here.ep_from(p), k).start()

        def forward_step(n):
            if n < len(steps):
                group, i, ks = steps[n]
                for k in ks:
                    forward(group, spread if group is now else spread_next, i, k)

        forward_own(spread, (h_recv, q_recv))
        for i in range(2):
            forward(now, spread, i, 0)
        for what in later:
            gather(what[0], what[1], what[2], ep)
        own_next = [pltpu.make_async_copy(what[2].at[block(ep), :], what[3].at[block(ep), :], lin.at[7 + i]) for i, what in enumerate(later)]
        for what in later:
            partner(what)
        middle, last = max(len(pairs) - 1, 0), max(ahead - 1, 0)
        for n in range(last + 1):
            gather_step(n + 2)
            sent_step(n)
            send_step(n + 2)
            forward_step(n)
            if n == middle:
                own_slice('y', h_recv, h_sl)
                copy_of(now[0], 0).wait_send()
                o_out = forward_part()
            if n == min(middle + 2, last):
                share_on(0)
            if n >= 2:
                gather_step(n + ahead)
            if n == min(1, last):
                forward_own(spread_next, (h_send_next, q_send_next))
                for i in range(2):
                    forward(later, spread_next, i, 0)
        send_step(ahead + 2)
        send_step(ahead + 3)
        for c in own_next:
            c.start()
        own_slice('z', q_recv, q_sl)
        copy_of(now[1], 0).wait_send()
    else:
        load_h, load_q = [pltpu.make_async_copy(src, dst, lin.at[2 + i * grid]) for i, (src, dst) in enumerate(((h_next, h_recv), (q_next, q_recv)))]
        load_slices = []
        for i, (axis, src, dst) in enumerate((('z', qsl_next, q_sl), ('y', hsl_next, h_sl))):
            for k in range(1, grid):
                part = rows_at(here.step(axis, k) * rows, rows, PACK)
                load_slices.append(pltpu.make_async_copy(src.at[part, :], dst.at[part, :], lin.at[2 + i * grid + k]))
        for c in [load_h] + weights + [load_q] + load_slices:
            c.start()
        here.barrier()
        back = list(zip(carry, carry_out))
        spread_unit = Spread(here, done_h, all_h, sp_s, sp_r)
        own_unit = pltpu.make_async_copy(done_h, all_h.at[here.dp], lin.at[1])
        spread_unit.send(0)
        spread_unit.send(1, (0,))

        def back_copy(j, k):
            src, dst = back[j]
            return remote(src_ref=src.at[block(here.ep_to(k)), :], dst_ref=dst.at[block(ep), :],
                          send_sem=ba_s.at[j, k], recv_sem=ba_r.at[j, k], device_id=(here.dp, here.ep_to(k)))

        def back_own(j):
            src, dst = back[j]
            return pltpu.make_async_copy(src.at[block(ep), :], dst.at[block(ep), :], ba_l.at[j])

        def send_back(j):
            for k in range(n_peer):
                back_copy(j, k).start()
            back_own(j).start()

        for j in range(len(carry)):
            send_back(j)
        make_eye()
        load_h.wait()
        o_out = forward_part()
        load_q.wait()
        own_slice('y', h_recv, h_sl)
        own_slice('z', q_recv, q_sl)
        own_unit.start()

    backward_pass()
    share_start(1)
    share_start(2)
    if first:
        sent_step(ahead)
        send_step(ahead + 4)
    else:
        share_on(0)
    untranspose(act, da_all, g_cols)
    untranspose(act_b, db_all, g_cols)
    share_on(1)
    share_on(2)
    if not first:
        spread_unit.receive(0)
        spread_unit.send(1, (1,))
    dh_pass()
    dh_out = pltpu.make_async_copy(dh_v, dh_h, loc.at[4])
    dh_out.start()
    if first:
        sent_step(ahead + 1)
        send_step(ahead + 5)
        forward_step(ahead)
        for k in range(1, grid):
            slices('z', q_recv, q_sl, qs_s, qs_r, k).wait_recv()
            slices('y', h_recv, h_sl, hs_s, hs_r, k).wait_recv()
    else:
        for c in load_slices:
            c.wait()
    share_done(1)
    weight_grad(0, da_all, h_sl)
    reduce_start(0)
    if not first:
        spread_unit.send(2, (0,))
    share_done(0)
    weight_grad(2, u_all, q_sl)
    share_done(2)
    weight_grad(1, db_all, h_sl)
    reduce_start(1)
    reduce_start(2)
    if first:
        forward_step(ahead + 1)
    else:
        spread_unit.receive(1)
    reduce_on(0)
    if not first:
        spread_unit.send(2, (1,))
    reduce_on(1)
    reduce_on(2)
    if first:
        for n in range(2, 5):
            forward_step(ahead + n)
    else:
        spread_unit.send(2, (2, 3))
    ends = reduce_end(0) + reduce_end(1) + reduce_end(2)
    if first:
        forward_step(ahead + 5)

    for j in range(3):
        for g in range(len(gathers)):
            share_t(g, j).wait_send()
            reduce_copy(g, j).wait_send()
    if first:
        for k in range(1, grid):
            for axis, buf, sl, send, recv in spread:
                slices(axis, buf, sl, send, recv, k).wait_send()
            for axis, buf, sl, send, recv in spread_next:
                slices(axis, buf, sl, send, recv, k).wait()
        for what in later:
            copy_of(what, 0).wait_send()
        for n in range(2, 6):
            sent_step(ahead + n)
        for c in own_next + [hid_out]:
            c.wait()
    else:
        for j in range(len(back)):
            for k in range(n_peer):
                back_copy(j, k).wait()
            back_own(j).wait()
        spread_unit.receive(2)
        for stage in range(3):
            spread_unit.sent(stage)
        own_unit.wait()
    for c in ends + [o_out, dh_out]:
        c.wait()


def expert_call(inputs, w_gate, w_up, w_down, expert, cap, grid, mesh_ep):
    first = expert == 0
    d_model = w_gate.shape[2]
    ff = w_gate.shape[1]
    rows = (mesh_ep if first else inputs[0].shape[0] // cap) * cap
    quarter, share = d_model // grid, ff // grid
    n_peer = rows // cap - 1
    chunk = min(1024, d_model)
    vmem, dma = pltpu.VMEM, pltpu.SemaphoreType.DMA
    hbm = pl.BlockSpec(memory_space=pl.ANY)
    on_chip = pl.BlockSpec(memory_space=pltpu.VMEM)
    row_block, slice_block = (rows, d_model), (grid * rows, quarter)
    scratch = [
        vmem(row_block, BF16), vmem(row_block, BF16),
        vmem((ff, d_model), BF16), vmem((ff, d_model), BF16), vmem((ff, d_model), BF16),
        vmem((ff, rows), F32), vmem((ff, rows), F32), vmem((ff, rows), F32),
        vmem((ff, grid * rows), BF16), vmem((ff, grid * rows), BF16), vmem((ff, grid * rows), BF16),
        vmem(slice_block, BF16), vmem(slice_block, BF16),
        vmem((3, ff, quarter), F32), vmem((3, 3, share, quarter), F32),
        vmem((rows, ff), BF16), vmem((rows, ff), BF16), vmem((rows, rows), BF16), dma((5 + 3 * UNITS,)),
    ] + [dma((grid,))] * 4 + [dma((6, 3))] * 4
    out = lambda shape, dtype=BF16: jax.ShapeDtypeStruct(shape, dtype)
    share_block = (UNITS, 3, share, quarter // UNITS)
    outs = [out(row_block), out(row_block), out(share_block, F32)]
    if first:
        tokens = inputs[-1].shape
        n_tok = tokens[0]
        scratch += [vmem((rows, i * n_tok), BF16) for i in (1, 2, 1, 2)] + [vmem(tokens, BF16)] * 3
        scratch += [vmem(row_block, BF16)] * 4 + [dma((n_peer,))] * 8 + [dma((grid,))] * 4 + [dma((9,))]
        operands = (*inputs, w_gate, w_up, w_down)
        outs += [out(row_block), out(row_block), out(slice_block), out(slice_block), out(tokens)] + [out((n_tok, LANES), F32)] * 3
        in_specs, out_specs = [on_chip] * 5 + [hbm] * 5, [hbm] * 8 + [on_chip] * 3
    else:
        h_next, q_next, hsl_next, qsl_next, *carry, done = inputs
        scratch += [vmem(row_block, BF16)] * 2 + [dma((2, n_peer))] * 2 + [dma((2,)), dma((2 + 2 * grid,))]
        scratch += [dma((UNITS, 15))] * 2
        operands = (h_next, q_next, hsl_next, qsl_next, w_gate, w_up, w_down, *carry, done)
        outs += [out(row_block), out(row_block), out((grid * grid,) + share_block, F32)]
        in_specs, out_specs = [hbm] * len(operands), [hbm] * len(outs)
    return pl.pallas_call(
        functools.partial(expert_kernel, (expert, grid, chunk, cap, first)),
        out_shape=tuple(outs), in_specs=in_specs, out_specs=tuple(out_specs), scratch_shapes=scratch,
        compiler_params=pltpu.CompilerParams(collective_id=expert, has_side_effects=True, vmem_limit_bytes=63 * 2 ** 20),
        cost_estimate=cost(2 * rows * d_model * ff * 9, STREAM),
    )(*operands)


def assemble_kernel(gate, up, down, *refs):
    n_pass = (len(refs) - 3) // 2 if len(refs) > 6 else 0
    outs = refs[-3 - n_pass:][:3]
    for j in range(n_pass):
        refs[-n_pass + j][ALL] = refs[j][ALL]
    grid, unit = gate.shape[1], gate.shape[-1]
    for c in range(grid):
        for i in range(UNITS):
            at = (c * UNITS + i) * unit
            outs[0][0, :, at:at + unit] = gate[0, c, i, 0]
            outs[1][0, :, at:at + unit] = up[0, c, i, 0]
            outs[2][0, :, at:at + unit] = down[c, 0, i, 0]


def assemble(gathered, expert, n_expert, into, through=()):
    grid, _, _, _, share, unit = gathered.shape
    cut = 2
    part = share // cut
    row_first = pl.BlockSpec((1, grid, UNITS, 1, part, unit), lambda r, h: (r, 0, 0, 0, h, 0))
    up_first = pl.BlockSpec((1, grid, UNITS, 1, part, unit), lambda r, h: (r, 0, 0, 1, h, 0))
    col_first = pl.BlockSpec((grid, 1, UNITS, 1, part, unit), lambda r, h: (0, r, 0, 2, h, 0))
    out_spec = pl.BlockSpec((1, part, grid * UNITS * unit), lambda r, h: (expert, r * cut + h, 0))
    whole = jax.ShapeDtypeStruct((n_expert, grid * share, grid * UNITS * unit), F32)
    strips = [pl.BlockSpec((x.shape[0] // (grid * cut), x.shape[1]), lambda r, h: (r * cut + h, 0)) for x in through]
    return pl.pallas_call(
        assemble_kernel, grid=(grid, cut), out_shape=(whole,) * 3 + tuple(jax.ShapeDtypeStruct(x.shape, x.dtype) for x in through),
        in_specs=[row_first, up_first, col_first] + strips + [pl.BlockSpec(memory_space=pl.ANY)] * len(into),
        out_specs=(out_spec,) * 3 + tuple(strips), input_output_aliases={3 + i: i for i in range(len(into))},
        compiler_params=pltpu.CompilerParams(vmem_limit_bytes=40 * 2 ** 20),
        cost_estimate=cost(1_000_000, 44_000_000),
    )(gathered, gathered, gathered, *through, *into)


def solution(mesh):
    n_ep = mesh.shape['ep']
    grid = round(mesh.shape['dp'] ** 0.5)
    tok_spec = P(('dp', 'ep'), None)
    row_spec = P(('dp', 'ep'))
    exp_spec = P('ep', None, None)

    def local_step(tok_x, tok_dy, exp_first, exp_second, eligible, slot_first, slot_second,
                   ln_weight, ln_bias, router, w_gate, w_up, w_down):
        n_local, _ = tok_x.shape
        n_exp = eligible.shape[1]
        local_exp = w_gate.shape[0]
        slot_cap = 3 * n_local // n_exp
        wg_t, wu_t = jnp.swapaxes(w_gate, 1, 2), jnp.swapaxes(w_up, 1, 2)

        columns = jnp.stack([exp_first, exp_second, slot_first, slot_second], axis=1)
        picks = jnp.stack([exp_first, exp_second, slot_first, slot_second])
        norm = jnp.stack([ln_weight, ln_bias]).astype(F32)
        router_t = jnp.pad(router.T, ((0, LANES - n_exp), (0, 0)))
        o, dh, share, *landed, hidden, stats, err_one, err_two = expert_call(
            (eligible, columns, picks, norm, router_t, tok_x, tok_dy), wg_t, wu_t, w_down, 0, slot_cap, grid, n_ep)
        o_next, dh_next, share, o, dh, held = expert_call((*landed, o, dh, share), wg_t, wu_t, w_down, 1, slot_cap, grid, n_ep)
        gathered_next = lax.all_gather(share, 'dp')
        held, out_tok, dx_tok, small = tail_call(
            held, o_next, dh_next, tok_x, tok_dy, hidden, o, dh, stats, err_one, err_two,
            norm, router_t, slot_cap, grid, local_exp + 1)
        gathered = [x.reshape((grid, grid) + share.shape) for x in (held, gathered_next)]
        d_router, d_ln_weight, d_ln_bias = small[:n_exp].T, small[PACK], small[PACK + 1]
        *weights, out_tok, dx_tok = assemble(gathered[0], 0, local_exp, (), (out_tok, dx_tok))
        weights = assemble(gathered[1], 1, local_exp, weights)
        dw_gate, dw_up, dw_down = jnp.swapaxes(weights[0], 1, 2), jnp.swapaxes(weights[1], 1, 2), weights[2]
        return out_tok, dx_tok, dw_gate, dw_up, dw_down, d_router, d_ln_weight, d_ln_bias

    return jax.shard_map(
        local_step, mesh=mesh,
        in_specs=(tok_spec, tok_spec, row_spec, row_spec, tok_spec, row_spec, row_spec,
                  P(), P(), P(), exp_spec, exp_spec, exp_spec),
        out_specs=(tok_spec, tok_spec, exp_spec, exp_spec, exp_spec, P(), P(), P()),
        check_vma=False)
```

```python
import functools

import jax
import jax.numpy as jnp
from jax import lax
from jax.experimental import pallas as pl
from jax.experimental.pallas import tpu as pltpu
from jax.sharding import PartitionSpec as P


LN_EPS = 1e-5
CORES = 2
UNITS = 4
NEAR, FAR = (1, 3), (3, 1)
LANES = 128
PACK = 16
STRIPS = 7
SMALL = 24
STREAM = 30_000_000
KEEP = {'keepdims': True}
F32 = jnp.float32
BF16 = jnp.bfloat16
ALL = Ellipsis
MESH_ID = pl.DeviceIdType.MESH
NT = (((1,), (1,)), ((), ()))


def ring_offsets(n_x):
    near = [d for d in (1, n_x - 1) if 0 < d < n_x]
    near = list(dict.fromkeys(near))
    far = [d for d in range(2, n_x - 1)]
    out = [(0, 1)]
    for group in (near, far):
        for core in range(CORES):
            out += [(d, core) for d in group]
    return out


class Place:
    def __init__(self, n_ep, grid):
        self.n_x, self.grid = n_ep // CORES, grid
        self.ep, self.dp = lax.axis_index('ep'), lax.axis_index('dp')
        self.x, self.core = self.ep // CORES, self.ep % CORES
        self.z, self.y = self.dp // grid, self.dp % grid
        self.offsets = ring_offsets(self.n_x)

    def ep_to(self, k):
        dx, dc = self.offsets[k]
        return lax.rem(self.x + dx, self.n_x) * CORES + lax.rem(self.core + dc, CORES)

    def ep_from(self, k):
        dx, dc = self.offsets[k]
        return lax.rem(self.x + (self.n_x - dx), self.n_x) * CORES + lax.rem(self.core + dc, CORES)

    def step(self, axis, k):
        here = self.y if axis == 'y' else self.z
        return lax.rem(here + k + self.grid, self.grid)

    def device(self, axis, k):
        if axis == 'y':
            return (self.z * self.grid + self.step('y', k), self.ep)
        return (self.step('z', k) * self.grid + self.y, self.ep)

    def flip(self, axis, bits):
        if axis == 'y':
            return (self.z * self.grid + (self.y ^ bits), self.ep)
        return ((self.z ^ bits) * self.grid + self.y, self.ep)

    def arrive(self):
        sem = pltpu.get_barrier_semaphore()
        peers = [(self.dp, self.ep_to(k)) for k in range(len(self.offsets))]
        for k in range(1, self.grid):
            peers += [self.device('y', k), self.device('z', k)]
        for peer in peers:
            pl.semaphore_signal(sem, inc=1, device_id=peer, device_id_type=MESH_ID)
        return len(peers)

    def barrier(self, signals=None):
        pl.semaphore_wait(pltpu.get_barrier_semaphore(), self.arrive() if signals is None else signals)


def widen(out, rows):
    out[ALL] = jnp.zeros_like(out)
    out[:rows.shape[0], :] = rows


def cost(flops, size):
    return pl.CostEstimate(flops=flops, bytes_accessed=size, transcendentals=0)


def rows_at(start, size, unit):
    return pl.ds(pl.multiple_of(start, unit), size)


class Spread:
    STAGES = [range(2 ** i - 1, 2 ** (i + 1) - 1) for i in range(UNITS)]

    def __init__(self, here, own, held, send, recv):
        self.here, self.own, self.held, self.sems = here, own, held, (send, recv)

    def plan(self, unit, index):
        axes = ('y', 'z') if unit < UNITS // 2 else ('z', 'y')
        one, two = FAR if unit % 2 else NEAR
        line = (0, one, two, one ^ two)
        if index < 1:
            return axes, (axes[0], one), (0, 0)
        if index < 3:
            return axes, (axes[0], two), (line[index - 1], 0)
        if index < 7:
            return axes, (axes[1], one), (line[index - 3], 0)
        return axes, (axes[1], two), (line[(index - 7) % 4], (0, one)[(index - 7) // 4])

    def copy(self, unit, index):
        axes, (axis, flip), offsets = self.plan(unit, index)
        at = dict(zip(axes, offsets))
        owner = (self.here.z ^ at['z']) * self.here.grid + (self.here.y ^ at['y'])
        held = self.held.at[owner, unit]
        source = self.own.at[unit] if self.own is not None and offsets == (0, 0) else held
        return pltpu.make_async_remote_copy(src_ref=source, dst_ref=held, send_sem=self.sems[0].at[unit, index],
                                            recv_sem=self.sems[1].at[unit, index], device_id=self.here.flip(axis, flip),
                                            device_id_type=MESH_ID)

    def each(self, stage, picks=None):
        ids = self.STAGES[stage]
        for index in ids if picks is None else [ids[p] for p in picks]:
            for unit in range(UNITS):
                yield self.copy(unit, index)

    def send(self, *what):
        for c in self.each(*what):
            c.start()

    def receive(self, *what):
        for c in self.each(*what):
            c.wait_recv()

    def sent(self, *what):
        for c in self.each(*what):
            c.wait_send()


def tail_kernel(grid, cap, *refs):
    refs = list(refs)
    take = lambda n: [refs.pop(0) for _ in range(n)]
    _, o_next_h, dh_next_h, x_h, dy_h, hid_h, o_h, dh_h, stats, err_one, err_two, lnw, router_in = take(13)
    held, out, dx, small = take(4)
    x_v, dy_v, hid_v, o_v, dh_v, sel_one, sel_two, grad_h, val, router = take(10)
    first, second, third, c_one, c_two, c_three = take(6)
    loc, sp_s, sp_r, ba_s, ba_r, s_one, r_one, s_two, r_two, s_three, r_three, s_four, r_four = take(13)
    n_tok, d_model = x_v.shape
    rows = o_next_h.shape[0]
    n_ep, _, width = first.shape
    wide = min(512, d_model)
    here = Place(n_ep, grid)
    n_peer = len(here.offsets)
    ep = here.ep
    remote = functools.partial(pltpu.make_async_remote_copy, device_id_type=MESH_ID)
    here.barrier()
    spread = Spread(here, None, held, sp_s, sp_r)
    spread.send(3)

    def block(e, base=0):
        return rows_at(base + e * cap, cap, PACK)

    pairs = ((o_next_h, o_v), (dh_next_h, dh_v))

    def back(j, k):
        src, dst = pairs[j]
        return remote(src_ref=src.at[block(here.ep_to(k)), :], dst_ref=dst.at[block(ep, rows), :],
                      send_sem=ba_s.at[j, k], recv_sem=ba_r.at[j, k], device_id=(here.dp, here.ep_to(k)))

    own = [pltpu.make_async_copy(src.at[block(ep), :], dst.at[block(ep, rows), :], loc.at[j]) for j, (src, dst) in enumerate(pairs)]
    for j in range(2):
        for k in range(n_peer):
            back(j, k).start()
        own[j].start()
    home = pl.ds(0, rows)
    loads = [pltpu.make_async_copy(src, dst, loc.at[2 + i]) for i, (src, dst) in enumerate((
        (x_h, x_v), (dy_h, dy_v), (hid_h, hid_v), (o_h, o_v.at[home, :]), (dh_h, dh_v.at[home, :])))]
    for c in loads:
        c.start()
    widen(router, router_in[ALL])
    slots = lax.broadcasted_iota(jnp.int32, (n_tok, 2 * rows), 1)
    sel_one[ALL] = (slots == stats[:, 4:5].astype(jnp.int32)).astype(F32).astype(BF16)
    sel_two[ALL] = (slots == stats[:, 5:6].astype(jnp.int32)).astype(F32).astype(BF16)
    gate_one, gate_two, mean, inv_std = [stats[:, i:i + 1] for i in range(4)]
    zero = jnp.zeros((n_tok, 1), F32)
    for c in loads:
        c.wait()
    own[0].wait()
    for k in range(n_peer):
        back(0, k).wait_recv()

    def mix(i, sums):
        cols = rows_at(i * wide, wide, LANES)
        one = jnp.dot(sel_one[ALL], o_v[:, cols], preferred_element_type=F32)
        two = jnp.dot(sel_two[ALL], o_v[:, cols], preferred_element_type=F32)
        dy = dy_v[:, cols].astype(F32)
        out[:, cols] = (x_v[:, cols].astype(F32) + (gate_one * one + gate_two * two)).astype(BF16)
        return sums[0] + jnp.sum(dy * one, axis=1, **KEEP), sums[1] + jnp.sum(dy * two, axis=1, **KEEP)

    dgate_one, dgate_two = lax.fori_loop(0, d_model // wide, mix, (zero, zero))
    d_logits = ((dgate_one * gate_one) * err_one[ALL] + (dgate_two * gate_two) * err_two[ALL]).astype(BF16)
    lanes = d_logits.shape[1]
    eye = (lax.broadcasted_iota(jnp.int32, (lanes, lanes), 0)
           == lax.broadcasted_iota(jnp.int32, (lanes, lanes), 1)).astype(F32).astype(BF16)
    d_logits_t = lax.dot_general(eye, d_logits, NT, preferred_element_type=F32).astype(BF16)[:PACK]
    sel_both = sel_one[ALL] + sel_two[ALL]
    row = lax.broadcasted_iota(jnp.int32, (8, wide), 0)
    own[1].wait()
    for k in range(n_peer):
        back(1, k).wait_recv()

    def gradient(i, sums):
        cols = rows_at(i * wide, wide, LANES)
        grad = (jnp.dot(d_logits, router[:, cols], preferred_element_type=F32)
                + jnp.dot(sel_both, dh_v[:, cols], preferred_element_type=F32))
        x_hat = (x_v[:, cols].astype(F32) - mean) * inv_std
        grad_h[:, cols] = grad
        val[:PACK, cols] = jnp.dot(d_logits_t, hid_v[:, cols], preferred_element_type=F32)
        d_weight = jnp.sum(grad * x_hat, axis=0, **KEEP)
        d_bias = jnp.sum(grad, axis=0, **KEEP)
        val[PACK:SMALL, cols] = jnp.where(row == 0, d_weight, jnp.where(row == 1, d_bias, 0.0))
        scaled = grad * lnw[:, cols]
        return sums[0] + jnp.sum(scaled, axis=1, **KEEP), sums[1] + jnp.sum(scaled * x_hat, axis=1, **KEEP)

    mean_one, mean_two = lax.fori_loop(0, d_model // wide, gradient, (zero, zero))
    mean_one, mean_two = mean_one / d_model, mean_two / d_model

    def part(e):
        return rows_at(e * width, width, LANES)

    def scatter(k):
        to = here.ep_to(k)
        return remote(src_ref=val.at[:, part(to)], dst_ref=first.at[ep], send_sem=s_one.at[k], recv_sem=r_one.at[k],
                      device_id=(here.dp, to))

    def along(axis, src, dst, send, recv, k):
        mine = here.y if axis == 'y' else here.z
        return remote(src_ref=src, dst_ref=dst.at[mine], send_sem=send.at[k], recv_sem=recv.at[k], device_id=here.device(axis, k))

    def gather(k):
        return remote(src_ref=c_three, dst_ref=small.at[:, part(ep)], send_sem=s_four.at[k], recv_sem=r_four.at[k],
                      device_id=(here.dp, here.ep_to(k)))

    def add_up(ref, n):
        total = ref[0]
        for i in range(1, n):
            total = total + ref[i]
        return total

    for k in range(n_peer):
        scatter(k).start()
    first[ep] = val[:, part(ep)]

    @pl.loop(0, d_model // wide)
    def _(i):
        cols = rows_at(i * wide, wide, LANES)
        x_hat = (x_v[:, cols].astype(F32) - mean) * inv_std
        step = inv_std * (grad_h[:, cols] * lnw[:, cols] - mean_one - x_hat * mean_two)
        dx[:, cols] = (dy_v[:, cols].astype(F32) + step).astype(BF16)

    for k in range(n_peer):
        scatter(k).wait_recv()
    c_one[ALL] = add_up(first, n_ep)
    second[here.y] = c_one[ALL]
    for k in range(1, grid):
        along('y', c_one, second, s_two, r_two, k).start()
    for k in range(1, grid):
        along('y', c_one, second, s_two, r_two, k).wait_recv()
    c_two[ALL] = add_up(second, grid)
    third[here.z] = c_two[ALL]
    for k in range(1, grid):
        along('z', c_two, third, s_three, r_three, k).start()
    for k in range(1, grid):
        along('z', c_two, third, s_three, r_three, k).wait_recv()
    c_three[ALL] = add_up(third, grid)
    for k in range(n_peer):
        gather(k).start()
    small[:, part(ep)] = c_three[ALL]
    for k in range(n_peer):
        gather(k).wait_recv()
    for k in range(n_peer):
        scatter(k).wait_send()
        gather(k).wait_send()
        back(0, k).wait_send()
        back(1, k).wait_send()
    for k in range(1, grid):
        along('y', c_one, second, s_two, r_two, k).wait_send()
        along('z', c_two, third, s_three, r_three, k).wait_send()
    spread.receive(3)
    spread.sent(3)


def tail_call(held, o_next, dh_next, tok_x, tok_dy, hidden, o, dh, stats, err_one, err_two, lnw, router, cap, grid, collective_id):
    vmem, dma = pltpu.VMEM, pltpu.SemaphoreType.DMA
    n_tok, d_model = tok_x.shape
    rows = o.shape[0]
    n_ep = rows // cap
    n_peer, width = n_ep - 1, d_model // n_ep
    hbm, on_chip = pl.BlockSpec(memory_space=pl.ANY), pl.BlockSpec(memory_space=pltpu.VMEM)
    tokens = jax.ShapeDtypeStruct((n_tok, d_model), BF16)
    peers, ring = dma((n_peer,)), dma((grid,))
    deep, both = dma((UNITS, 15)), dma((2, n_peer))
    return pl.pallas_call(
        functools.partial(tail_kernel, grid, cap),
        out_shape=(jax.ShapeDtypeStruct(held.shape, F32), tokens, tokens, jax.ShapeDtypeStruct((SMALL, d_model), F32)),
        in_specs=[hbm] * 8 + [on_chip] * 5, out_specs=(hbm, on_chip, on_chip, on_chip), input_output_aliases={0: 0},
        scratch_shapes=[vmem((n_tok, d_model), BF16)] * 3 + [vmem((2 * rows, d_model), BF16)] * 2
        + [vmem((n_tok, 2 * rows), BF16)] * 2 + [vmem((n_tok, d_model), F32), vmem((SMALL, d_model), F32), vmem((LANES, d_model), BF16)]
        + [vmem((n_ep, SMALL, width), F32), vmem((grid, SMALL, width), F32), vmem((grid, SMALL, width), F32)] + [vmem((SMALL, width), F32)] * 3
        + [dma((7,)), deep, deep, both, both,
           peers, peers, ring, ring, ring, ring, peers, peers],
        compiler_params=pltpu.CompilerParams(collective_id=collective_id, has_side_effects=True, vmem_limit_bytes=50 * 2 ** 20),
        cost_estimate=cost(10_000_000_000, STREAM),
        name='tail',
    )(held, o_next, dh_next, tok_x, tok_dy, hidden, o, dh, stats, err_one, err_two, lnw, router)


def expert_kernel(dims, *refs):
    expert, grid, chunk, cap, first = dims
    refs = list(refs)
    take = lambda n: [refs.pop(0) for _ in range(n)]
    if first:
        marks, *lines = take(1 + UNITS)
        lnw, lnb, router_in, x_h, dy_h, wg_h, wu_h, wd_h = take(8)
        o_h, dh_h, sh_h, h_next, q_next, hsl_next, qsl_next, hid_h, all_h, stats, err_one, err_two = take(12)
    else:
        h_next, q_next, hsl_next, qsl_next, wg_h, wu_h, wd_h, *carry = take(9)
        done_h, _ = take(2)
        o_h, dh_h, sh_h, *carry_out = take(5)
        all_h, = take(1)
    h_recv, q_recv, wg, wu, wd, a_t, b_t, d_t, u_all, da_all, db_all, h_sl, q_sl, dw, rsb, act, act_b, eye = take(18)
    loc, hs_s, hs_r, qs_s, qs_r, ga_s, ga_r, rs_s, rs_r = take(9)
    if first:
        sel_h, sel_q, sel_h_next, sel_q_next, hidden, grad_one, grad_two, h_send, q_send, h_send_next, q_send_next, router, wide_table = take(13)
        xh_s, xh_r, xq_s, xq_r, nh_s, nh_r, nq_s, nq_r, ns_h_s, ns_h_r, ns_q_s, ns_q_r, lin, sp_s, sp_r = take(15)
        o_v, dh_v = h_send, q_send
    else:
        o_v, dh_v = take(2)
        ba_s, ba_r, ba_l, lin, sp_s, sp_r = take(6)
    rows, d_model = h_recv.shape
    ff = wg.shape[0]
    quarter = d_model // grid
    share = ff // grid
    here = Place(rows // cap, grid)
    n_peer = len(here.offsets)
    ep = here.ep
    remote = functools.partial(pltpu.make_async_remote_copy, device_id_type=MESH_ID)
    wide = chunk // 2

    def spot(axis):
        return here.y if axis == 'y' else here.z

    def block(e):
        return rows_at(e * cap, cap, PACK)

    weights = [pltpu.make_async_copy(src.at[expert], dst, loc.at[i]) for i, (src, dst) in enumerate(((wg_h, wg), (wu_h, wu), (wd_h, wd)))]

    def x_copy(src, dst, send, recv, k):
        return remote(src_ref=src.at[block(here.ep_to(k)), :], dst_ref=dst.at[block(ep), :],
                      send_sem=send.at[k], recv_sem=recv.at[k], device_id=(here.dp, here.ep_to(k)))

    def slice_copy(axis, buf, sl, send, recv, src_ep, k):
        return remote(src_ref=buf.at[block(src_ep), rows_at(here.step(axis, k) * quarter, quarter, LANES)],
                      dst_ref=sl.at[rows_at(spot(axis) * rows + src_ep * cap, cap, PACK), :],
                      send_sem=send.at[k], recv_sem=recv.at[k], device_id=here.device(axis, k))

    def slices(axis, buf, sl, send, recv, k):
        return remote(src_ref=buf.at[:, pl.ds(0, quarter)], dst_ref=sl.at[pl.ds(0, rows), :],
                      send_sem=send.at[k], recv_sem=recv.at[k], device_id=here.device(axis, k))

    half = ff // 2
    halves = ((pl.ds(0, half), NEAR), (pl.ds(half, half), FAR))
    gathers = [(ref, part, axis, *order) for ref, axis in ((u_all, 'z'), (da_all, 'y'), (db_all, 'y')) for part, order in halves]

    def share_t(g, j):
        ref, part, axis, one, two = gathers[g]
        flip = two if j else one
        owner = spot(axis) ^ (one if j == 2 else 0)
        view = ref.at[part, rows_at(owner * rows, rows, LANES)]
        return remote(src_ref=view, dst_ref=view, send_sem=ga_s.at[g, j], recv_sem=ga_r.at[g, j], device_id=here.flip(axis, flip))

    def share_start(t):
        for g in (2 * t, 2 * t + 1):
            share_t(g, 0).start()

    def share_on(t):
        for g in (2 * t, 2 * t + 1):
            share_t(g, 0).wait_recv()
            for j in (1, 2):
                share_t(g, j).start()

    def share_done(t):
        for g in (2 * t, 2 * t + 1):
            for j in (1, 2):
                share_t(g, j).wait_recv()

    wing = quarter // 2
    wings = ((pl.ds(0, wing), NEAR), (pl.ds(wing, wing), FAR))
    reduces = [(t, cols, axis, *order) for t, axis in enumerate('zzy') for cols, order in wings]

    def part_at(i):
        return rows_at(i * share, share, 8)

    def reduce_copy(r, j):
        t, cols, axis, one, two = reduces[r]
        here_at = spot(axis)
        flip, chunk_at = ((one, here_at ^ one), (one, here_at ^ one ^ two), (two, here_at ^ two))[j]
        return remote(src_ref=dw.at[t, part_at(chunk_at), cols], dst_ref=rsb.at[t, j, :, cols],
                      send_sem=rs_s.at[r, j], recv_sem=rs_r.at[r, j], device_id=here.flip(axis, flip))

    def reduce_start(t):
        for r in (2 * t, 2 * t + 1):
            for j in (0, 1):
                reduce_copy(r, j).start()

    def reduce_on(t):
        for r in (2 * t, 2 * t + 1):
            _, cols, axis, _, two = reduces[r]
            reduce_copy(r, 0).wait_recv()
            reduce_copy(r, 1).wait_recv()
            on = part_at(spot(axis) ^ two)
            dw[t, on, cols] = dw[t, on, cols] + rsb[t, 1, :, cols]
            reduce_copy(r, 2).start()

    def reduce_end(t):
        axis = 'zzy'[t]
        for r in (2 * t, 2 * t + 1):
            reduce_copy(r, 2).wait_recv()
        rsb[t, 0] = dw[t, part_at(spot(axis)), :] + rsb[t, 0] + rsb[t, 2]
        unit = quarter // UNITS
        outs = [pltpu.make_async_copy(rsb.at[t, 0, :, pl.ds(i * unit, unit)], sh_h.at[i, t], loc.at[5 + t * UNITS + i]) for i in range(UNITS)]
        for c in outs:
            c.start()
        return outs

    def own_slice(axis, buf, sl):
        sl[rows_at(spot(axis) * rows, rows, PACK), :] = buf[:, rows_at(spot(axis) * quarter, quarter, LANES)]

    strip = ff // STRIPS
    u_cols = rows_at(here.z * rows, rows, LANES)
    g_cols = rows_at(here.y * rows, rows, LANES)

    def forward_pass():
        a_t[ALL] = jnp.zeros_like(a_t)
        b_t[ALL] = jnp.zeros_like(b_t)

        @pl.loop(0, d_model // chunk)
        def _(i):
            cols = rows_at(i * chunk, chunk, LANES)
            a_t[ALL] += lax.dot_general(wg[:, cols], h_recv[:, cols], NT, preferred_element_type=F32)
            b_t[ALL] += lax.dot_general(wu[:, cols], h_recv[:, cols], NT, preferred_element_type=F32)

        @pl.loop(0, STRIPS)
        def _(i):
            r = rows_at(i * strip, strip, PACK)
            a = a_t[r, :]
            u_all[r, u_cols] = (a * jax.nn.sigmoid(a) * b_t[r, :]).astype(BF16)

    def backward_pass():
        d_t[ALL] = jnp.zeros_like(d_t)

        @pl.loop(0, d_model // chunk)
        def _(i):
            cols = rows_at(i * chunk, chunk, LANES)
            d_t[ALL] += lax.dot_general(wd[:, cols], q_recv[:, cols], NT, preferred_element_type=F32)

        @pl.loop(0, STRIPS)
        def _(i):
            r = rows_at(i * strip, strip, PACK)
            a, b, du = a_t[r, :], b_t[r, :], d_t[r, :]
            sig = jax.nn.sigmoid(a)
            silu = a * sig
            da_all[r, g_cols] = (du * b * sig * (1.0 + a * (1.0 - sig))).astype(BF16)
            db_all[r, g_cols] = (du * silu).astype(BF16)

    def untranspose(out, ref, cols):
        out[ALL] = lax.dot_general(eye[ALL], ref[:, cols], NT, preferred_element_type=F32).astype(BF16)

    def o_pass():
        @pl.loop(0, d_model // wide)
        def _(i):
            cols = rows_at(i * wide, wide, LANES)
            o_v[:, cols] = jnp.dot(act[ALL], wd[:, cols], preferred_element_type=F32).astype(BF16)

    def dh_pass():
        @pl.loop(0, d_model // wide)
        def _(i):
            cols = rows_at(i * wide, wide, LANES)
            dh_v[:, cols] = (jnp.dot(act[ALL], wg[:, cols], preferred_element_type=F32)
                             + jnp.dot(act_b[ALL], wu[:, cols], preferred_element_type=F32)).astype(BF16)

    def weight_grad(t, left, right):
        @pl.loop(0, quarter // wide)
        def _(i):
            cols = rows_at(i * wide, wide, LANES)
            dw[t, :, cols] = jnp.dot(left[ALL], right[:, cols], preferred_element_type=F32)

    def forward_part():
        weights[0].wait()
        weights[1].wait()
        forward_pass()
        share_start(0)
        untranspose(act, u_all, u_cols)
        weights[2].wait()
        o_pass()
        o_out = pltpu.make_async_copy(o_v, o_h, loc.at[3])
        o_out.start()
        return o_out

    def make_eye():
        eye[ALL] = (lax.broadcasted_iota(jnp.int32, (rows, rows), 0)
                    == lax.broadcasted_iota(jnp.int32, (rows, rows), 1)).astype(F32).astype(BF16)

    if first:
        inputs = [pltpu.make_async_copy(src, dst, lin.at[i]) for i, (src, dst) in enumerate(((x_h, hidden), (dy_h, grad_two)))]
        n_tok = hidden.shape[0]
        lane = lax.broadcasted_iota(jnp.int32, stats.shape, 1)
        n_exp = router_in.shape[0]
        for c in inputs:
            c.start()
        signals = here.arrive()
        make_eye()

        def place(ids, slots):
            local = jnp.bitwise_and(ids, 1)
            return jnp.where(slots >= 0, local * rows + jnp.right_shift(ids, 1) * cap + slots, -1)

        for e, (one, two) in enumerate(((sel_h, sel_q), (sel_h_next, sel_q_next))):
            slot = lax.broadcasted_iota(jnp.int32, one.shape, 0) + e * rows
            hits = [(slot == place(lines[i][ALL], lines[i + 2][ALL])).astype(F32).astype(BF16) for i in range(2)]
            one[ALL] = hits[0] + hits[1]
            for i in range(2):
                two[:, i * n_tok:(i + 1) * n_tok] = hits[i]
        inputs[0].wait()
        strip_rows = 2 * PACK

        @pl.loop(0, n_tok // strip_rows)
        def _(i):
            r = rows_at(i * strip_rows, strip_rows, PACK)
            x = hidden[r, :].astype(F32)
            mean = jnp.mean(x, axis=1, **KEEP)
            centered = x - mean
            inv_std = lax.rsqrt(jnp.mean(centered * centered, axis=1, **KEEP) + LN_EPS)
            hidden[r, :] = (centered * inv_std * lnw[ALL] + lnb[ALL]).astype(BF16)
            at = lane[:strip_rows]
            stats[r, :] = jnp.where(at == 2, mean, jnp.where(at == 3, inv_std, 0.0))

        hid_out = pltpu.make_async_copy(hidden, hid_h, lin.at[2])
        hid_out.start()

        def gates():
            widen(router, router_in[ALL])
            row = lax.broadcasted_iota(jnp.int32, marks.shape, 0)
            index_rows = sum(jnp.where(row == i, lines[i][ALL], 0) for i in range(UNITS))
            widen(wide_table, jnp.concatenate([marks[ALL], index_rows]).astype(F32).astype(BF16))
            columns = lax.dot_general(eye[:n_tok, :n_tok], wide_table[ALL], NT, preferred_element_type=F32)
            logits = lax.dot_general(hidden[ALL], router[ALL], NT, preferred_element_type=F32)
            ints = [columns[:, n_exp + i:n_exp + i + 1].astype(jnp.int32) for i in range(UNITS)]
            choices, allowed = ints[:2], jnp.logical_and(columns > 0, lane < n_exp)
            found = [place(*ints[i::2]) for i in range(2)]
            found = [value.astype(F32) for value in found]
            for choice, err in zip(choices, (err_one, err_two)):
                masked = jnp.where(allowed, logits, -1e30)
                weight = jnp.exp(masked - jnp.max(masked, axis=1, **KEEP))
                prob = weight / jnp.sum(weight, axis=1, **KEEP)
                pick = (lane == choice).astype(F32)
                found.append(jnp.sum(prob * pick, axis=1, **KEEP))
                err[ALL] = pick - prob
                allowed = jnp.logical_and(allowed, lane != choice)
            total = stats[ALL]
            for i, value in zip((4, 5, 0, 1), found):
                total = jnp.where(lane == i, value, total)
            stats[ALL] = total
            inputs[1].wait()

            @pl.loop(0, d_model // wide)
            def _(i):
                cols = rows_at(i * wide, wide, LANES)
                dy = grad_two[:, cols].astype(F32)
                grad_one[:, cols] = (stats[:, 0:1] * dy).astype(BF16)
                grad_two[:, cols] = (stats[:, 1:2] * dy).astype(BF16)

        def gather(sel, source, out, e):
            @pl.loop(0, d_model // chunk)
            def _(i):
                cols = rows_at(i * chunk, chunk, LANES)
                total = jnp.dot(sel[block(e), :n_tok], source[0][:, cols], preferred_element_type=F32)
                for j in range(1, len(source)):
                    total += jnp.dot(sel[block(e), j * n_tok:(j + 1) * n_tok], source[j][:, cols], preferred_element_type=F32)
                out[block(e), cols] = total.astype(BF16)

        rows_h, rows_q = (hidden,), (grad_one, grad_two)
        now = ((sel_h, rows_h, h_send, h_recv, xh_s, xh_r), (sel_q, rows_q, q_send, q_recv, xq_s, xq_r))
        later = ((sel_h_next, rows_h, h_send_next, h_next, nh_s, nh_r), (sel_q_next, rows_q, q_send_next, q_next, nq_s, nq_r))

        def copy_of(what, k):
            _, _, out, recv_buf, send, recv = what
            return x_copy(out, recv_buf, send, recv, k)

        others = range(1, n_peer)
        pairs = list(zip(others[::2], others[1::2]))
        steps = [(group, i, ks) for group, order in ((now, (0, 1)), (later, (1, 0))) for i in order for ks in pairs]
        ahead = 2 * len(pairs)

        def gather_step(n):
            if n < len(steps):
                group, i, ks = steps[n]
                for k in ks:
                    gather(group[i][0], group[i][1], group[i][2], here.ep_to(k))

        def send_step(n):
            if n < len(steps):
                group, i, ks = steps[n]
                for k in ks:
                    copy_of(group[i], k).start()

        def sent_step(n):
            if n < len(steps):
                group, i, ks = steps[n]
                for k in ks:
                    copy_of(group[i], k).wait_send()

        def partner(what):
            gather(what[0], what[1], what[2], here.ep_to(0))
            copy_of(what, 0).start()

        gather_step(0)
        here.barrier(signals)
        send_step(0)
        gather_step(1)
        send_step(1)
        for c in weights:
            c.start()
        for i, what in enumerate(now):
            partner(what)
            gather(what[0], what[1], what[3], ep)
            if not i:
                gates()
        spread = (('y', h_recv, h_sl, hs_s, hs_r), ('z', q_recv, q_sl, qs_s, qs_r))
        spread_next = (('y', h_next, hsl_next, ns_h_s, ns_h_r), ('z', q_next, qsl_next, ns_q_s, ns_q_r))

        def forward_own(spread, bufs):
            for (axis, _, sl, send, recv), buf in zip(spread, bufs):
                for k in range(1, grid):
                    slice_copy(axis, buf, sl, send, recv, ep, k).start()

        def forward(group, spread, i, p):
            axis, buf, sl, send, recv = spread[i]
            copy_of(group[i], p).wait_recv()
            for k in range(1, grid):
                slice_copy(axis, buf, sl, send, recv, here.ep_from(p), k).start()

        def forward_step(n):
            if n < len(steps):
                group, i, ks = steps[n]
                for k in ks:
                    forward(group, spread if group is now else spread_next, i, k)

        forward_own(spread, (h_recv, q_recv))
        for i in range(2):
            forward(now, spread, i, 0)
        for what in later:
            gather(what[0], what[1], what[2], ep)
        own_next = [pltpu.make_async_copy(what[2].at[block(ep), :], what[3].at[block(ep), :], lin.at[7 + i]) for i, what in enumerate(later)]
        for what in later:
            partner(what)
        middle, last = max(len(pairs) - 1, 0), max(ahead - 1, 0)
        for n in range(last + 1):
            gather_step(n + 2)
            sent_step(n)
            send_step(n + 2)
            forward_step(n)
            if n == middle:
                own_slice('y', h_recv, h_sl)
                copy_of(now[0], 0).wait_send()
                o_out = forward_part()
            if n == min(middle + 2, last):
                share_on(0)
            if n >= 2:
                gather_step(n + ahead)
            if n == min(1, last):
                forward_own(spread_next, (h_send_next, q_send_next))
                for i in range(2):
                    forward(later, spread_next, i, 0)
        send_step(ahead + 2)
        send_step(ahead + 3)
        for c in own_next:
            c.start()
        own_slice('z', q_recv, q_sl)
        copy_of(now[1], 0).wait_send()
    else:
        load_h, load_q = [pltpu.make_async_copy(src, dst, lin.at[2 + i * grid]) for i, (src, dst) in enumerate(((h_next, h_recv), (q_next, q_recv)))]
        load_slices = []
        for i, (axis, src, dst) in enumerate((('z', qsl_next, q_sl), ('y', hsl_next, h_sl))):
            for k in range(1, grid):
                part = rows_at(here.step(axis, k) * rows, rows, PACK)
                load_slices.append(pltpu.make_async_copy(src.at[part, :], dst.at[part, :], lin.at[2 + i * grid + k]))
        for c in [load_h] + weights + [load_q] + load_slices:
            c.start()
        here.barrier()
        back = list(zip(carry, carry_out))
        spread_unit = Spread(here, done_h, all_h, sp_s, sp_r)
        own_unit = pltpu.make_async_copy(done_h, all_h.at[here.dp], lin.at[1])
        spread_unit.send(1, (1,))
        spread_unit.send(2, (0,))

        def back_copy(j, k):
            src, dst = back[j]
            return remote(src_ref=src.at[block(here.ep_to(k)), :], dst_ref=dst.at[block(ep), :],
                          send_sem=ba_s.at[j, k], recv_sem=ba_r.at[j, k], device_id=(here.dp, here.ep_to(k)))

        def back_own(j):
            src, dst = back[j]
            return pltpu.make_async_copy(src.at[block(ep), :], dst.at[block(ep), :], ba_l.at[j])

        def send_back(j):
            for k in range(n_peer):
                back_copy(j, k).start()
            back_own(j).start()

        for j in range(len(carry)):
            send_back(j)
        make_eye()
        load_h.wait()
        o_out = forward_part()
        load_q.wait()
        own_slice('y', h_recv, h_sl)
        own_slice('z', q_recv, q_sl)
        own_unit.start()

    backward_pass()
    share_start(1)
    share_start(2)
    if first:
        sent_step(ahead)
        send_step(ahead + 4)
    else:
        share_on(0)
    untranspose(act, da_all, g_cols)
    untranspose(act_b, db_all, g_cols)
    share_on(1)
    share_on(2)
    dh_pass()
    dh_out = pltpu.make_async_copy(dh_v, dh_h, loc.at[4])
    dh_out.start()
    if first:
        sent_step(ahead + 1)
        send_step(ahead + 5)
        forward_step(ahead)
        for k in range(1, grid):
            slices('z', q_recv, q_sl, qs_s, qs_r, k).wait_recv()
            slices('y', h_recv, h_sl, hs_s, hs_r, k).wait_recv()
    else:
        for c in load_slices:
            c.wait()
    share_done(1)
    weight_grad(0, da_all, h_sl)
    reduce_start(0)
    share_done(0)
    weight_grad(2, u_all, q_sl)
    share_done(2)
    weight_grad(1, db_all, h_sl)
    reduce_start(1)
    reduce_start(2)
    if first:
        forward_step(ahead + 1)
    else:
        spread_unit.receive(1, (1,))
    reduce_on(0)
    if not first:
        spread_unit.send(2, (1,))
    reduce_on(1)
    reduce_on(2)
    if first:
        for n in range(2, 5):
            forward_step(ahead + n)
    else:
        spread_unit.send(2, (2, 3))
    ends = reduce_end(0) + reduce_end(1) + reduce_end(2)
    if first:
        for c in ends:
            c.wait()
        ends = []
        spread_unit = Spread(here, sh_h, all_h, sp_s, sp_r)
        spread_unit.send(0)
        spread_unit.send(1, (0,))
        forward_step(ahead + 5)

    for j in range(3):
        for g in range(len(gathers)):
            share_t(g, j).wait_send()
            reduce_copy(g, j).wait_send()
    if first:
        for k in range(1, grid):
            for axis, buf, sl, send, recv in spread:
                slices(axis, buf, sl, send, recv, k).wait_send()
            for axis, buf, sl, send, recv in spread_next:
                slices(axis, buf, sl, send, recv, k).wait()
        for what in later:
            copy_of(what, 0).wait_send()
        for n in range(2, 6):
            sent_step(ahead + n)
        for c in own_next + [hid_out]:
            c.wait()
        for stage, picks in enumerate((None, (0,))):
            spread_unit.receive(stage, picks)
            spread_unit.sent(stage, picks)
    else:
        for j in range(len(back)):
            for k in range(n_peer):
                back_copy(j, k).wait()
            back_own(j).wait()
        spread_unit.receive(2)
        spread_unit.sent(1, (1,))
        spread_unit.sent(2)
        own_unit.wait()
    for c in ends + [o_out, dh_out]:
        c.wait()


def expert_call(inputs, w_gate, w_up, w_down, expert, cap, grid, mesh_ep):
    first = expert == 0
    d_model = w_gate.shape[2]
    ff = w_gate.shape[1]
    rows = (mesh_ep if first else inputs[0].shape[0] // cap) * cap
    quarter, share = d_model // grid, ff // grid
    n_peer = rows // cap - 1
    chunk = min(1024, d_model)
    vmem, dma = pltpu.VMEM, pltpu.SemaphoreType.DMA
    hbm = pl.BlockSpec(memory_space=pl.ANY)
    on_chip = pl.BlockSpec(memory_space=pltpu.VMEM)
    row_block, slice_block = (rows, d_model), (grid * rows, quarter)
    scratch = [
        vmem(row_block, BF16), vmem(row_block, BF16),
        vmem((ff, d_model), BF16), vmem((ff, d_model), BF16), vmem((ff, d_model), BF16),
        vmem((ff, rows), F32), vmem((ff, rows), F32), vmem((ff, rows), F32),
        vmem((ff, grid * rows), BF16), vmem((ff, grid * rows), BF16), vmem((ff, grid * rows), BF16),
        vmem(slice_block, BF16), vmem(slice_block, BF16),
        vmem((3, ff, quarter), F32), vmem((3, 3, share, quarter), F32),
        vmem((rows, ff), BF16), vmem((rows, ff), BF16), vmem((rows, rows), BF16), dma((5 + 3 * UNITS,)),
    ] + [dma((grid,))] * 4 + [dma((6, 3))] * 4
    out = lambda shape, dtype=BF16: jax.ShapeDtypeStruct(shape, dtype)
    share_block = (UNITS, 3, share, quarter // UNITS)
    outs = [out(row_block), out(row_block), out(share_block, F32)]
    if first:
        tokens = inputs[-1].shape
        n_tok = tokens[0]
        scratch += [vmem((rows, i * n_tok), BF16) for i in (1, 2, 1, 2)] + [vmem(tokens, BF16)] * 3
        scratch += [vmem(row_block, BF16)] * 4 + [vmem((LANES, d_model), BF16), vmem((LANES, n_tok), BF16)] + [dma((n_peer,))] * 8 + [dma((grid,))] * 4 + [dma((9,))] + [dma((UNITS, 15))] * 2
        operands = (*inputs, w_gate, w_up, w_down)
        outs += [out(row_block), out(row_block), out(slice_block), out(slice_block), out(tokens)]
        outs += [out((grid * grid,) + share_block, F32)] + [out((n_tok, LANES), F32)] * 3
        aliases = {}
        in_specs, out_specs = [on_chip] * 8 + [hbm] * 5, [hbm] * 9 + [on_chip] * 3
    else:
        h_next, q_next, hsl_next, qsl_next, *carry, done, held = inputs
        scratch += [vmem(row_block, BF16)] * 2 + [dma((2, n_peer))] * 2 + [dma((2,)), dma((2 + 2 * grid,))]
        scratch += [dma((UNITS, 15))] * 2
        operands = (h_next, q_next, hsl_next, qsl_next, w_gate, w_up, w_down, *carry, done, held)
        outs += [out(row_block), out(row_block), out((grid * grid,) + share_block, F32)]
        in_specs, out_specs = [hbm] * len(operands), [hbm] * len(outs)
        aliases = {len(operands) - 1: len(outs) - 1}
    return pl.pallas_call(
        functools.partial(expert_kernel, (expert, grid, chunk, cap, first)),
        out_shape=tuple(outs), in_specs=in_specs, out_specs=tuple(out_specs), scratch_shapes=scratch, input_output_aliases=aliases,
        compiler_params=pltpu.CompilerParams(collective_id=expert, has_side_effects=True, vmem_limit_bytes=63 * 2 ** 20),
        cost_estimate=cost(2 * rows * d_model * ff * 9, STREAM),
    )(*operands)


def assemble_kernel(gate, up, down, *refs):
    n_pass = (len(refs) - 3) // 2 if len(refs) > 6 else 0
    outs = refs[-3 - n_pass:][:3]
    for j in range(n_pass):
        refs[-n_pass + j][ALL] = refs[j][ALL]
    grid, unit = gate.shape[1], gate.shape[-1]
    for c in range(grid):
        for i in range(UNITS):
            at = (c * UNITS + i) * unit
            outs[0][0, :, at:at + unit] = gate[0, c, i, 0]
            outs[1][0, :, at:at + unit] = up[0, c, i, 0]
            outs[2][0, :, at:at + unit] = down[c, 0, i, 0]


def assemble(gathered, expert, n_expert, into, through=()):
    grid, _, _, _, share, unit = gathered.shape
    cut = 2
    part = share // cut
    row_first = pl.BlockSpec((1, grid, UNITS, 1, part, unit), lambda r, h: (r, 0, 0, 0, h, 0))
    up_first = pl.BlockSpec((1, grid, UNITS, 1, part, unit), lambda r, h: (r, 0, 0, 1, h, 0))
    col_first = pl.BlockSpec((grid, 1, UNITS, 1, part, unit), lambda r, h: (0, r, 0, 2, h, 0))
    out_spec = pl.BlockSpec((1, part, grid * UNITS * unit), lambda r, h: (expert, r * cut + h, 0))
    whole = jax.ShapeDtypeStruct((n_expert, grid * share, grid * UNITS * unit), F32)
    strips = [pl.BlockSpec((x.shape[0] // (grid * cut), x.shape[1]), lambda r, h: (r * cut + h, 0)) for x in through]
    return pl.pallas_call(
        assemble_kernel, grid=(grid, cut), out_shape=(whole,) * 3 + tuple(jax.ShapeDtypeStruct(x.shape, x.dtype) for x in through),
        in_specs=[row_first, up_first, col_first] + strips + [pl.BlockSpec(memory_space=pl.ANY)] * len(into),
        out_specs=(out_spec,) * 3 + tuple(strips), input_output_aliases={3 + i: i for i in range(len(into))},
        compiler_params=pltpu.CompilerParams(vmem_limit_bytes=40 * 2 ** 20),
        cost_estimate=cost(1_000_000, 44_000_000),
    )(gathered, gathered, gathered, *through, *into)


def solution(mesh):
    n_ep = mesh.shape['ep']
    grid = round(mesh.shape['dp'] ** 0.5)
    tok_spec = P(('dp', 'ep'), None)
    row_spec = P(('dp', 'ep'))
    exp_spec = P('ep', None, None)

    def local_step(tok_x, tok_dy, exp_first, exp_second, eligible, slot_first, slot_second,
                   ln_weight, ln_bias, router, w_gate, w_up, w_down):
        n_local, _ = tok_x.shape
        n_exp = eligible.shape[1]
        local_exp = w_gate.shape[0]
        slot_cap = 3 * n_local // n_exp
        wg_t, wu_t = jnp.swapaxes(w_gate, 1, 2), jnp.swapaxes(w_up, 1, 2)

        lines = [x[None] for x in (exp_first, exp_second, slot_first, slot_second)]
        lnw, lnb = ln_weight.astype(F32)[None], ln_bias.astype(F32)[None]
        router_t = router.T
        o, dh, share, *landed, hidden, held, stats, err_one, err_two = expert_call(
            (eligible.T, *lines, lnw, lnb, router_t, tok_x, tok_dy), wg_t, wu_t, w_down, 0, slot_cap, grid, n_ep)
        o_next, dh_next, share, o, dh, held = expert_call((*landed, o, dh, share, held), wg_t, wu_t, w_down, 1, slot_cap, grid, n_ep)
        gathered_next = lax.all_gather(share, 'dp')
        held, out_tok, dx_tok, small = tail_call(
            held, o_next, dh_next, tok_x, tok_dy, hidden, o, dh, stats, err_one, err_two,
            lnw, router_t, slot_cap, grid, local_exp + 1)
        gathered = [x.reshape((grid, grid) + share.shape) for x in (held, gathered_next)]
        d_router, d_ln_weight, d_ln_bias = small[:n_exp].T, small[PACK], small[PACK + 1]
        *weights, out_tok, dx_tok = assemble(gathered[0], 0, local_exp, (), (out_tok, dx_tok))
        weights = assemble(gathered[1], 1, local_exp, weights)
        dw_gate, dw_up, dw_down = jnp.swapaxes(weights[0], 1, 2), jnp.swapaxes(weights[1], 1, 2), weights[2]
        return out_tok, dx_tok, dw_gate, dw_up, dw_down, d_router, d_ln_weight, d_ln_bias

    return jax.shard_map(
        local_step, mesh=mesh,
        in_specs=(tok_spec, tok_spec, row_spec, row_spec, tok_spec, row_spec, row_spec,
                  P(), P(), P(), exp_spec, exp_spec, exp_spec),
        out_specs=(tok_spec, tok_spec, exp_spec, exp_spec, exp_spec, P(), P(), P()),
        check_vma=False)
```

```python
import functools

import jax
import jax.numpy as jnp
from jax import lax
from jax.experimental import pallas as pl
from jax.experimental.pallas import tpu as pltpu
from jax.sharding import PartitionSpec as P


LN_EPS = 1e-5
CORES = 2
UNITS = 4
NEAR, FAR = (1, 3), (3, 1)
LANES = 128
PACK = 16
STRIPS = 7
SMALL = 24
STREAM = 30_000_000
KEEP = {'keepdims': True}
F32 = jnp.float32
BF16 = jnp.bfloat16
ALL = Ellipsis
MESH_ID = pl.DeviceIdType.MESH
NT = (((1,), (1,)), ((), ()))


def ring_offsets(n_x):
    near = [d for d in (1, n_x - 1) if 0 < d < n_x]
    near = list(dict.fromkeys(near))
    far = [d for d in range(2, n_x - 1)]
    out = [(0, 1)]
    for group in (near, far):
        for core in range(CORES):
            out += [(d, core) for d in group]
    return out


class Place:
    def __init__(self, n_ep, grid):
        self.n_x, self.grid = n_ep // CORES, grid
        self.ep, self.dp = lax.axis_index('ep'), lax.axis_index('dp')
        self.x, self.core = self.ep // CORES, self.ep % CORES
        self.z, self.y = self.dp // grid, self.dp % grid
        self.offsets = ring_offsets(self.n_x)

    def ep_to(self, k):
        dx, dc = self.offsets[k]
        return lax.rem(self.x + dx, self.n_x) * CORES + lax.rem(self.core + dc, CORES)

    def ep_from(self, k):
        dx, dc = self.offsets[k]
        return lax.rem(self.x + (self.n_x - dx), self.n_x) * CORES + lax.rem(self.core + dc, CORES)

    def step(self, axis, k):
        here = self.y if axis == 'y' else self.z
        return lax.rem(here + k + self.grid, self.grid)

    def device(self, axis, k):
        if axis == 'y':
            return (self.z * self.grid + self.step('y', k), self.ep)
        return (self.step('z', k) * self.grid + self.y, self.ep)

    def flip(self, axis, bits):
        if axis == 'y':
            return (self.z * self.grid + (self.y ^ bits), self.ep)
        return ((self.z ^ bits) * self.grid + self.y, self.ep)

    def arrive(self):
        sem = pltpu.get_barrier_semaphore()
        peers = [(self.dp, self.ep_to(k)) for k in range(len(self.offsets))]
        for k in range(1, self.grid):
            peers += [self.device('y', k), self.device('z', k)]
        for peer in peers:
            pl.semaphore_signal(sem, inc=1, device_id=peer, device_id_type=MESH_ID)
        return len(peers)

    def barrier(self, signals=None):
        pl.semaphore_wait(pltpu.get_barrier_semaphore(), self.arrive() if signals is None else signals)


def widen(out, rows):
    out[ALL] = jnp.zeros_like(out)
    out[:rows.shape[0], :] = rows


def cost(flops, size):
    return pl.CostEstimate(flops=flops, bytes_accessed=size, transcendentals=0)


def rows_at(start, size, unit):
    return pl.ds(pl.multiple_of(start, unit), size)


class Spread:
    STAGES = [range(2 ** i - 1, 2 ** (i + 1) - 1) for i in range(UNITS)]

    def __init__(self, here, own, held, send, recv):
        self.here, self.own, self.held, self.sems = here, own, held, (send, recv)

    def plan(self, unit, index):
        axes = ('y', 'z') if unit < UNITS // 2 else ('z', 'y')
        one, two = FAR if unit % 2 else NEAR
        line = (0, one, two, one ^ two)
        if index < 1:
            return axes, (axes[0], one), (0, 0)
        if index < 3:
            return axes, (axes[0], two), (line[index - 1], 0)
        if index < 7:
            return axes, (axes[1], one), (line[index - 3], 0)
        return axes, (axes[1], two), (line[(index - 7) % 4], (0, one)[(index - 7) // 4])

    def copy(self, unit, index):
        axes, (axis, flip), offsets = self.plan(unit, index)
        at = dict(zip(axes, offsets))
        owner = (self.here.z ^ at['z']) * self.here.grid + (self.here.y ^ at['y'])
        held = self.held.at[owner, unit]
        source = self.own.at[unit] if self.own is not None and offsets == (0, 0) else held
        return pltpu.make_async_remote_copy(src_ref=source, dst_ref=held, send_sem=self.sems[0].at[unit, index],
                                            recv_sem=self.sems[1].at[unit, index], device_id=self.here.flip(axis, flip),
                                            device_id_type=MESH_ID)

    def each(self, stage, picks=None):
        ids = self.STAGES[stage]
        for index in ids if picks is None else [ids[p] for p in picks]:
            for unit in range(UNITS):
                yield self.copy(unit, index)

    def send(self, stage, picks=None):
        for c in self.each(stage, picks):
            c.start()

    def receive(self, stage):
        for c in self.each(stage):
            c.wait_recv()

    def sent(self, stage):
        for c in self.each(stage):
            c.wait_send()


def tail_kernel(grid, cap, *refs):
    refs = list(refs)
    take = lambda n: [refs.pop(0) for _ in range(n)]
    _, o_next_h, dh_next_h, x_h, dy_h, hid_h, o_h, dh_h, stats, err_one, err_two, lnw, router_in = take(13)
    held, out, dx, small = take(4)
    x_v, dy_v, hid_v, o_v, dh_v, sel_one, sel_two, grad_h, val, router = take(10)
    first, second, third, c_one, c_two, c_three = take(6)
    loc, sp_s, sp_r, ba_s, ba_r, s_one, r_one, s_two, r_two, s_three, r_three, s_four, r_four = take(13)
    n_tok, d_model = x_v.shape
    rows = o_next_h.shape[0]
    n_ep, _, width = first.shape
    wide = min(512, d_model)
    here = Place(n_ep, grid)
    n_peer = len(here.offsets)
    ep = here.ep
    remote = functools.partial(pltpu.make_async_remote_copy, device_id_type=MESH_ID)
    here.barrier()
    spread = Spread(here, None, held, sp_s, sp_r)
    spread.send(3)

    def block(e, base=0):
        return rows_at(base + e * cap, cap, PACK)

    pairs = ((o_next_h, o_v), (dh_next_h, dh_v))

    def back(j, k):
        src, dst = pairs[j]
        return remote(src_ref=src.at[block(here.ep_to(k)), :], dst_ref=dst.at[block(ep, rows), :],
                      send_sem=ba_s.at[j, k], recv_sem=ba_r.at[j, k], device_id=(here.dp, here.ep_to(k)))

    own = [pltpu.make_async_copy(src.at[block(ep), :], dst.at[block(ep, rows), :], loc.at[j]) for j, (src, dst) in enumerate(pairs)]
    for j in range(2):
        for k in range(n_peer):
            back(j, k).start()
        own[j].start()
    home = pl.ds(0, rows)
    loads = [pltpu.make_async_copy(src, dst, loc.at[2 + i]) for i, (src, dst) in enumerate((
        (x_h, x_v), (dy_h, dy_v), (hid_h, hid_v), (o_h, o_v.at[home, :]), (dh_h, dh_v.at[home, :])))]
    for c in loads:
        c.start()
    widen(router, router_in[ALL])
    slots = lax.broadcasted_iota(jnp.int32, (n_tok, 2 * rows), 1)
    sel_one[ALL] = (slots == stats[:, 4:5].astype(jnp.int32)).astype(F32).astype(BF16)
    sel_two[ALL] = (slots == stats[:, 5:6].astype(jnp.int32)).astype(F32).astype(BF16)
    gate_one, gate_two, mean, inv_std = [stats[:, i:i + 1] for i in range(4)]
    zero = jnp.zeros((n_tok, 1), F32)
    for c in loads:
        c.wait()
    own[0].wait()
    for k in range(n_peer):
        back(0, k).wait_recv()

    def mix(i, sums):
        cols = rows_at(i * wide, wide, LANES)
        one = jnp.dot(sel_one[ALL], o_v[:, cols], preferred_element_type=F32)
        two = jnp.dot(sel_two[ALL], o_v[:, cols], preferred_element_type=F32)
        dy = dy_v[:, cols].astype(F32)
        out[:, cols] = (x_v[:, cols].astype(F32) + (gate_one * one + gate_two * two)).astype(BF16)
        return sums[0] + jnp.sum(dy * one, axis=1, **KEEP), sums[1] + jnp.sum(dy * two, axis=1, **KEEP)

    dgate_one, dgate_two = lax.fori_loop(0, d_model // wide, mix, (zero, zero))
    d_logits = ((dgate_one * gate_one) * err_one[ALL] + (dgate_two * gate_two) * err_two[ALL]).astype(BF16)
    lanes = d_logits.shape[1]
    eye = (lax.broadcasted_iota(jnp.int32, (lanes, lanes), 0)
           == lax.broadcasted_iota(jnp.int32, (lanes, lanes), 1)).astype(F32).astype(BF16)
    d_logits_t = lax.dot_general(eye, d_logits, NT, preferred_element_type=F32).astype(BF16)[:PACK]
    sel_both = sel_one[ALL] + sel_two[ALL]
    row = lax.broadcasted_iota(jnp.int32, (8, wide), 0)
    own[1].wait()
    for k in range(n_peer):
        back(1, k).wait_recv()

    def gradient(i, sums):
        cols = rows_at(i * wide, wide, LANES)
        grad = (jnp.dot(d_logits, router[:, cols], preferred_element_type=F32)
                + jnp.dot(sel_both, dh_v[:, cols], preferred_element_type=F32))
        x_hat = (x_v[:, cols].astype(F32) - mean) * inv_std
        grad_h[:, cols] = grad
        val[:PACK, cols] = jnp.dot(d_logits_t, hid_v[:, cols], preferred_element_type=F32)
        d_weight = jnp.sum(grad * x_hat, axis=0, **KEEP)
        d_bias = jnp.sum(grad, axis=0, **KEEP)
        val[PACK:SMALL, cols] = jnp.where(row == 0, d_weight, jnp.where(row == 1, d_bias, 0.0))
        scaled = grad * lnw[:, cols]
        return sums[0] + jnp.sum(scaled, axis=1, **KEEP), sums[1] + jnp.sum(scaled * x_hat, axis=1, **KEEP)

    mean_one, mean_two = lax.fori_loop(0, d_model // wide, gradient, (zero, zero))
    mean_one, mean_two = mean_one / d_model, mean_two / d_model

    def part(e):
        return rows_at(e * width, width, LANES)

    def scatter(k):
        to = here.ep_to(k)
        return remote(src_ref=val.at[:, part(to)], dst_ref=first.at[ep], send_sem=s_one.at[k], recv_sem=r_one.at[k],
                      device_id=(here.dp, to))

    def along(axis, src, dst, send, recv, k):
        mine = here.y if axis == 'y' else here.z
        return remote(src_ref=src, dst_ref=dst.at[mine], send_sem=send.at[k], recv_sem=recv.at[k], device_id=here.device(axis, k))

    def gather(k):
        return remote(src_ref=c_three, dst_ref=small.at[:, part(ep)], send_sem=s_four.at[k], recv_sem=r_four.at[k],
                      device_id=(here.dp, here.ep_to(k)))

    def add_up(ref, n):
        total = ref[0]
        for i in range(1, n):
            total = total + ref[i]
        return total

    for k in range(n_peer):
        scatter(k).start()
    first[ep] = val[:, part(ep)]

    @pl.loop(0, d_model // wide)
    def _(i):
        cols = rows_at(i * wide, wide, LANES)
        x_hat = (x_v[:, cols].astype(F32) - mean) * inv_std
        step = inv_std * (grad_h[:, cols] * lnw[:, cols] - mean_one - x_hat * mean_two)
        dx[:, cols] = (dy_v[:, cols].astype(F32) + step).astype(BF16)

    for k in range(n_peer):
        scatter(k).wait_recv()
    c_one[ALL] = add_up(first, n_ep)
    second[here.y] = c_one[ALL]
    for k in range(1, grid):
        along('y', c_one, second, s_two, r_two, k).start()
    for k in range(1, grid):
        along('y', c_one, second, s_two, r_two, k).wait_recv()
    c_two[ALL] = add_up(second, grid)
    third[here.z] = c_two[ALL]
    for k in range(1, grid):
        along('z', c_two, third, s_three, r_three, k).start()
    for k in range(1, grid):
        along('z', c_two, third, s_three, r_three, k).wait_recv()
    c_three[ALL] = add_up(third, grid)
    for k in range(n_peer):
        gather(k).start()
    small[:, part(ep)] = c_three[ALL]
    for k in range(n_peer):
        gather(k).wait_recv()
    for k in range(n_peer):
        scatter(k).wait_send()
        gather(k).wait_send()
        back(0, k).wait_send()
        back(1, k).wait_send()
    for k in range(1, grid):
        along('y', c_one, second, s_two, r_two, k).wait_send()
        along('z', c_two, third, s_three, r_three, k).wait_send()
    spread.receive(3)
    spread.sent(3)


def tail_call(held, o_next, dh_next, tok_x, tok_dy, hidden, o, dh, stats, err_one, err_two, lnw, router, cap, grid, collective_id):
    vmem, dma = pltpu.VMEM, pltpu.SemaphoreType.DMA
    n_tok, d_model = tok_x.shape
    rows = o.shape[0]
    n_ep = rows // cap
    n_peer, width = n_ep - 1, d_model // n_ep
    hbm, on_chip = pl.BlockSpec(memory_space=pl.ANY), pl.BlockSpec(memory_space=pltpu.VMEM)
    tokens = jax.ShapeDtypeStruct((n_tok, d_model), BF16)
    peers, ring = dma((n_peer,)), dma((grid,))
    deep, both = dma((UNITS, 15)), dma((2, n_peer))
    return pl.pallas_call(
        functools.partial(tail_kernel, grid, cap),
        out_shape=(jax.ShapeDtypeStruct(held.shape, F32), tokens, tokens, jax.ShapeDtypeStruct((SMALL, d_model), F32)),
        in_specs=[hbm] * 8 + [on_chip] * 5, out_specs=(hbm, on_chip, on_chip, on_chip), input_output_aliases={0: 0},
        scratch_shapes=[vmem((n_tok, d_model), BF16)] * 3 + [vmem((2 * rows, d_model), BF16)] * 2
        + [vmem((n_tok, 2 * rows), BF16)] * 2 + [vmem((n_tok, d_model), F32), vmem((SMALL, d_model), F32), vmem((LANES, d_model), BF16)]
        + [vmem((n_ep, SMALL, width), F32), vmem((grid, SMALL, width), F32), vmem((grid, SMALL, width), F32)] + [vmem((SMALL, width), F32)] * 3
        + [dma((7,)), deep, deep, both, both,
           peers, peers, ring, ring, ring, ring, peers, peers],
        compiler_params=pltpu.CompilerParams(collective_id=collective_id, has_side_effects=True, vmem_limit_bytes=50 * 2 ** 20),
        cost_estimate=cost(10_000_000_000, STREAM),
        name='tail',
    )(held, o_next, dh_next, tok_x, tok_dy, hidden, o, dh, stats, err_one, err_two, lnw, router)


def expert_kernel(dims, *refs):
    expert, grid, chunk, cap, first = dims
    refs = list(refs)
    take = lambda n: [refs.pop(0) for _ in range(n)]
    if first:
        marks, *lines = take(1 + UNITS)
        lnw, lnb, router_in, x_h, dy_h, wg_h, wu_h, wd_h = take(8)
        o_h, dh_h, sh_h, h_next, q_next, hsl_next, qsl_next, hid_h, stats, err_one, err_two = take(11)
    else:
        h_next, q_next, hsl_next, qsl_next, wg_h, wu_h, wd_h, *carry = take(9)
        done_h, = take(1)
        o_h, dh_h, sh_h, *carry_out = take(5)
        all_h, = take(1)
    h_recv, q_recv, wg, wu, wd, a_t, b_t, d_t, u_all, da_all, db_all, h_sl, q_sl, dw, rsb, act, act_b, eye = take(18)
    loc, hs_s, hs_r, qs_s, qs_r, ga_s, ga_r, rs_s, rs_r = take(9)
    if first:
        sel_h, sel_q, sel_h_next, sel_q_next, hidden, grad_one, grad_two, h_send, q_send, h_send_next, q_send_next, router, wide_table = take(13)
        xh_s, xh_r, xq_s, xq_r, nh_s, nh_r, nq_s, nq_r, ns_h_s, ns_h_r, ns_q_s, ns_q_r, lin = take(13)
        o_v, dh_v = h_send, q_send
    else:
        o_v, dh_v = take(2)
        ba_s, ba_r, ba_l, lin, sp_s, sp_r = take(6)
    rows, d_model = h_recv.shape
    ff = wg.shape[0]
    quarter = d_model // grid
    share = ff // grid
    here = Place(rows // cap, grid)
    n_peer = len(here.offsets)
    ep = here.ep
    remote = functools.partial(pltpu.make_async_remote_copy, device_id_type=MESH_ID)
    wide = chunk // 2

    def spot(axis):
        return here.y if axis == 'y' else here.z

    def block(e):
        return rows_at(e * cap, cap, PACK)

    weights = [pltpu.make_async_copy(src.at[expert], dst, loc.at[i]) for i, (src, dst) in enumerate(((wg_h, wg), (wu_h, wu), (wd_h, wd)))]

    def x_copy(src, dst, send, recv, k):
        return remote(src_ref=src.at[block(here.ep_to(k)), :], dst_ref=dst.at[block(ep), :],
                      send_sem=send.at[k], recv_sem=recv.at[k], device_id=(here.dp, here.ep_to(k)))

    def slice_copy(axis, buf, sl, send, recv, src_ep, k):
        return remote(src_ref=buf.at[block(src_ep), rows_at(here.step(axis, k) * quarter, quarter, LANES)],
                      dst_ref=sl.at[rows_at(spot(axis) * rows + src_ep * cap, cap, PACK), :],
                      send_sem=send.at[k], recv_sem=recv.at[k], device_id=here.device(axis, k))

    def slices(axis, buf, sl, send, recv, k):
        return remote(src_ref=buf.at[:, pl.ds(0, quarter)], dst_ref=sl.at[pl.ds(0, rows), :],
                      send_sem=send.at[k], recv_sem=recv.at[k], device_id=here.device(axis, k))

    half = ff // 2
    halves = ((pl.ds(0, half), NEAR), (pl.ds(half, half), FAR))
    gathers = [(ref, part, axis, *order) for ref, axis in ((u_all, 'z'), (da_all, 'y'), (db_all, 'y')) for part, order in halves]

    def share_t(g, j):
        ref, part, axis, one, two = gathers[g]
        flip = two if j else one
        owner = spot(axis) ^ (one if j == 2 else 0)
        view = ref.at[part, rows_at(owner * rows, rows, LANES)]
        return remote(src_ref=view, dst_ref=view, send_sem=ga_s.at[g, j], recv_sem=ga_r.at[g, j], device_id=here.flip(axis, flip))

    def share_start(t):
        for g in (2 * t, 2 * t + 1):
            share_t(g, 0).start()

    def share_on(t):
        for g in (2 * t, 2 * t + 1):
            share_t(g, 0).wait_recv()
            for j in (1, 2):
                share_t(g, j).start()

    def share_done(t):
        for g in (2 * t, 2 * t + 1):
            for j in (1, 2):
                share_t(g, j).wait_recv()

    wing = quarter // 2
    wings = ((pl.ds(0, wing), NEAR), (pl.ds(wing, wing), FAR))
    reduces = [(t, cols, axis, *order) for t, axis in enumerate('zzy') for cols, order in wings]

    def part_at(i):
        return rows_at(i * share, share, 8)

    def reduce_copy(r, j):
        t, cols, axis, one, two = reduces[r]
        here_at = spot(axis)
        flip, chunk_at = ((one, here_at ^ one), (one, here_at ^ one ^ two), (two, here_at ^ two))[j]
        return remote(src_ref=dw.at[t, part_at(chunk_at), cols], dst_ref=rsb.at[t, j, :, cols],
                      send_sem=rs_s.at[r, j], recv_sem=rs_r.at[r, j], device_id=here.flip(axis, flip))

    def reduce_start(t):
        for r in (2 * t, 2 * t + 1):
            for j in (0, 1):
                reduce_copy(r, j).start()

    def reduce_on(t):
        for r in (2 * t, 2 * t + 1):
            _, cols, axis, _, two = reduces[r]
            reduce_copy(r, 0).wait_recv()
            reduce_copy(r, 1).wait_recv()
            on = part_at(spot(axis) ^ two)
            dw[t, on, cols] = dw[t, on, cols] + rsb[t, 1, :, cols]
            reduce_copy(r, 2).start()

    def reduce_end(t):
        axis = 'zzy'[t]
        for r in (2 * t, 2 * t + 1):
            reduce_copy(r, 2).wait_recv()
        rsb[t, 0] = dw[t, part_at(spot(axis)), :] + rsb[t, 0] + rsb[t, 2]
        unit = quarter // UNITS
        outs = [pltpu.make_async_copy(rsb.at[t, 0, :, pl.ds(i * unit, unit)], sh_h.at[i, t], loc.at[5 + t * UNITS + i]) for i in range(UNITS)]
        for c in outs:
            c.start()
        return outs

    def own_slice(axis, buf, sl):
        sl[rows_at(spot(axis) * rows, rows, PACK), :] = buf[:, rows_at(spot(axis) * quarter, quarter, LANES)]

    strip = ff // STRIPS
    u_cols = rows_at(here.z * rows, rows, LANES)
    g_cols = rows_at(here.y * rows, rows, LANES)

    def forward_pass():
        a_t[ALL] = jnp.zeros_like(a_t)
        b_t[ALL] = jnp.zeros_like(b_t)

        @pl.loop(0, d_model // chunk)
        def _(i):
            cols = rows_at(i * chunk, chunk, LANES)
            a_t[ALL] += lax.dot_general(wg[:, cols], h_recv[:, cols], NT, preferred_element_type=F32)
            b_t[ALL] += lax.dot_general(wu[:, cols], h_recv[:, cols], NT, preferred_element_type=F32)

        @pl.loop(0, STRIPS)
        def _(i):
            r = rows_at(i * strip, strip, PACK)
            a = a_t[r, :]
            u_all[r, u_cols] = (a * jax.nn.sigmoid(a) * b_t[r, :]).astype(BF16)

    def backward_pass():
        d_t[ALL] = jnp.zeros_like(d_t)

        @pl.loop(0, d_model // chunk)
        def _(i):
            cols = rows_at(i * chunk, chunk, LANES)
            d_t[ALL] += lax.dot_general(wd[:, cols], q_recv[:, cols], NT, preferred_element_type=F32)

        @pl.loop(0, STRIPS)
        def _(i):
            r = rows_at(i * strip, strip, PACK)
            a, b, du = a_t[r, :], b_t[r, :], d_t[r, :]
            sig = jax.nn.sigmoid(a)
            silu = a * sig
            da_all[r, g_cols] = (du * b * sig * (1.0 + a * (1.0 - sig))).astype(BF16)
            db_all[r, g_cols] = (du * silu).astype(BF16)

    def untranspose(out, ref, cols):
        out[ALL] = lax.dot_general(eye[ALL], ref[:, cols], NT, preferred_element_type=F32).astype(BF16)

    def o_pass():
        @pl.loop(0, d_model // wide)
        def _(i):
            cols = rows_at(i * wide, wide, LANES)
            o_v[:, cols] = jnp.dot(act[ALL], wd[:, cols], preferred_element_type=F32).astype(BF16)

    def dh_pass():
        @pl.loop(0, d_model // wide)
        def _(i):
            cols = rows_at(i * wide, wide, LANES)
            dh_v[:, cols] = (jnp.dot(act[ALL], wg[:, cols], preferred_element_type=F32)
                             + jnp.dot(act_b[ALL], wu[:, cols], preferred_element_type=F32)).astype(BF16)

    def weight_grad(t, left, right):
        @pl.loop(0, quarter // wide)
        def _(i):
            cols = rows_at(i * wide, wide, LANES)
            dw[t, :, cols] = jnp.dot(left[ALL], right[:, cols], preferred_element_type=F32)

    def forward_part():
        weights[0].wait()
        weights[1].wait()
        forward_pass()
        share_start(0)
        untranspose(act, u_all, u_cols)
        weights[2].wait()
        o_pass()
        o_out = pltpu.make_async_copy(o_v, o_h, loc.at[3])
        o_out.start()
        return o_out

    def make_eye():
        eye[ALL] = (lax.broadcasted_iota(jnp.int32, (rows, rows), 0)
                    == lax.broadcasted_iota(jnp.int32, (rows, rows), 1)).astype(F32).astype(BF16)

    if first:
        inputs = [pltpu.make_async_copy(src, dst, lin.at[i]) for i, (src, dst) in enumerate(((x_h, hidden), (dy_h, grad_two)))]
        n_tok = hidden.shape[0]
        lane = lax.broadcasted_iota(jnp.int32, stats.shape, 1)
        n_exp = router_in.shape[0]
        for c in inputs:
            c.start()
        signals = here.arrive()
        make_eye()

        def place(ids, slots):
            local = jnp.bitwise_and(ids, 1)
            return jnp.where(slots >= 0, local * rows + jnp.right_shift(ids, 1) * cap + slots, -1)

        for e, (one, two) in enumerate(((sel_h, sel_q), (sel_h_next, sel_q_next))):
            slot = lax.broadcasted_iota(jnp.int32, one.shape, 0) + e * rows
            hits = [(slot == place(lines[i][ALL], lines[i + 2][ALL])).astype(F32).astype(BF16) for i in range(2)]
            one[ALL] = hits[0] + hits[1]
            for i in range(2):
                two[:, i * n_tok:(i + 1) * n_tok] = hits[i]
        inputs[0].wait()
        strip_rows = 2 * PACK

        @pl.loop(0, n_tok // strip_rows)
        def _(i):
            r = rows_at(i * strip_rows, strip_rows, PACK)
            x = hidden[r, :].astype(F32)
            mean = jnp.mean(x, axis=1, **KEEP)
            centered = x - mean
            inv_std = lax.rsqrt(jnp.mean(centered * centered, axis=1, **KEEP) + LN_EPS)
            hidden[r, :] = (centered * inv_std * lnw[ALL] + lnb[ALL]).astype(BF16)
            at = lane[:strip_rows]
            stats[r, :] = jnp.where(at == 2, mean, jnp.where(at == 3, inv_std, 0.0))

        hid_out = pltpu.make_async_copy(hidden, hid_h, lin.at[2])
        hid_out.start()

        def gates():
            widen(router, router_in[ALL])
            row = lax.broadcasted_iota(jnp.int32, marks.shape, 0)
            index_rows = sum(jnp.where(row == i, lines[i][ALL], 0) for i in range(UNITS))
            widen(wide_table, jnp.concatenate([marks[ALL], index_rows]).astype(F32).astype(BF16))
            columns = lax.dot_general(eye[:n_tok, :n_tok], wide_table[ALL], NT, preferred_element_type=F32)
            logits = lax.dot_general(hidden[ALL], router[ALL], NT, preferred_element_type=F32)
            ints = [columns[:, n_exp + i:n_exp + i + 1].astype(jnp.int32) for i in range(UNITS)]
            choices, allowed = ints[:2], jnp.logical_and(columns > 0, lane < n_exp)
            found = [place(*ints[i::2]) for i in range(2)]
            found = [value.astype(F32) for value in found]
            for choice, err in zip(choices, (err_one, err_two)):
                masked = jnp.where(allowed, logits, -1e30)
                weight = jnp.exp(masked - jnp.max(masked, axis=1, **KEEP))
                prob = weight / jnp.sum(weight, axis=1, **KEEP)
                pick = (lane == choice).astype(F32)
                found.append(jnp.sum(prob * pick, axis=1, **KEEP))
                err[ALL] = pick - prob
                allowed = jnp.logical_and(allowed, lane != choice)
            total = stats[ALL]
            for i, value in zip((4, 5, 0, 1), found):
                total = jnp.where(lane == i, value, total)
            stats[ALL] = total
            inputs[1].wait()

            @pl.loop(0, d_model // wide)
            def _(i):
                cols = rows_at(i * wide, wide, LANES)
                dy = grad_two[:, cols].astype(F32)
                grad_one[:, cols] = (stats[:, 0:1] * dy).astype(BF16)
                grad_two[:, cols] = (stats[:, 1:2] * dy).astype(BF16)

        def gather(sel, source, out, e):
            @pl.loop(0, d_model // chunk)
            def _(i):
                cols = rows_at(i * chunk, chunk, LANES)
                total = jnp.dot(sel[block(e), :n_tok], source[0][:, cols], preferred_element_type=F32)
                for j in range(1, len(source)):
                    total += jnp.dot(sel[block(e), j * n_tok:(j + 1) * n_tok], source[j][:, cols], preferred_element_type=F32)
                out[block(e), cols] = total.astype(BF16)

        rows_h, rows_q = (hidden,), (grad_one, grad_two)
        now = ((sel_h, rows_h, h_send, h_recv, xh_s, xh_r), (sel_q, rows_q, q_send, q_recv, xq_s, xq_r))
        later = ((sel_h_next, rows_h, h_send_next, h_next, nh_s, nh_r), (sel_q_next, rows_q, q_send_next, q_next, nq_s, nq_r))

        def copy_of(what, k):
            _, _, out, recv_buf, send, recv = what
            return x_copy(out, recv_buf, send, recv, k)

        others = range(1, n_peer)
        pairs = list(zip(others[::2], others[1::2]))
        steps = [(group, i, ks) for group, order in ((now, (0, 1)), (later, (1, 0))) for i in order for ks in pairs]
        ahead = 2 * len(pairs)

        def gather_step(n):
            if n < len(steps):
                group, i, ks = steps[n]
                for k in ks:
                    gather(group[i][0], group[i][1], group[i][2], here.ep_to(k))

        def send_step(n):
            if n < len(steps):
                group, i, ks = steps[n]
                for k in ks:
                    copy_of(group[i], k).start()

        def sent_step(n):
            if n < len(steps):
                group, i, ks = steps[n]
                for k in ks:
                    copy_of(group[i], k).wait_send()

        def partner(what):
            gather(what[0], what[1], what[2], here.ep_to(0))
            copy_of(what, 0).start()

        gather_step(0)
        here.barrier(signals)
        send_step(0)
        gather_step(1)
        send_step(1)
        for c in weights:
            c.start()
        for i, what in enumerate(now):
            partner(what)
            gather(what[0], what[1], what[3], ep)
            if not i:
                gates()
        spread = (('y', h_recv, h_sl, hs_s, hs_r), ('z', q_recv, q_sl, qs_s, qs_r))
        spread_next = (('y', h_next, hsl_next, ns_h_s, ns_h_r), ('z', q_next, qsl_next, ns_q_s, ns_q_r))

        def forward_own(spread, bufs):
            for (axis, _, sl, send, recv), buf in zip(spread, bufs):
                for k in range(1, grid):
                    slice_copy(axis, buf, sl, send, recv, ep, k).start()

        def forward(group, spread, i, p):
            axis, buf, sl, send, recv = spread[i]
            copy_of(group[i], p).wait_recv()
            for k in range(1, grid):
                slice_copy(axis, buf, sl, send, recv, here.ep_from(p), k).start()

        def forward_step(n):
            if n < len(steps):
                group, i, ks = steps[n]
                for k in ks:
                    forward(group, spread if group is now else spread_next, i, k)

        forward_own(spread, (h_recv, q_recv))
        for i in range(2):
            forward(now, spread, i, 0)
        for what in later:
            gather(what[0], what[1], what[2], ep)
        own_next = [pltpu.make_async_copy(what[2].at[block(ep), :], what[3].at[block(ep), :], lin.at[7 + i]) for i, what in enumerate(later)]
        for what in later:
            partner(what)
        middle, last = max(len(pairs) - 1, 0), max(ahead - 1, 0)
        for n in range(last + 1):
            gather_step(n + 2)
            sent_step(n)
            send_step(n + 2)
            forward_step(n)
            if n == middle:
                own_slice('y', h_recv, h_sl)
                copy_of(now[0], 0).wait_send()
                o_out = forward_part()
            if n == min(middle + 2, last):
                share_on(0)
            if n >= 2:
                gather_step(n + ahead)
            if n == min(1, last):
                forward_own(spread_next, (h_send_next, q_send_next))
                for i in range(2):
                    forward(later, spread_next, i, 0)
        send_step(ahead + 2)
        send_step(ahead + 3)
        for c in own_next:
            c.start()
        own_slice('z', q_recv, q_sl)
        copy_of(now[1], 0).wait_send()
    else:
        load_h, load_q = [pltpu.make_async_copy(src, dst, lin.at[2 + i * grid]) for i, (src, dst) in enumerate(((h_next, h_recv), (q_next, q_recv)))]
        load_slices = []
        for i, (axis, src, dst) in enumerate((('z', qsl_next, q_sl), ('y', hsl_next, h_sl))):
            for k in range(1, grid):
                part = rows_at(here.step(axis, k) * rows, rows, PACK)
                load_slices.append(pltpu.make_async_copy(src.at[part, :], dst.at[part, :], lin.at[2 + i * grid + k]))
        for c in [load_h] + weights + [load_q] + load_slices:
            c.start()
        here.barrier()
        back = list(zip(carry, carry_out))
        spread_unit = Spread(here, done_h, all_h, sp_s, sp_r)
        own_unit = pltpu.make_async_copy(done_h, all_h.at[here.dp], lin.at[1])
        spread_unit.send(0)
        spread_unit.send(1, (0,))

        def back_copy(j, k):
            src, dst = back[j]
            return remote(src_ref=src.at[block(here.ep_to(k)), :], dst_ref=dst.at[block(ep), :],
                          send_sem=ba_s.at[j, k], recv_sem=ba_r.at[j, k], device_id=(here.dp, here.ep_to(k)))

        def back_own(j):
            src, dst = back[j]
            return pltpu.make_async_copy(src.at[block(ep), :], dst.at[block(ep), :], ba_l.at[j])

        def send_back(j):
            for k in range(n_peer):
                back_copy(j, k).start()
            back_own(j).start()

        for j in range(len(carry)):
            send_back(j)
        make_eye()
        load_h.wait()
        o_out = forward_part()
        load_q.wait()
        own_slice('y', h_recv, h_sl)
        own_slice('z', q_recv, q_sl)
        own_unit.start()

    backward_pass()
    share_start(1)
    share_start(2)
    if first:
        sent_step(ahead)
        send_step(ahead + 4)
    else:
        share_on(0)
    untranspose(act, da_all, g_cols)
    untranspose(act_b, db_all, g_cols)
    share_on(1)
    share_on(2)
    if not first:
        spread_unit.receive(0)
        spread_unit.send(1, (1,))
    dh_pass()
    dh_out = pltpu.make_async_copy(dh_v, dh_h, loc.at[4])
    dh_out.start()
    if first:
        sent_step(ahead + 1)
        send_step(ahead + 5)
        forward_step(ahead)
        for k in range(1, grid):
            slices('z', q_recv, q_sl, qs_s, qs_r, k).wait_recv()
            slices('y', h_recv, h_sl, hs_s, hs_r, k).wait_recv()
    else:
        for c in load_slices:
            c.wait()
    share_done(1)
    weight_grad(0, da_all, h_sl)
    reduce_start(0)
    if not first:
        spread_unit.send(2, (0,))
    share_done(0)
    weight_grad(2, u_all, q_sl)
    share_done(2)
    weight_grad(1, db_all, h_sl)
    reduce_start(1)
    reduce_start(2)
    if first:
        forward_step(ahead + 1)
    else:
        spread_unit.receive(1)
    reduce_on(0)
    if not first:
        spread_unit.send(2, (1,))
    reduce_on(1)
    reduce_on(2)
    if first:
        for n in range(2, 5):
            forward_step(ahead + n)
    else:
        spread_unit.send(2, (2, 3))
    ends = reduce_end(0) + reduce_end(1) + reduce_end(2)
    if first:
        forward_step(ahead + 5)

    for j in range(3):
        for g in range(len(gathers)):
            share_t(g, j).wait_send()
            reduce_copy(g, j).wait_send()
    if first:
        for k in range(1, grid):
            for axis, buf, sl, send, recv in spread:
                slices(axis, buf, sl, send, recv, k).wait_send()
            for axis, buf, sl, send, recv in spread_next:
                slices(axis, buf, sl, send, recv, k).wait()
        for what in later:
            copy_of(what, 0).wait_send()
        for n in range(2, 6):
            sent_step(ahead + n)
        for c in own_next + [hid_out]:
            c.wait()
    else:
        for j in range(len(back)):
            for k in range(n_peer):
                back_copy(j, k).wait()
            back_own(j).wait()
        spread_unit.receive(2)
        for stage in range(3):
            spread_unit.sent(stage)
        own_unit.wait()
    for c in ends + [o_out, dh_out]:
        c.wait()


def expert_call(inputs, w_gate, w_up, w_down, expert, cap, grid, mesh_ep):
    first = expert == 0
    d_model = w_gate.shape[2]
    ff = w_gate.shape[1]
    rows = (mesh_ep if first else inputs[0].shape[0] // cap) * cap
    quarter, share = d_model // grid, ff // grid
    n_peer = rows // cap - 1
    chunk = min(1024, d_model)
    vmem, dma = pltpu.VMEM, pltpu.SemaphoreType.DMA
    hbm = pl.BlockSpec(memory_space=pl.ANY)
    on_chip = pl.BlockSpec(memory_space=pltpu.VMEM)
    row_block, slice_block = (rows, d_model), (grid * rows, quarter)
    scratch = [
        vmem(row_block, BF16), vmem(row_block, BF16),
        vmem((ff, d_model), BF16), vmem((ff, d_model), BF16), vmem((ff, d_model), BF16),
        vmem((ff, rows), F32), vmem((ff, rows), F32), vmem((ff, rows), F32),
        vmem((ff, grid * rows), BF16), vmem((ff, grid * rows), BF16), vmem((ff, grid * rows), BF16),
        vmem(slice_block, BF16), vmem(slice_block, BF16),
        vmem((3, ff, quarter), F32), vmem((3, 3, share, quarter), F32),
        vmem((rows, ff), BF16), vmem((rows, ff), BF16), vmem((rows, rows), BF16), dma((5 + 3 * UNITS,)),
    ] + [dma((grid,))] * 4 + [dma((6, 3))] * 4
    out = lambda shape, dtype=BF16: jax.ShapeDtypeStruct(shape, dtype)
    share_block = (UNITS, 3, share, quarter // UNITS)
    outs = [out(row_block), out(row_block), out(share_block, F32)]
    if first:
        tokens = inputs[-1].shape
        n_tok = tokens[0]
        scratch += [vmem((rows, i * n_tok), BF16) for i in (1, 2, 1, 2)] + [vmem(tokens, BF16)] * 3
        scratch += [vmem(row_block, BF16)] * 4 + [vmem((LANES, d_model), BF16), vmem((LANES, n_tok), BF16)] + [dma((n_peer,))] * 8 + [dma((grid,))] * 4 + [dma((9,))]
        operands = (*inputs, w_gate, w_up, w_down)
        outs += [out(row_block), out(row_block), out(slice_block), out(slice_block), out(tokens)] + [out((n_tok, LANES), F32)] * 3
        in_specs, out_specs = [on_chip] * 8 + [hbm] * 5, [hbm] * 8 + [on_chip] * 3
    else:
        h_next, q_next, hsl_next, qsl_next, *carry, done = inputs
        scratch += [vmem(row_block, BF16)] * 2 + [dma((2, n_peer))] * 2 + [dma((2,)), dma((2 + 2 * grid,))]
        scratch += [dma((UNITS, 15))] * 2
        operands = (h_next, q_next, hsl_next, qsl_next, w_gate, w_up, w_down, *carry, done)
        outs += [out(row_block), out(row_block), out((grid * grid,) + share_block, F32)]
        in_specs, out_specs = [hbm] * len(operands), [hbm] * len(outs)
    return pl.pallas_call(
        functools.partial(expert_kernel, (expert, grid, chunk, cap, first)),
        out_shape=tuple(outs), in_specs=in_specs, out_specs=tuple(out_specs), scratch_shapes=scratch,
        compiler_params=pltpu.CompilerParams(collective_id=expert, has_side_effects=True, vmem_limit_bytes=63 * 2 ** 20),
        cost_estimate=cost(2 * rows * d_model * ff * 9, STREAM),
    )(*operands)


def assemble_kernel(gate, up, down, *refs):
    n_pass = (len(refs) - 3) // 2 if len(refs) > 6 else 0
    outs = refs[-3 - n_pass:][:3]
    for j in range(n_pass):
        refs[-n_pass + j][ALL] = refs[j][ALL]
    grid, unit = gate.shape[1], gate.shape[-1]
    for c in range(grid):
        for i in range(UNITS):
            at = (c * UNITS + i) * unit
            outs[0][0, :, at:at + unit] = gate[0, c, i, 0]
            outs[1][0, :, at:at + unit] = up[0, c, i, 0]
            outs[2][0, :, at:at + unit] = down[c, 0, i, 0]


def assemble(gathered, expert, n_expert, into, through=()):
    grid, _, _, _, share, unit = gathered.shape
    cut = 2
    part = share // cut
    row_first = pl.BlockSpec((1, grid, UNITS, 1, part, unit), lambda r, h: (r, 0, 0, 0, h, 0))
    up_first = pl.BlockSpec((1, grid, UNITS, 1, part, unit), lambda r, h: (r, 0, 0, 1, h, 0))
    col_first = pl.BlockSpec((grid, 1, UNITS, 1, part, unit), lambda r, h: (0, r, 0, 2, h, 0))
    out_spec = pl.BlockSpec((1, part, grid * UNITS * unit), lambda r, h: (expert, r * cut + h, 0))
    whole = jax.ShapeDtypeStruct((n_expert, grid * share, grid * UNITS * unit), F32)
    strips = [pl.BlockSpec((x.shape[0] // (grid * cut), x.shape[1]), lambda r, h: (r * cut + h, 0)) for x in through]
    return pl.pallas_call(
        assemble_kernel, grid=(grid, cut), out_shape=(whole,) * 3 + tuple(jax.ShapeDtypeStruct(x.shape, x.dtype) for x in through),
        in_specs=[row_first, up_first, col_first] + strips + [pl.BlockSpec(memory_space=pl.ANY)] * len(into),
        out_specs=(out_spec,) * 3 + tuple(strips), input_output_aliases={3 + i: i for i in range(len(into))},
        compiler_params=pltpu.CompilerParams(vmem_limit_bytes=40 * 2 ** 20),
        cost_estimate=cost(1_000_000, 44_000_000),
    )(gathered, gathered, gathered, *through, *into)


def solution(mesh):
    n_ep = mesh.shape['ep']
    grid = round(mesh.shape['dp'] ** 0.5)
    tok_spec = P(('dp', 'ep'), None)
    row_spec = P(('dp', 'ep'))
    exp_spec = P('ep', None, None)

    def local_step(tok_x, tok_dy, exp_first, exp_second, eligible, slot_first, slot_second,
                   ln_weight, ln_bias, router, w_gate, w_up, w_down):
        n_local, _ = tok_x.shape
        n_exp = eligible.shape[1]
        local_exp = w_gate.shape[0]
        slot_cap = 3 * n_local // n_exp
        wg_t, wu_t = jnp.swapaxes(w_gate, 1, 2), jnp.swapaxes(w_up, 1, 2)

        lines = [x[None] for x in (exp_first, exp_second, slot_first, slot_second)]
        lnw, lnb = ln_weight.astype(F32)[None], ln_bias.astype(F32)[None]
        router_t = router.T
        o, dh, share, *landed, hidden, stats, err_one, err_two = expert_call(
            (eligible.T, *lines, lnw, lnb, router_t, tok_x, tok_dy), wg_t, wu_t, w_down, 0, slot_cap, grid, n_ep)
        o_next, dh_next, share, o, dh, held = expert_call((*landed, o, dh, share), wg_t, wu_t, w_down, 1, slot_cap, grid, n_ep)
        gathered_next = lax.all_gather(share, 'dp')
        held, out_tok, dx_tok, small = tail_call(
            held, o_next, dh_next, tok_x, tok_dy, hidden, o, dh, stats, err_one, err_two,
            lnw, router_t, slot_cap, grid, local_exp + 1)
        gathered = [x.reshape((grid, grid) + share.shape) for x in (held, gathered_next)]
        d_router, d_ln_weight, d_ln_bias = small[:n_exp].T, small[PACK], small[PACK + 1]
        *weights, out_tok, dx_tok = assemble(gathered[0], 0, local_exp, (), (out_tok, dx_tok))
        weights = assemble(gathered[1], 1, local_exp, weights)
        dw_gate, dw_up, dw_down = jnp.swapaxes(weights[0], 1, 2), jnp.swapaxes(weights[1], 1, 2), weights[2]
        return out_tok, dx_tok, dw_gate, dw_up, dw_down, d_router, d_ln_weight, d_ln_bias

    return jax.shard_map(
        local_step, mesh=mesh,
        in_specs=(tok_spec, tok_spec, row_spec, row_spec, tok_spec, row_spec, row_spec,
                  P(), P(), P(), exp_spec, exp_spec, exp_spec),
        out_specs=(tok_spec, tok_spec, exp_spec, exp_spec, exp_spec, P(), P(), P()),
        check_vma=False)
```
